32 devices in a mesh: clip: 16 (over z, y, core), seq: 2 (over x).
Axes of the slice: x: 2, y: 2, z: 4, core: 2. Of those that a mesh axis runs over, the one named last changes fastest.
Arguments:
- patches: bfloat16 [4096, 1280], P('clip'), may hold values from -6 to 6
- clip_tokens: int32 [16], P('clip'), may hold values from 16 to 64
- positions: int32 [16, 64], P('clip'), may hold values from 0 to 255, as said below
- norm_gain: float32 [1280], replicated, may hold values from 0.5 to 1.5
- norm_bias: float32 [1280], replicated, may hold values from -3 to 3
- w_qkv: bfloat16 [1280, 3, 1280], P(None, None, 'seq'), may hold values from -0.9503289 to 0.9503289
- b_qkv: float32 [3, 1280], P(None, 'seq'), may hold values from -3 to 3
- w_proj: bfloat16 [1280, 1280], P('seq'), may hold values from -0.15625 to 0.15625
- b_proj: float32 [1280], replicated, may hold values from -3 to 3
- merge_gain: float32 [1280], replicated, may hold values from 0.5 to 1.5
- merge_bias: float32 [1280], replicated, may hold values from -3 to 3
- grad_placed: bfloat16 [4096, 5120], P(('clip', 'seq')), may hold values from -0.09375 to 0.09375
Outputs:
- placed: bfloat16 [4096, 5120], P(('clip', 'seq'))
- grad_qkv: float32 [2, 1920, 1280], P('seq', 'clip')
The draws below stay inside these ranges and needn't reach their ends.
Inputs may be any that keep to these rules, and one draw needn't show every extreme that they name: The positions of one clip are distinct.
All inputs are finite; a program needn't handle non-finite values.
Results may differ from the reference program's by a relative error of at most 0.01.
Values may be sent and summed in bfloat16 or wider, within the bound.
No kernel may reach another device: no remote copies, remote signals or barrier semaphores. Data moves between devices by JAX's collectives and lax.ppermute only.
A program may use at most 64 MiB of HBM per device.

```python
import jax
import jax.numpy as jnp
from jax import lax

D = 1280
HEADS = 16
BLOCK = 256
HEAD = 80
TOKENS_CLIP = 64
LEN = 256
GROUPS = 16
N_SEQ = 2


def draw_positions(key, part):
    subkeys = jax.random.split(key, GROUPS)
    rows = jax.vmap(lambda single: jax.random.permutation(single, LEN)[:TOKENS_CLIP])(subkeys)
    return rows.astype(jnp.int32)


def draw_w_qkv(key, part):
    spread = D ** (-0.5)
    base = jnp.clip(jax.random.normal(key, (D, 3, D), jnp.float32), -6.0, 6.0) * spread
    return base.astype(jnp.bfloat16)


def plant(result, stream_key, least, top_value):
    dims = result.shape
    place = [jax.random.randint(jax.random.fold_in(stream_key, axis), (), 0, dims[axis]) for axis in range(len(dims))]
    result = result.at[tuple(place)].set(least)
    longest = dims.index(max(dims))
    place[longest] = (place[longest] + 1) % dims[longest]
    return result.at[tuple(place)].set(top_value)


def steps_of(own_key, dims, shards, least, largest):
    def one(dim, shards_of):
        heights = jax.random.uniform(jax.random.fold_in(jax.random.fold_in(own_key, 6), dim), (shards_of,), jnp.float32, least / len(shards), largest / len(shards))
        return jnp.repeat(jnp.exp(heights), dims[dim] // shards_of).reshape((-1,) + (1,) * (len(dims) - dim - 1))

    factor_of = one(*shards[0])
    for cut in shards[1:]:
        factor_of = factor_of * one(*cut)
    return factor_of


def gaussian(key, shape, width, bound, cuts=(), held_as=jnp.bfloat16):
    values = jax.random.normal(key, shape, jnp.float32) * width
    if len(cuts) > 0:
        values = steps_of(key, shape, cuts, -0.22, 0.18) * values
    return jnp.clip(values, min=-bound, max=bound).astype(held_as)


def setup_inputs(seed: int = 0) -> dict:
    streams_of = jax.random.split(jax.random.key(seed), 13)
    patches = gaussian(streams_of[0], (GROUPS * BLOCK, D), 1.0, 6.0, ((0, 16),))
    clip_tokens = plant(jax.random.randint(streams_of[1], (GROUPS,), BLOCK // 16, BLOCK // 4 + 1), jax.random.fold_in(streams_of[1], 1), BLOCK // 16, (BLOCK // 4 + 1) - 1).astype(jnp.int32)
    positions = draw_positions(jax.random.fold_in(streams_of[12], 71), 0)
    norm_gain = jnp.clip(1.0 + 0.1 * jax.random.normal(streams_of[3], (D,), jnp.float32), 0.5, 1.5)
    norm_bias = gaussian(streams_of[4], (D,), 0.5, 3.0, (), jnp.float32)
    w_qkv = draw_w_qkv(jax.random.fold_in(streams_of[12], 71), 0)
    b_qkv = gaussian(streams_of[6], (3, D), 0.5, 3.0, ((1, 2),), jnp.float32)
    w_proj = gaussian(streams_of[7], (D, D), D ** -0.5, 0.15625, ((0, 2),))
    b_proj = gaussian(streams_of[8], (D,), 0.5, 3.0, (), jnp.float32)
    merge_gain = jnp.clip(1.0 + 0.1 * jax.random.normal(streams_of[9], (D,), jnp.float32), 0.5, 1.5)
    merge_bias = gaussian(streams_of[10], (D,), 0.5, 3.0, (), jnp.float32)
    grad_placed = gaussian(streams_of[11], (GROUPS * LEN, 4 * D), ((GROUPS * BLOCK) ** -0.5), 0.09375, ((0, 32),))
    return {"patches": patches, "clip_tokens": clip_tokens, "positions": positions, "norm_gain": norm_gain, "norm_bias": norm_bias, "w_qkv": w_qkv, "b_qkv": b_qkv, "w_proj": w_proj, "b_proj": b_proj, "merge_gain": merge_gain, "merge_bias": merge_bias, "grad_placed": grad_placed}


EPSILON = 1e-06

def lowered(values):
    return lax.optimization_barrier(values.astype(jnp.bfloat16))

def normalize(values, gain_row, bias_row):
    center = values - lax.optimization_barrier(jnp.mean(values, axis=-1, keepdims=True))
    inverse = lax.rsqrt(lax.optimization_barrier(jnp.mean(center * center, axis=-1, keepdims=True)) + EPSILON)
    unit_rows = center * inverse
    return (unit_rows * gain_row + bias_row, unit_rows, inverse)

def normalize_back(upstream, unit_rows, inverse, gain_row):
    scaled = upstream * gain_row
    return inverse * (scaled - lax.optimization_barrier(jnp.mean(scaled, axis=-1, keepdims=True)) - unit_rows * lax.optimization_barrier(jnp.mean(scaled * unit_rows, axis=-1, keepdims=True)))

def one_clip(patch_rows, live_count, places, grad_rows, norm_gain, norm_bias, w_qkv, b_qkv, w_proj, b_proj, merge_gain, merge_bias):
    widened = patch_rows.astype(jnp.float32)
    normed = normalize(widened, norm_gain, norm_bias)[0].astype(jnp.bfloat16)
    triple = jnp.dot(normed, w_qkv.reshape(D, 3 * D), preferred_element_type=jnp.float32).reshape(BLOCK, 3, D) + b_qkv
    triple = lowered(triple)
    query_rows = triple[:, 0].reshape(BLOCK, HEADS, HEAD).astype(jnp.float32)
    key_rows = triple[:, 1].reshape(BLOCK, HEADS, HEAD).astype(jnp.float32)
    value_rows = triple[:, 2].reshape(BLOCK, HEADS, HEAD).astype(jnp.float32)
    scaling = HEAD ** (-0.5)
    scores = jnp.einsum('qhd,khd->hqk', query_rows, key_rows) * scaling
    live_keys = jnp.arange(BLOCK, dtype=jnp.int32) < 4 * live_count
    scores = jnp.where(live_keys[None, None, :], scores, -1e+30)
    highest = lax.optimization_barrier(jnp.max(scores, axis=-1, keepdims=True))
    powers = jnp.exp(scores - highest)
    weights = powers / lax.optimization_barrier(jnp.sum(powers, axis=-1, keepdims=True))
    weights_low = lowered(weights).astype(jnp.float32)
    attended = jnp.einsum('hqk,khd->qhd', weights_low, value_rows).reshape(BLOCK, D).astype(jnp.bfloat16)
    output = jnp.dot(attended, w_proj, preferred_element_type=jnp.float32) + b_proj + widened
    merged_full, unit_rows, inverse = normalize(output, merge_gain, merge_bias)
    merged = merged_full.reshape(BLOCK // 4, 4 * D).astype(jnp.bfloat16)
    live_tokens = jnp.arange(BLOCK // 4, dtype=jnp.int32) < live_count
    window_rows = jnp.arange(LEN, dtype=jnp.int32)
    selector = ((places[None, :] == window_rows[:, None]) & live_tokens[None, :]).astype(jnp.bfloat16)
    placed = jnp.dot(selector, merged, preferred_element_type=jnp.float32).astype(jnp.bfloat16)
    token_grad = jnp.dot(selector.T, grad_rows, preferred_element_type=jnp.float32)
    upstream = token_grad.reshape(BLOCK, D)
    row_grad = normalize_back(upstream, unit_rows, inverse, merge_gain).astype(jnp.bfloat16)
    attn_grad = lowered(jnp.dot(row_grad, w_proj.T, preferred_element_type=jnp.float32))
    attn_grad = attn_grad.reshape(BLOCK, HEADS, HEAD).astype(jnp.float32)
    prob_grad = jnp.einsum('qhd,khd->hqk', attn_grad, value_rows)
    value_grad = jnp.einsum('hqk,qhd->khd', weights_low, attn_grad)
    score_grad = weights * (prob_grad - lax.optimization_barrier(jnp.sum(prob_grad * weights, axis=-1, keepdims=True))) * scaling
    score_grad = lowered(score_grad).astype(jnp.float32)
    query_grad = jnp.einsum('hqk,khd->qhd', score_grad, key_rows)
    key_grad = jnp.einsum('hqk,qhd->khd', score_grad, query_rows)
    triple_grad = jnp.stack([query_grad, key_grad, value_grad], axis=1).reshape(BLOCK, 3 * D).astype(jnp.bfloat16)
    contribution = lax.dot_general(normed, triple_grad, (((0,), (0,)), ((), ())), preferred_element_type=jnp.float32)
    return (placed, contribution)

def reference(patches, clip_tokens, positions, norm_gain, norm_bias, w_qkv, b_qkv, w_proj, b_proj, merge_gain, merge_bias, grad_placed):
    groups = clip_tokens.shape[0]
    clip_rows = patches.reshape(groups, BLOCK, D)
    window_grads = grad_placed.reshape(groups, LEN, 4 * D)

    def advance(running, sliced):
        patch_rows, live_count, places, grad_rows = sliced
        placed, contribution = one_clip(patch_rows, live_count, places, grad_rows, norm_gain, norm_bias, w_qkv, b_qkv, w_proj, b_proj, merge_gain, merge_bias)
        return (running + contribution, placed)
    running, placed = lax.scan(advance, jnp.zeros((D, 3 * D), jnp.float32), (clip_rows, clip_tokens, positions, window_grads))
    placed = placed.reshape(groups * LEN, 4 * D)
    grad_qkv = running.reshape(D, 3, N_SEQ, D // N_SEQ).transpose(2, 1, 3, 0).reshape(N_SEQ, 3 * (D // N_SEQ), D)
    return (placed, grad_qkv)
```

```python
import functools

import jax
import jax.numpy as jnp
from jax import lax
from jax.experimental import pallas as pl
from jax.experimental.pallas import tpu as pltpu
from jax.sharding import PartitionSpec as P

HEAD = 80


EPSILON = 1e-06


def normalize(values, gain_row, bias_row):
    center = values - jnp.mean(values, axis=-1, keepdims=True)
    inverse = lax.rsqrt(jnp.mean(center * center, axis=-1, keepdims=True) + EPSILON)
    unit_rows = center * inverse
    return (unit_rows * gain_row + bias_row, unit_rows, inverse)


def normalize_back(upstream, unit_rows, inverse, gain_row):
    scaled = upstream * gain_row
    return inverse * (
        scaled
        - jnp.mean(scaled, axis=-1, keepdims=True)
        - unit_rows * jnp.mean(scaled * unit_rows, axis=-1, keepdims=True)
    )


def leading(left, right):
    return lax.dot_general(
        left, right, (((0,), (0,)), ((), ())), preferred_element_type=jnp.float32
    )


def trailing(left, right):
    return lax.dot_general(
        left, right, (((1,), (1,)), ((), ())), preferred_element_type=jnp.float32
    )


def general_body(
    patches,
    clip_tokens,
    positions,
    norm_gain,
    norm_bias,
    w_qkv,
    b_qkv,
    w_proj,
    b_proj,
    merge_gain,
    merge_bias,
    grad_placed,
):
    block_rows = patches.shape[0]
    model_width = patches.shape[1]
    local_width = w_qkv.shape[2]
    local_heads = local_width // HEAD
    live_count = clip_tokens[0]
    places = positions[0]
    widened = patches.astype(jnp.float32)
    normed = normalize(widened, norm_gain, norm_bias)[0].astype(jnp.bfloat16)
    triple = jnp.dot(
        normed, w_qkv.reshape(model_width, 3 * local_width), preferred_element_type=jnp.float32
    )
    triple = (triple.reshape(block_rows, 3, local_width) + b_qkv).astype(jnp.bfloat16)
    query_rows = triple[:, 0].reshape(block_rows, local_heads, HEAD)
    key_rows = triple[:, 1].reshape(block_rows, local_heads, HEAD)
    value_rows = triple[:, 2].reshape(block_rows, local_heads, HEAD)
    scaling = HEAD ** (-0.5)
    scores = (
        jnp.einsum("qhd,khd->hqk", query_rows, key_rows, preferred_element_type=jnp.float32)
        * scaling
    )
    live_keys = jnp.arange(block_rows, dtype=jnp.int32) < 4 * live_count
    scores = jnp.where(live_keys[None, None, :], scores, -1e30)
    highest = jnp.max(scores, axis=-1, keepdims=True)
    powers = jnp.exp(scores - highest)
    weights = powers / jnp.sum(powers, axis=-1, keepdims=True)
    weights_low = weights.astype(jnp.bfloat16)
    attended = jnp.einsum(
        "hqk,khd->qhd", weights_low, value_rows, preferred_element_type=jnp.float32
    )
    attended = attended.reshape(block_rows, local_width).astype(jnp.bfloat16)
    partial_value = jnp.dot(attended, w_proj, preferred_element_type=jnp.float32)
    summed_share = lax.psum_scatter(
        partial_value.astype(jnp.bfloat16), "seq", scatter_dimension=0, tiled=True
    ).astype(jnp.float32)
    share_count = summed_share.shape[0]
    own_start = lax.axis_index("seq") * share_count
    own_patches = lax.dynamic_slice_in_dim(widened, own_start, share_count, 0)
    output_share = summed_share + b_proj + own_patches
    output = lax.all_gather(output_share.astype(jnp.bfloat16), "seq", axis=0, tiled=True).astype(
        output_share.dtype
    )
    merged_full, unit_rows, inverse = normalize(output, merge_gain, merge_bias)
    merged = merged_full.reshape(block_rows // 4, 4 * model_width).astype(jnp.bfloat16)
    live_tokens = jnp.arange(block_rows // 4, dtype=jnp.int32) < live_count
    share_rows = grad_placed.shape[0]
    rows_here = lax.axis_index("seq") * share_rows + jnp.arange(share_rows, dtype=jnp.int32)
    selector = ((places[None, :] == rows_here[:, None]) & live_tokens[None, :]).astype(jnp.bfloat16)
    placed = jnp.dot(selector, merged, preferred_element_type=jnp.float32).astype(jnp.bfloat16)
    own_grad = leading(selector, grad_placed)
    token_grad = lax.psum(own_grad.astype(jnp.bfloat16), "seq").astype(jnp.float32)
    upstream = token_grad.reshape(block_rows, model_width)
    row_grad = normalize_back(upstream, unit_rows, inverse, merge_gain).astype(jnp.bfloat16)
    attn_grad = lax.dot_general(
        row_grad, w_proj, (((1,), (1,)), ((), ())), preferred_element_type=jnp.float32
    )
    attn_grad = attn_grad.astype(jnp.bfloat16).reshape(block_rows, local_heads, HEAD)
    prob_grad = jnp.einsum(
        "qhd,khd->hqk", attn_grad, value_rows, preferred_element_type=jnp.float32
    )
    value_grad = jnp.einsum(
        "hqk,qhd->khd", weights_low, attn_grad, preferred_element_type=jnp.float32
    )
    score_grad = (
        weights * (prob_grad - jnp.sum(prob_grad * weights, axis=-1, keepdims=True)) * scaling
    )
    score_grad = score_grad.astype(jnp.bfloat16)
    query_grad = jnp.einsum(
        "hqk,khd->qhd", score_grad, key_rows, preferred_element_type=jnp.float32
    )
    key_grad = jnp.einsum(
        "hqk,qhd->khd", score_grad, query_rows, preferred_element_type=jnp.float32
    )
    triple_grad = jnp.stack([query_grad, key_grad, value_grad], axis=1)
    triple_grad = triple_grad.reshape(block_rows, 3 * local_width).astype(jnp.bfloat16)
    full_term = leading(triple_grad, normed)
    summed = lax.psum_scatter(full_term, "clip", scatter_dimension=0, tiled=True)
    return (placed, summed[None])


def place_masks(rel_row, share_rows, rows):
    window = lax.broadcasted_iota(jnp.int32, (share_rows, rows), 0)
    patch = lax.broadcasted_iota(jnp.int32, (share_rows, rows), 1)
    hit = window == rel_row
    return [
        jnp.where(hit & (lax.rem(patch, 4) == k), 1.0, 0.0).astype(jnp.bfloat16) for k in range(4)
    ]


def pull_kernel(rel_ref, grad_ref, out_ref):
    width = out_ref.shape[1]
    masks = place_masks(rel_ref[...], grad_ref.shape[0], out_ref.shape[0])
    total = None
    for k in range(4):
        term = leading(masks[k], grad_ref[:, k * width : (k + 1) * width])
        total = term if total is None else total + term
    out_ref[...] = total.astype(out_ref.dtype)


def place_kernel(rel_ref, merged_ref, out_ref):
    width = merged_ref.shape[1]
    masks = place_masks(rel_ref[...], out_ref.shape[0], merged_ref.shape[0])
    for k in range(4):
        term = jnp.dot(masks[k], merged_ref[...], preferred_element_type=jnp.float32)
        out_ref[:, k * width : (k + 1) * width] = term.astype(out_ref.dtype)


def forward_kernel(
    live_ref,
    patches_ref,
    gain_ref,
    bias_ref,
    wq_ref,
    wk_ref,
    wv_ref,
    b_ref,
    proj_ref,
    normed_ref,
    triple_ref,
    probs_ref,
    partial_ref,
    attended_ref,
):
    rows = patches_ref.shape[0]
    normed_ref[...] = normalize(
        patches_ref[...].astype(jnp.float32), gain_ref[...], bias_ref[...]
    )[0].astype(jnp.bfloat16)
    for t, w_ref in enumerate((wq_ref, wk_ref, wv_ref)):
        part = jnp.dot(normed_ref[...], w_ref[...], preferred_element_type=jnp.float32)
        triple_ref[t] = (part + b_ref[t : t + 1, :]).astype(jnp.bfloat16)
    live = lax.broadcasted_iota(jnp.int32, (rows, rows), 1) < 4 * live_ref[0]
    scaling = HEAD ** (-0.5)
    for h in range(probs_ref.shape[0]):
        cols = slice(h * HEAD, (h + 1) * HEAD)
        scores = trailing(triple_ref[0, :, cols], triple_ref[1, :, cols]) * scaling
        scores = jnp.where(live, scores, -1e30)
        powers = jnp.exp(scores - jnp.max(scores, axis=-1, keepdims=True))
        weights = (powers / jnp.sum(powers, axis=-1, keepdims=True)).astype(jnp.bfloat16)
        probs_ref[h] = weights
        attended_ref[:, cols] = jnp.dot(
            weights, triple_ref[2, :, cols], preferred_element_type=jnp.float32
        ).astype(jnp.bfloat16)
    partial_ref[...] = jnp.dot(
        attended_ref[...], proj_ref[...], preferred_element_type=jnp.float32
    ).astype(jnp.bfloat16)


def backward_kernel(
    turn_ref,
    own_ref,
    other_ref,
    patches_ref,
    b_ref,
    gain_ref,
    bias_ref,
    up_own_ref,
    up_other_ref,
    proj_ref,
    triple_ref,
    probs_ref,
    merged_ref,
    out0_ref,
    out1_ref,
    out2_ref,
    out3_ref,
    back_ref,
    slots_ref,
):
    output = (
        own_ref[...].astype(jnp.float32)
        + other_ref[...].astype(jnp.float32)
        + b_ref[...]
        + patches_ref[...].astype(jnp.float32)
    )
    merged, unit_rows, inverse = normalize(output, gain_ref[...], bias_ref[...])
    merged_ref[...] = merged.astype(jnp.bfloat16)
    upstream = up_own_ref[...].astype(jnp.float32) + up_other_ref[...].astype(jnp.float32)
    row_grad = normalize_back(upstream, unit_rows, inverse, gain_ref[...]).astype(jnp.bfloat16)
    back_ref[...] = trailing(row_grad, proj_ref[...]).astype(jnp.bfloat16)
    scaling = HEAD ** (-0.5)
    heads = probs_ref.shape[0]
    per_block = slots_ref.shape[2] // HEAD
    turn = turn_ref[0]

    def put(t, h, value):
        piece = t * heads + h
        block, sub = piece // per_block, piece % per_block
        slot = lax.bitwise_xor(turn, block % 4)
        slots_ref[slot, block // 4, sub * HEAD : (sub + 1) * HEAD, :] = value.astype(jnp.bfloat16)

    for h in range(heads):
        cols = slice(h * HEAD, (h + 1) * HEAD)
        back = back_ref[:, cols]
        weights = probs_ref[h]
        put(2, h, leading(back, weights))
        prob_grad = trailing(back, triple_ref[2, :, cols])
        wide = weights.astype(jnp.float32)
        inner = jnp.sum(prob_grad * wide, axis=-1, keepdims=True)
        score_grad = (wide * (prob_grad - inner) * scaling).astype(jnp.bfloat16)
        put(
            0,
            h,
            lax.dot_general(
                triple_ref[1, :, cols],
                score_grad,
                (((0,), (1,)), ((), ())),
                preferred_element_type=jnp.float32,
            ),
        )
        put(1, h, leading(triple_ref[0, :, cols], score_grad))
    for k, out_ref in enumerate((out0_ref, out1_ref, out2_ref, out3_ref)):
        out_ref[...] = slots_ref[k]


def product_kernel(core_ref, t0, t1, t2, t3, n0, n1, n2, n3, keep_ref, send_ref, sum_ref):
    half = keep_ref.shape[1]
    mine = pl.multiple_of(core_ref[0] * half, 8)
    others = pl.multiple_of((1 - core_ref[0]) * half, 8)
    for side in range(2):
        total = None
        for t_ref, n_ref in ((t0, n0), (t1, n1), (t2, n2), (t3, n3)):
            term = jnp.dot(t_ref[side], n_ref[...], preferred_element_type=jnp.float32)
            total = term if total is None else total + term
        sum_ref[...] = total
        keep_ref[side] = sum_ref[pl.ds(mine, half), :]
        send_ref[side] = sum_ref[pl.ds(others, half), :].astype(jnp.bfloat16)


def call(kernel, name, outs, scalars, flops, args, scratch=()):
    vmem = pl.BlockSpec(memory_space=pltpu.VMEM)
    smem = pl.BlockSpec(memory_space=pltpu.SMEM)
    return pl.pallas_call(
        kernel,
        name=name,
        out_shape=outs,
        in_specs=[smem] * scalars + [vmem] * (len(args) - scalars),
        out_specs=jax.tree.map(lambda _: vmem, outs),
        scratch_shapes=list(scratch),
        cost_estimate=pl.CostEstimate(flops=flops, bytes_accessed=4_000_000, transcendentals=0),
        compiler_params=pltpu.CompilerParams(vmem_limit_bytes=56 * 1024 * 1024),
    )(*args)


def fast_body(
    n_clip,
    patches,
    clip_tokens,
    positions,
    norm_gain,
    norm_bias,
    w_qkv,
    b_qkv,
    w_proj,
    b_proj,
    merge_gain,
    merge_bias,
    grad_placed,
):
    rows, width = patches.shape
    local = w_qkv.shape[2]
    heads = local // HEAD
    share_rows = grad_placed.shape[0]
    low = jnp.bfloat16
    shape = jax.ShapeDtypeStruct
    me = lax.axis_index("clip")
    live_count = clip_tokens[0]
    tokens = jnp.arange(rows, dtype=jnp.int32) // 4
    spread = jnp.repeat(positions[0], rows // positions.shape[1])
    rel = jnp.where(tokens < live_count, spread - lax.axis_index("seq") * share_rows, -1)[None]

    def swap(value):
        return lax.ppermute(value, "seq", [(0, 1), (1, 0)])

    def flip(value, bits):
        return lax.ppermute(value, "clip", [(i, i ^ bits) for i in range(n_clip)])

    up_own = call(
        pull_kernel,
        "pull",
        shape((rows, width), low),
        0,
        8 * rows * share_rows * width,
        (rel, grad_placed),
    )
    up_other = swap(up_own)
    row = lambda v: v[None]
    normed, triple, probs, partial = call(
        forward_kernel,
        "forward",
        (
            shape((rows, width), low),
            shape((3, rows, local), low),
            shape((heads, rows, rows), low),
            shape((rows, width), low),
        ),
        1,
        8 * rows * width * local,
        (
            clip_tokens,
            patches,
            row(norm_gain),
            row(norm_bias),
            w_qkv[:, 0],
            w_qkv[:, 1],
            w_qkv[:, 2],
            b_qkv,
            w_proj,
        ),
        (pltpu.VMEM((rows, local), low),),
    )
    other = swap(partial)
    normed_of = [normed] + [flip(normed, q << 1) for q in (1, 2, 3)]
    block = 3 * local // 8
    merged, *sent = call(
        backward_kernel,
        "backward",
        (shape((rows, width), low),) + (shape((2, block, rows), low),) * 4,
        1,
        6 * rows * width * local,
        (
            jnp.reshape((me >> 1) & 3, (1,)),
            partial,
            other,
            patches,
            row(b_proj),
            row(merge_gain),
            row(merge_bias),
            up_own,
            up_other,
            w_proj,
            triple,
            probs,
        ),
        (pltpu.VMEM((rows, local), low), pltpu.VMEM((4, 2, block, rows), low)),
    )
    taken = [sent[0]] + [flip(sent[q], q << 1) for q in (1, 2, 3)]
    placed = call(
        place_kernel,
        "place",
        shape((share_rows, 4 * width), low),
        0,
        8 * rows * share_rows * width,
        (rel, merged),
    )
    keep, send = call(
        product_kernel,
        "product",
        (shape((2, block // 2, width), jnp.float32), shape((2, block // 2, width), low)),
        1,
        16 * block * rows * width,
        (jnp.reshape(me & 1, (1,)), *taken, *normed_of),
        (pltpu.VMEM((block, width), jnp.float32),),
    )
    pair = keep + flip(send, 1).astype(jnp.float32)
    side = me >> 3
    mine = lax.dynamic_index_in_dim(pair, side, 0, keepdims=False)
    theirs = lax.dynamic_index_in_dim(pair, 1 - side, 0, keepdims=False)
    summed = mine + flip(theirs.astype(low), 8).astype(jnp.float32)
    return (placed, summed[None])


def solution(mesh):
    n_clip, n_seq = mesh.shape["clip"], mesh.shape["seq"]
    body = general_body
    if n_clip == 2 * 4 * 2 and n_seq == 2:
        body = functools.partial(fast_body, n_clip)
    return jax.shard_map(
        body,
        mesh=mesh,
        in_specs=(
            P("clip", None),
            P("clip"),
            P("clip", None),
            P(),
            P(),
            P(None, None, "seq"),
            P(None, "seq"),
            P("seq", None),
            P(),
            P(),
            P(),
            P(("clip", "seq"), None),
        ),
        out_specs=(P(("clip", "seq"), None), P("seq", "clip", None)),
        check_vma=False,
    )
```

```python
import functools

import jax
import jax.numpy as jnp
from jax import lax
from jax.experimental import pallas as pl
from jax.experimental.pallas import tpu as pltpu
from jax.sharding import PartitionSpec as P


HEAD = 80


EPSILON = 1e-06


def normalize(values, gain_row, bias_row):
    center = values - jnp.mean(values, axis=-1, keepdims=True)
    inverse = lax.rsqrt(jnp.mean(center * center, axis=-1, keepdims=True) + EPSILON)
    unit_rows = center * inverse
    return (unit_rows * gain_row + bias_row, unit_rows, inverse)


def normalize_back(upstream, unit_rows, inverse, gain_row):
    scaled = upstream * gain_row
    return inverse * (
        scaled
        - jnp.mean(scaled, axis=-1, keepdims=True)
        - unit_rows * jnp.mean(scaled * unit_rows, axis=-1, keepdims=True)
    )


def leading(left, right):
    return lax.dot_general(
        left, right, (((0,), (0,)), ((), ())), preferred_element_type=jnp.float32
    )


def trailing(left, right):
    return lax.dot_general(
        left, right, (((1,), (1,)), ((), ())), preferred_element_type=jnp.float32
    )


def general_body(
    patches,
    clip_tokens,
    positions,
    norm_gain,
    norm_bias,
    w_qkv,
    b_qkv,
    w_proj,
    b_proj,
    merge_gain,
    merge_bias,
    grad_placed,
):
    block_rows = patches.shape[0]
    model_width = patches.shape[1]
    local_width = w_qkv.shape[2]
    local_heads = local_width // HEAD
    live_count = clip_tokens[0]
    places = positions[0]
    widened = patches.astype(jnp.float32)
    normed = normalize(widened, norm_gain, norm_bias)[0].astype(jnp.bfloat16)
    triple = jnp.dot(
        normed, w_qkv.reshape(model_width, 3 * local_width), preferred_element_type=jnp.float32
    )
    triple = (triple.reshape(block_rows, 3, local_width) + b_qkv).astype(jnp.bfloat16)
    query_rows = triple[:, 0].reshape(block_rows, local_heads, HEAD)
    key_rows = triple[:, 1].reshape(block_rows, local_heads, HEAD)
    value_rows = triple[:, 2].reshape(block_rows, local_heads, HEAD)
    scaling = HEAD ** (-0.5)
    scores = (
        jnp.einsum("qhd,khd->hqk", query_rows, key_rows, preferred_element_type=jnp.float32)
        * scaling
    )
    live_keys = jnp.arange(block_rows, dtype=jnp.int32) < 4 * live_count
    scores = jnp.where(live_keys[None, None, :], scores, -1e30)
    highest = jnp.max(scores, axis=-1, keepdims=True)
    powers = jnp.exp(scores - highest)
    weights = powers / jnp.sum(powers, axis=-1, keepdims=True)
    weights_low = weights.astype(jnp.bfloat16)
    attended = jnp.einsum(
        "hqk,khd->qhd", weights_low, value_rows, preferred_element_type=jnp.float32
    )
    attended = attended.reshape(block_rows, local_width).astype(jnp.bfloat16)
    partial_value = jnp.dot(attended, w_proj, preferred_element_type=jnp.float32)
    summed_share = lax.psum_scatter(
        partial_value.astype(jnp.bfloat16), "seq", scatter_dimension=0, tiled=True
    ).astype(jnp.float32)
    share_count = summed_share.shape[0]
    own_start = lax.axis_index("seq") * share_count
    own_patches = lax.dynamic_slice_in_dim(widened, own_start, share_count, 0)
    output_share = summed_share + b_proj + own_patches
    output = lax.all_gather(output_share.astype(jnp.bfloat16), "seq", axis=0, tiled=True).astype(
        output_share.dtype
    )
    merged_full, unit_rows, inverse = normalize(output, merge_gain, merge_bias)
    merged = merged_full.reshape(block_rows // 4, 4 * model_width).astype(jnp.bfloat16)
    live_tokens = jnp.arange(block_rows // 4, dtype=jnp.int32) < live_count
    share_rows = grad_placed.shape[0]
    rows_here = lax.axis_index("seq") * share_rows + jnp.arange(share_rows, dtype=jnp.int32)
    selector = ((places[None, :] == rows_here[:, None]) & live_tokens[None, :]).astype(jnp.bfloat16)
    placed = jnp.dot(selector, merged, preferred_element_type=jnp.float32).astype(jnp.bfloat16)
    own_grad = leading(selector, grad_placed)
    token_grad = lax.psum(own_grad.astype(jnp.bfloat16), "seq").astype(jnp.float32)
    upstream = token_grad.reshape(block_rows, model_width)
    row_grad = normalize_back(upstream, unit_rows, inverse, merge_gain).astype(jnp.bfloat16)
    attn_grad = lax.dot_general(
        row_grad, w_proj, (((1,), (1,)), ((), ())), preferred_element_type=jnp.float32
    )
    attn_grad = attn_grad.astype(jnp.bfloat16).reshape(block_rows, local_heads, HEAD)
    prob_grad = jnp.einsum(
        "qhd,khd->hqk", attn_grad, value_rows, preferred_element_type=jnp.float32
    )
    value_grad = jnp.einsum(
        "hqk,qhd->khd", weights_low, attn_grad, preferred_element_type=jnp.float32
    )
    score_grad = (
        weights * (prob_grad - jnp.sum(prob_grad * weights, axis=-1, keepdims=True)) * scaling
    )
    score_grad = score_grad.astype(jnp.bfloat16)
    query_grad = jnp.einsum(
        "hqk,khd->qhd", score_grad, key_rows, preferred_element_type=jnp.float32
    )
    key_grad = jnp.einsum(
        "hqk,qhd->khd", score_grad, query_rows, preferred_element_type=jnp.float32
    )
    triple_grad = jnp.stack([query_grad, key_grad, value_grad], axis=1)
    triple_grad = triple_grad.reshape(block_rows, 3 * local_width).astype(jnp.bfloat16)
    full_term = leading(triple_grad, normed)
    summed = lax.psum_scatter(full_term, "clip", scatter_dimension=0, tiled=True)
    return (placed, summed[None])


def place_masks(live_ref, places_ref, share_rows, rows):
    tokens = places_ref.shape[1]
    token = lax.broadcasted_iota(jnp.int32, (tokens, rows), 0)
    owner = lax.broadcasted_iota(jnp.int32, (tokens, rows), 1) // 4
    spread = jnp.where((token == owner) & (token < live_ref[0]), 1.0, 0.0)
    shifted = jnp.broadcast_to(places_ref[...].astype(jnp.float32) + 1.0, (8, tokens))
    row = jnp.dot(shifted, spread, precision=lax.Precision.HIGHEST)[:1] - 1.0
    first = lax.axis_index("seq") * share_rows
    window = lax.broadcasted_iota(jnp.int32, (share_rows, rows), 0) + first
    patch = lax.broadcasted_iota(jnp.int32, (share_rows, rows), 1)
    hit = window.astype(jnp.float32) == row
    return [
        jnp.where(hit & (lax.rem(patch, 4) == k), 1.0, 0.0).astype(jnp.bfloat16) for k in range(4)
    ]


def pull_kernel(live_ref, places_ref, grad_ref, out_ref):
    width = out_ref.shape[1]
    masks = place_masks(live_ref, places_ref, grad_ref.shape[0], out_ref.shape[0])
    total = None
    for k in range(4):
        term = leading(masks[k], grad_ref[:, k * width : (k + 1) * width])
        total = term if total is None else total + term
    out_ref[...] = total.astype(out_ref.dtype)


def place_kernel(live_ref, places_ref, merged_ref, _, out_ref):
    width = merged_ref.shape[1]
    masks = place_masks(live_ref, places_ref, out_ref.shape[0], merged_ref.shape[0])
    for k in range(4):
        term = jnp.dot(masks[k], merged_ref[...], preferred_element_type=jnp.float32)
        out_ref[:, k * width : (k + 1) * width] = term.astype(out_ref.dtype)


def begin(sources, targets, sems, first=0):
    copies = [
        pltpu.make_async_copy(source, target, sems.at[first + k])
        for k, (source, target) in enumerate(zip(sources, targets, strict=True))
    ]
    for copy in copies:
        copy.start()
    return copies


def forward_kernel(
    live_ref,
    gain_ref,
    bias_ref,
    b_ref,
    patches_hbm,
    w_hbm,
    proj_hbm,
    normed_ref,
    triple_ref,
    probs_ref,
    partial_ref,
    patches_ref,
    w_ref,
    proj_ref,
    attended_ref,
    sems,
):
    rows = patches_ref.shape[0]
    came = begin(
        (patches_hbm, w_hbm.at[0], w_hbm.at[1], w_hbm.at[2], proj_hbm),
        (patches_ref, w_ref.at[0], w_ref.at[1], w_ref.at[2], proj_ref),
        sems,
    )
    came[0].wait()
    normed_ref[...] = normalize(
        patches_ref[...].astype(jnp.float32), gain_ref[...][None, :], bias_ref[...][None, :]
    )[0].astype(jnp.bfloat16)
    for t in range(3):
        came[1 + t].wait()
        part = jnp.dot(normed_ref[...], w_ref[t], preferred_element_type=jnp.float32)
        triple_ref[t] = (part + b_ref[t : t + 1, :]).astype(jnp.bfloat16)
    live = lax.broadcasted_iota(jnp.int32, (rows, rows), 1) < 4 * live_ref[0]
    steep = HEAD ** (-0.5) * 1.4426950408889634
    for h in range(probs_ref.shape[0]):
        cols = slice(h * HEAD, (h + 1) * HEAD)
        scores = trailing(triple_ref[0, :, cols], triple_ref[1, :, cols])
        scores = jnp.where(live, scores, -1e30)
        powers = jnp.exp2((scores - jnp.max(scores, axis=-1, keepdims=True)) * steep)
        weights = powers * (1.0 / jnp.sum(powers, axis=-1, keepdims=True))
        weights = weights.astype(jnp.bfloat16)
        probs_ref[h] = weights
        attended_ref[:, cols] = jnp.dot(
            weights, triple_ref[2, :, cols], preferred_element_type=jnp.float32
        ).astype(jnp.bfloat16)
    came[4].wait()
    partial_ref[...] = jnp.dot(
        attended_ref[...], proj_ref[...], preferred_element_type=jnp.float32
    ).astype(jnp.bfloat16)


def backward_kernel(
    b_ref,
    gain_ref,
    bias_ref,
    own_ref,
    other_ref,
    patches_ref,
    up_own_ref,
    up_other_ref,
    proj_ref,
    triple_ref,
    probs_ref,
    merged_ref,
    *refs,
):
    outs, (back_ref, slots_ref) = refs[:8], refs[8:]
    gain = gain_ref[...][None, :]
    output = (
        own_ref[...].astype(jnp.float32)
        + other_ref[...].astype(jnp.float32)
        + b_ref[...][None, :]
        + patches_ref[...].astype(jnp.float32)
    )
    merged, unit_rows, inverse = normalize(output, gain, bias_ref[...][None, :])
    merged_ref[...] = merged.astype(jnp.bfloat16)
    upstream = up_own_ref[...].astype(jnp.float32) + up_other_ref[...].astype(jnp.float32)
    row_grad = normalize_back(upstream, unit_rows, inverse, gain).astype(jnp.bfloat16)
    back_ref[...] = trailing(row_grad, proj_ref[...]).astype(jnp.bfloat16)
    scaling = HEAD ** (-0.5)
    heads = probs_ref.shape[0]
    per_block = slots_ref.shape[2] // HEAD
    me = lax.axis_index("clip")
    turn = lax.bitwise_and(lax.shift_right_logical(me, 1), 3)
    away = 1 - lax.shift_right_logical(me, 3)

    def put(t, h, value):
        piece = t * heads + h
        block, sub = piece // per_block, piece % per_block
        slot = lax.bitwise_xor(turn, block % 4)
        side = lax.bitwise_xor(away, block // 4)
        slots_ref[side, slot, sub * HEAD : (sub + 1) * HEAD, :] = value.astype(jnp.bfloat16)

    for h in range(heads):
        cols = slice(h * HEAD, (h + 1) * HEAD)
        back = back_ref[:, cols]
        weights = probs_ref[h]
        put(2, h, leading(back, weights))
        prob_grad = trailing(back, triple_ref[2, :, cols])
        wide = weights.astype(jnp.float32)
        inner = jnp.sum(prob_grad * wide, axis=-1, keepdims=True)
        score_grad = (wide * (prob_grad - inner)).astype(jnp.bfloat16)
        query_grad = lax.dot_general(
            triple_ref[1, :, cols],
            score_grad,
            (((0,), (1,)), ((), ())),
            preferred_element_type=jnp.float32,
        )
        put(0, h, query_grad * scaling)
        put(1, h, leading(triple_ref[0, :, cols], score_grad) * scaling)
    for k, out_ref in enumerate(outs):
        out_ref[...] = slots_ref[k // 4, k % 4]


def product_kernel(*refs):
    t_refs, n_refs = refs[:4], refs[4:8]
    keep_ref, send_ref, sum_ref = refs[-3:]
    half = keep_ref.shape[0]
    core = lax.bitwise_and(lax.axis_index("clip"), 1)
    total = None
    for t_ref, n_ref in zip(t_refs, n_refs, strict=True):
        term = jnp.dot(t_ref[...], n_ref[...], preferred_element_type=jnp.float32)
        total = term if total is None else total + term
    sum_ref[...] = total
    keep_ref[...] = sum_ref[pl.ds(pl.multiple_of(core * half, 8), half), :]
    other = sum_ref[pl.ds(pl.multiple_of((1 - core) * half, 8), half), :]
    send_ref[...] = other.astype(jnp.bfloat16)


def call(kernel, outs, kinds, flops, args, scratch=(), limit=30):
    spec = {
        "s": pl.BlockSpec(memory_space=pltpu.SMEM),
        "v": pl.BlockSpec(memory_space=pltpu.VMEM),
        "a": pl.BlockSpec(memory_space=pl.ANY),
    }
    return pl.pallas_call(
        kernel,
        out_shape=outs,
        in_specs=[spec[kind] for kind in kinds],
        out_specs=jax.tree.map(lambda _: spec["v"], outs),
        scratch_shapes=list(scratch),
        cost_estimate=pl.CostEstimate(flops=flops, bytes_accessed=4_000_000, transcendentals=0),
        compiler_params=pltpu.CompilerParams(vmem_limit_bytes=limit * 1024 * 1024),
    )(*args)


def fast_body(
    n_clip,
    patches,
    clip_tokens,
    positions,
    norm_gain,
    norm_bias,
    w_qkv,
    b_qkv,
    w_proj,
    b_proj,
    merge_gain,
    merge_bias,
    grad_placed,
):
    rows, width = patches.shape
    local = w_qkv.shape[2]
    heads = local // HEAD
    share_rows = grad_placed.shape[0]
    low = jnp.bfloat16
    shape = jax.ShapeDtypeStruct
    full = shape((rows, width), low)

    def swap(value):
        return lax.ppermute(value, "seq", [(0, 1), (1, 0)])

    def flip(value, bits):
        return lax.ppermute(value, "clip", [(i, i ^ bits) for i in range(n_clip)])

    up_own = call(
        pull_kernel,
        full,
        "svv",
        8 * rows * share_rows * width,
        (clip_tokens, positions, grad_placed),
    )
    up_other = swap(up_own)
    normed, triple, probs, partial = call(
        forward_kernel,
        (full, shape((3, rows, local), low), shape((heads, rows, rows), low), full),
        "svvvaaa",
        8 * rows * width * local,
        (
            clip_tokens,
            norm_gain,
            norm_bias,
            b_qkv,
            patches,
            jnp.transpose(w_qkv, (1, 0, 2)),
            w_proj,
        ),
        (
            pltpu.VMEM((rows, width), low),
            pltpu.VMEM((3, width, local), low),
            pltpu.VMEM((local, width), low),
            pltpu.VMEM((rows, local), low),
            pltpu.SemaphoreType.DMA((5,)),
        ),
        limit=52,
    )
    other = swap(partial)
    normed_of = [normed] + [flip(normed, q << 1) for q in (1, 2, 3)]
    block = 3 * local // 8
    merged, *sent = call(
        backward_kernel,
        (full,) + (shape((block, rows), low),) * 8,
        "v" * 11,
        6 * rows * width * local,
        (
            b_proj,
            merge_gain,
            merge_bias,
            partial,
            other,
            patches,
            up_own,
            up_other,
            w_proj,
            triple,
            probs,
        ),
        (pltpu.VMEM((rows, local), low), pltpu.VMEM((2, 4, block, rows), low)),
    )

    def exchange(sent):
        return [sent[0]] + [flip(sent[q], q << 1) for q in (1, 2, 3)]

    def product(taken, after=()):
        return call(
            product_kernel,
            (shape((block // 2, width), jnp.float32), shape((block // 2, width), low)),
            "v" * 8 + "a" * len(after),
            8 * block * rows * width,
            (*taken, *normed_of, *after),
            (pltpu.VMEM((block, width), jnp.float32),),
        )

    far_taken = exchange(sent[:4])
    near_taken = exchange(sent[4:])
    far_keep, far_send = product(far_taken)
    far_came = flip(far_send, 1)
    far_sum = (far_keep + far_came.astype(jnp.float32)).astype(low)
    crossing = flip(far_sum, 8)
    near_keep, near_send = product(near_taken, (far_sum,))
    near_came = flip(near_send, 1)
    placed = call(
        place_kernel,
        shape((share_rows, 4 * width), low),
        "svva",
        8 * rows * share_rows * width,
        (clip_tokens, positions, merged, far_sum),
    )
    summed = near_keep + near_came.astype(jnp.float32) + crossing.astype(jnp.float32)
    return (placed, summed[None])


def solution(mesh):
    n_clip, n_seq = mesh.shape["clip"], mesh.shape["seq"]
    fast = n_clip == 2 * 4 * 2 and n_seq == 2
    body = functools.partial(fast_body, n_clip) if fast else general_body
    return jax.shard_map(
        body,
        mesh=mesh,
        in_specs=(
            P("clip", None),
            P("clip"),
            P("clip", None),
            P(),
            P(),
            P(None, None, "seq"),
            P(None, "seq"),
            P("seq", None),
            P(),
            P(),
            P(),
            P(("clip", "seq"), None),
        ),
        out_specs=(P(("clip", "seq"), None), P("seq", "clip", None)),
        check_vma=False,
    )
```

```python
import functools

import jax
import jax.numpy as jnp
from jax import lax
from jax.experimental import pallas as pl
from jax.experimental.pallas import tpu as pltpu
from jax.sharding import PartitionSpec as P


HEAD = 80


EPSILON = 1e-06


def normalize(values, gain_row, bias_row):
    center = values - jnp.mean(values, axis=-1, keepdims=True)
    inverse = lax.rsqrt(jnp.mean(center * center, axis=-1, keepdims=True) + EPSILON)
    unit_rows = center * inverse
    return (unit_rows * gain_row + bias_row, unit_rows, inverse)


def normalize_back(upstream, unit_rows, inverse, gain_row):
    scaled = upstream * gain_row
    return inverse * (
        scaled
        - jnp.mean(scaled, axis=-1, keepdims=True)
        - unit_rows * jnp.mean(scaled * unit_rows, axis=-1, keepdims=True)
    )


def leading(left, right):
    return lax.dot_general(
        left, right, (((0,), (0,)), ((), ())), preferred_element_type=jnp.float32
    )


def trailing(left, right):
    return lax.dot_general(
        left, right, (((1,), (1,)), ((), ())), preferred_element_type=jnp.float32
    )


def general_body(
    patches,
    clip_tokens,
    positions,
    norm_gain,
    norm_bias,
    w_qkv,
    b_qkv,
    w_proj,
    b_proj,
    merge_gain,
    merge_bias,
    grad_placed,
):
    block_rows = patches.shape[0]
    model_width = patches.shape[1]
    local_width = w_qkv.shape[2]
    local_heads = local_width // HEAD
    live_count = clip_tokens[0]
    places = positions[0]
    widened = patches.astype(jnp.float32)
    normed = normalize(widened, norm_gain, norm_bias)[0].astype(jnp.bfloat16)
    triple = jnp.dot(
        normed, w_qkv.reshape(model_width, 3 * local_width), preferred_element_type=jnp.float32
    )
    triple = (triple.reshape(block_rows, 3, local_width) + b_qkv).astype(jnp.bfloat16)
    query_rows = triple[:, 0].reshape(block_rows, local_heads, HEAD)
    key_rows = triple[:, 1].reshape(block_rows, local_heads, HEAD)
    value_rows = triple[:, 2].reshape(block_rows, local_heads, HEAD)
    scaling = HEAD ** (-0.5)
    scores = (
        jnp.einsum("qhd,khd->hqk", query_rows, key_rows, preferred_element_type=jnp.float32)
        * scaling
    )
    live_keys = jnp.arange(block_rows, dtype=jnp.int32) < 4 * live_count
    scores = jnp.where(live_keys[None, None, :], scores, -1e30)
    highest = jnp.max(scores, axis=-1, keepdims=True)
    powers = jnp.exp(scores - highest)
    weights = powers / jnp.sum(powers, axis=-1, keepdims=True)
    weights_low = weights.astype(jnp.bfloat16)
    attended = jnp.einsum(
        "hqk,khd->qhd", weights_low, value_rows, preferred_element_type=jnp.float32
    )
    attended = attended.reshape(block_rows, local_width).astype(jnp.bfloat16)
    partial_value = jnp.dot(attended, w_proj, preferred_element_type=jnp.float32)
    summed_share = lax.psum_scatter(
        partial_value.astype(jnp.bfloat16), "seq", scatter_dimension=0, tiled=True
    ).astype(jnp.float32)
    share_count = summed_share.shape[0]
    own_start = lax.axis_index("seq") * share_count
    own_patches = lax.dynamic_slice_in_dim(widened, own_start, share_count, 0)
    output_share = summed_share + b_proj + own_patches
    output = lax.all_gather(output_share.astype(jnp.bfloat16), "seq", axis=0, tiled=True).astype(
        output_share.dtype
    )
    merged_full, unit_rows, inverse = normalize(output, merge_gain, merge_bias)
    merged = merged_full.reshape(block_rows // 4, 4 * model_width).astype(jnp.bfloat16)
    live_tokens = jnp.arange(block_rows // 4, dtype=jnp.int32) < live_count
    share_rows = grad_placed.shape[0]
    rows_here = lax.axis_index("seq") * share_rows + jnp.arange(share_rows, dtype=jnp.int32)
    selector = ((places[None, :] == rows_here[:, None]) & live_tokens[None, :]).astype(jnp.bfloat16)
    placed = jnp.dot(selector, merged, preferred_element_type=jnp.float32).astype(jnp.bfloat16)
    own_grad = leading(selector, grad_placed)
    token_grad = lax.psum(own_grad.astype(jnp.bfloat16), "seq").astype(jnp.float32)
    upstream = token_grad.reshape(block_rows, model_width)
    row_grad = normalize_back(upstream, unit_rows, inverse, merge_gain).astype(jnp.bfloat16)
    attn_grad = lax.dot_general(
        row_grad, w_proj, (((1,), (1,)), ((), ())), preferred_element_type=jnp.float32
    )
    attn_grad = attn_grad.astype(jnp.bfloat16).reshape(block_rows, local_heads, HEAD)
    prob_grad = jnp.einsum(
        "qhd,khd->hqk", attn_grad, value_rows, preferred_element_type=jnp.float32
    )
    value_grad = jnp.einsum(
        "hqk,qhd->khd", weights_low, attn_grad, preferred_element_type=jnp.float32
    )
    score_grad = (
        weights * (prob_grad - jnp.sum(prob_grad * weights, axis=-1, keepdims=True)) * scaling
    )
    score_grad = score_grad.astype(jnp.bfloat16)
    query_grad = jnp.einsum(
        "hqk,khd->qhd", score_grad, key_rows, preferred_element_type=jnp.float32
    )
    key_grad = jnp.einsum(
        "hqk,qhd->khd", score_grad, query_rows, preferred_element_type=jnp.float32
    )
    triple_grad = jnp.stack([query_grad, key_grad, value_grad], axis=1)
    triple_grad = triple_grad.reshape(block_rows, 3 * local_width).astype(jnp.bfloat16)
    full_term = leading(triple_grad, normed)
    summed = lax.psum_scatter(full_term, "clip", scatter_dimension=0, tiled=True)
    return (placed, summed[None])


def place_masks(live_ref, places, share_rows, rows, first_row):
    tokens = places.shape[1]
    token = lax.broadcasted_iota(jnp.int32, (tokens, rows), 0)
    owner = (lax.broadcasted_iota(jnp.int32, (tokens, rows), 1) + first_row) // 4
    spread = jnp.where((token == owner) & (token < live_ref[0]), 1.0, 0.0)
    shifted = jnp.broadcast_to(places.astype(jnp.float32) + 1.0, (8, tokens))
    row = jnp.dot(shifted, spread, precision=lax.Precision.HIGHEST)[:1] - 1.0
    first = lax.axis_index("seq") * share_rows
    window = lax.broadcasted_iota(jnp.int32, (share_rows, rows), 0) + first
    patch = lax.broadcasted_iota(jnp.int32, (share_rows, rows), 1)
    hit = window.astype(jnp.float32) == row
    return [
        jnp.where(hit & (lax.rem(patch, 4) == k), 1.0, 0.0).astype(jnp.bfloat16) for k in range(4)
    ]


def begin(sources, targets, sems, first=0):
    copies = [
        pltpu.make_async_copy(source, target, sems.at[first + k])
        for k, (source, target) in enumerate(zip(sources, targets, strict=True))
    ]
    for copy in copies:
        copy.start()
    return copies


def half_start(half, own):
    seq = lax.axis_index("seq")
    return pl.multiple_of((seq if own else 1 - seq) * half, 128)


def prepare_kernel(
    live_ref,
    gain_ref,
    bias_ref,
    patches_hbm,
    places_hbm,
    grad_hbm,
    normed_ref,
    keep_ref,
    send_ref,
    patches_ref,
    places_ref,
    grad_ref,
    sems,
):
    width = send_ref.shape[1]
    half = send_ref.shape[0]
    came = begin((patches_hbm, places_hbm, grad_hbm), (patches_ref, places_ref, grad_ref), sems)
    came[0].wait()
    normed_ref[...] = normalize(
        patches_ref[...].astype(jnp.float32), gain_ref[...][None, :], bias_ref[...][None, :]
    )[0].astype(jnp.bfloat16)
    came[1].wait()
    came[2].wait()
    for out_ref, own in ((send_ref, False), (keep_ref, True)):
        masks = place_masks(
            live_ref, places_ref[...], grad_ref.shape[0], half, half_start(half, own)
        )
        total = None
        for k in range(4):
            term = leading(masks[k], grad_ref[:, k * width : (k + 1) * width])
            total = term if total is None else total + term
        out_ref[...] = total.astype(out_ref.dtype)


def place_kernel(live_ref, places_ref, own_ref, other_ref, _, out_ref):
    half, width = own_ref.shape
    share_rows = out_ref.shape[0]
    own = place_masks(live_ref, places_ref[...], share_rows, half, half_start(half, True))
    other = place_masks(live_ref, places_ref[...], share_rows, half, half_start(half, False))
    for k in range(4):
        term = jnp.dot(own[k], own_ref[...], preferred_element_type=jnp.float32)
        term += jnp.dot(other[k], other_ref[...], preferred_element_type=jnp.float32)
        out_ref[:, k * width : (k + 1) * width] = term.astype(out_ref.dtype)


def attend(live_ref, triple_ref, start, probs_ref, attended_ref):
    half, rows = probs_ref.shape[1:]
    live = lax.broadcasted_iota(jnp.int32, (half, rows), 1) < 4 * live_ref[0]
    steep = HEAD ** (-0.5) * 1.4426950408889634
    for h in range(probs_ref.shape[0]):
        cols = slice(h * HEAD, (h + 1) * HEAD)
        scores = trailing(triple_ref[0, pl.ds(start, half), cols], triple_ref[1, :, cols])
        scores = jnp.where(live, scores, -1e30)
        powers = jnp.exp2((scores - jnp.max(scores, axis=-1, keepdims=True)) * steep)
        weights = powers * (1.0 / jnp.sum(powers, axis=-1, keepdims=True))
        weights = weights.astype(jnp.bfloat16)
        probs_ref[h] = weights
        attended_ref[:, cols] = jnp.dot(
            weights, triple_ref[2, :, cols], preferred_element_type=jnp.float32
        ).astype(jnp.bfloat16)


def first_kernel(
    live_ref,
    b_ref,
    normed_hbm,
    w_hbm,
    proj_hbm,
    triple_ref,
    probs_ref,
    send_ref,
    normed_ref,
    w_ref,
    proj_ref,
    attended_ref,
    sems,
):
    came = begin(
        (normed_hbm, w_hbm.at[0], w_hbm.at[1], w_hbm.at[2], proj_hbm),
        (normed_ref, w_ref.at[0], w_ref.at[1], w_ref.at[2], proj_ref),
        sems,
    )
    came[0].wait()
    for t in range(3):
        came[1 + t].wait()
        part = jnp.dot(normed_ref[...], w_ref[t], preferred_element_type=jnp.float32)
        triple_ref[t] = (part + b_ref[t : t + 1, :]).astype(jnp.bfloat16)
    start = half_start(send_ref.shape[0], False)
    attend(live_ref, triple_ref, start, probs_ref, attended_ref)
    came[4].wait()
    send_ref[...] = jnp.dot(
        attended_ref[...], proj_ref[...], preferred_element_type=jnp.float32
    ).astype(jnp.bfloat16)


def second_kernel(live_ref, triple_ref, proj_ref, probs_ref, keep_ref, attended_ref):
    start = half_start(keep_ref.shape[0], True)
    attend(live_ref, triple_ref, start, probs_ref, attended_ref)
    keep_ref[...] = jnp.dot(attended_ref[...], proj_ref[...], preferred_element_type=jnp.float32)


def middle_kernel(
    b_ref,
    gain_ref,
    bias_ref,
    keep_ref,
    came_ref,
    patches_ref,
    up_keep_ref,
    up_came_ref,
    merged_ref,
    back_ref,
):
    half = keep_ref.shape[0]
    gain = gain_ref[...][None, :]
    output = (
        keep_ref[...]
        + came_ref[...].astype(jnp.float32)
        + b_ref[...][None, :]
        + patches_ref[pl.ds(half_start(half, True), half), :].astype(jnp.float32)
    )
    merged, unit_rows, inverse = normalize(output, gain, bias_ref[...][None, :])
    merged_ref[...] = merged.astype(jnp.bfloat16)
    upstream = up_keep_ref[...].astype(jnp.float32) + up_came_ref[...].astype(jnp.float32)
    back_ref[...] = normalize_back(upstream, unit_rows, inverse, gain).astype(jnp.bfloat16)


def attend_back(row_ref, proj_ref, triple_ref, probs_ref, back_ref, start, put):
    half = row_ref.shape[0]
    back_ref[...] = trailing(row_ref[...], proj_ref[...]).astype(jnp.bfloat16)
    scaling = HEAD ** (-0.5)
    for h in range(probs_ref.shape[0]):
        cols = slice(h * HEAD, (h + 1) * HEAD)
        back = back_ref[:, cols]
        weights = probs_ref[h]
        prob_grad = trailing(back, triple_ref[2, :, cols])
        wide = weights.astype(jnp.float32)
        inner = jnp.sum(prob_grad * wide, axis=-1, keepdims=True)
        score_grad = (wide * (prob_grad - inner)).astype(jnp.bfloat16)
        query_grad = lax.dot_general(
            triple_ref[1, :, cols],
            score_grad,
            (((0,), (1,)), ((), ())),
            preferred_element_type=jnp.float32,
        )
        key_grad = leading(triple_ref[0, pl.ds(start, half), cols], score_grad)
        put(h, query_grad * scaling, key_grad * scaling, leading(back, weights))


def own_back_kernel(
    row_ref, proj_ref, triple_ref, probs_ref, query_ref, key_ref, value_ref, back_ref
):
    def put(h, query_grad, key_grad, value_grad):
        rows = slice(h * HEAD, (h + 1) * HEAD)
        query_ref[rows, :] = query_grad.astype(jnp.bfloat16)
        key_ref[rows, :] = key_grad
        value_ref[rows, :] = value_grad

    start = half_start(row_ref.shape[0], True)
    attend_back(row_ref, proj_ref, triple_ref, probs_ref, back_ref, start, put)


def other_back_kernel(
    row_ref, proj_ref, triple_ref, probs_ref, query_ref, key_ref, value_ref, *refs
):
    outs, (back_ref, slots_ref) = refs[:8], refs[8:]
    half = row_ref.shape[0]
    heads = probs_ref.shape[0]
    per_block = slots_ref.shape[2] // HEAD
    me = lax.axis_index("clip")
    turn = lax.bitwise_and(lax.shift_right_logical(me, 1), 3)
    away = 1 - lax.shift_right_logical(me, 3)
    mine, start = half_start(half, True), half_start(half, False)

    def where(t, h):
        piece = t * heads + h
        block, sub = piece // per_block, piece % per_block
        slot = lax.bitwise_xor(turn, block % 4)
        side = lax.bitwise_xor(away, block // 4)
        return side, slot, slice(sub * HEAD, (sub + 1) * HEAD)

    def put(h, query_grad, key_grad, value_grad):
        rows = slice(h * HEAD, (h + 1) * HEAD)
        side, slot, place = where(0, h)
        slots_ref[side, slot, place, pl.ds(mine, half)] = query_ref[rows, :]
        slots_ref[side, slot, place, pl.ds(start, half)] = query_grad.astype(jnp.bfloat16)
        side, slot, place = where(1, h)
        slots_ref[side, slot, place, :] = (key_ref[rows, :] + key_grad).astype(jnp.bfloat16)
        side, slot, place = where(2, h)
        slots_ref[side, slot, place, :] = (value_ref[rows, :] + value_grad).astype(jnp.bfloat16)

    attend_back(row_ref, proj_ref, triple_ref, probs_ref, back_ref, start, put)
    for k, out_ref in enumerate(outs):
        out_ref[...] = slots_ref[k // 4, k % 4]


def product_kernel(*refs):
    t_refs, n_refs = refs[:4], refs[4:8]
    keep_ref, send_ref, sum_ref = refs[-3:]
    half = keep_ref.shape[0]
    core = lax.bitwise_and(lax.axis_index("clip"), 1)
    total = None
    for t_ref, n_ref in zip(t_refs, n_refs, strict=True):
        term = jnp.dot(t_ref[...], n_ref[...], preferred_element_type=jnp.float32)
        total = term if total is None else total + term
    sum_ref[...] = total
    keep_ref[...] = sum_ref[pl.ds(pl.multiple_of(core * half, 8), half), :]
    other = sum_ref[pl.ds(pl.multiple_of((1 - core) * half, 8), half), :]
    send_ref[...] = other.astype(jnp.bfloat16)


def call(kernel, outs, kinds, flops, args, scratch=(), limit=30):
    spec = {
        "s": pl.BlockSpec(memory_space=pltpu.SMEM),
        "v": pl.BlockSpec(memory_space=pltpu.VMEM),
        "a": pl.BlockSpec(memory_space=pl.ANY),
    }
    return pl.pallas_call(
        kernel,
        out_shape=outs,
        in_specs=[spec[kind] for kind in kinds],
        out_specs=jax.tree.map(lambda _: spec["v"], outs),
        scratch_shapes=list(scratch),
        cost_estimate=pl.CostEstimate(flops=flops, bytes_accessed=4_000_000, transcendentals=0),
        compiler_params=pltpu.CompilerParams(vmem_limit_bytes=limit * 1024 * 1024),
    )(*args)


def fast_body(
    n_clip,
    patches,
    clip_tokens,
    positions,
    norm_gain,
    norm_bias,
    w_qkv,
    b_qkv,
    w_proj,
    b_proj,
    merge_gain,
    merge_bias,
    grad_placed,
):
    rows, width = patches.shape
    local = w_qkv.shape[2]
    heads = local // HEAD
    share_rows = grad_placed.shape[0]
    low = jnp.bfloat16
    shape = jax.ShapeDtypeStruct
    full = shape((rows, width), low)

    def swap(value):
        return lax.ppermute(value, "seq", [(0, 1), (1, 0)])

    def flip(value, bits):
        return lax.ppermute(value, "clip", [(i, i ^ bits) for i in range(n_clip)])

    half = rows // 2
    part, wide = shape((half, width), low), shape((half, width), jnp.float32)
    probs_half = shape((heads, half, rows), low)
    attended = pltpu.VMEM((half, local), low)
    block = 3 * local // 8
    normed, up_keep, up_send = call(
        prepare_kernel,
        (full, part, part),
        "svvaaa",
        8 * rows * share_rows * width,
        (clip_tokens, norm_gain, norm_bias, patches, positions, grad_placed),
        (
            pltpu.VMEM((rows, width), low),
            pltpu.VMEM(positions.shape, jnp.int32),
            pltpu.VMEM(grad_placed.shape, low),
            pltpu.SemaphoreType.DMA((3,)),
        ),
        limit=62,
    )
    up_came = swap(up_send)
    normed_of = [normed] + [flip(normed, q << 1) for q in (1, 2)]
    normed_of += [flip(normed, 3 << 1)]
    triple, other_probs, part_send = call(
        first_kernel,
        (shape((3, rows, local), low), probs_half, part),
        "svaaa",
        7 * rows * width * local,
        (clip_tokens, b_qkv, normed, jnp.transpose(w_qkv, (1, 0, 2)), w_proj),
        (
            pltpu.VMEM((rows, width), low),
            pltpu.VMEM((3, width, local), low),
            pltpu.VMEM((local, width), low),
            attended,
            pltpu.SemaphoreType.DMA((5,)),
        ),
        limit=51,
    )
    part_came = swap(part_send)
    own_probs, part_keep = call(
        second_kernel,
        (probs_half, wide),
        "svv",
        3 * half * width * local,
        (clip_tokens, triple, w_proj),
        (attended,),
    )
    merged, own_rows = call(
        middle_kernel,
        (part, part),
        "v" * 8,
        100 * half * width,
        (
            b_proj,
            merge_gain,
            merge_bias,
            part_keep,
            part_came,
            patches,
            up_keep,
            up_came,
        ),
    )
    other_rows = swap(own_rows)
    other_merged = swap(merged)
    query_own, key_own, value_own = call(
        own_back_kernel,
        (
            shape((local, half), low),
            shape((local, rows), jnp.float32),
            shape((local, rows), jnp.float32),
        ),
        "vvvv",
        4 * half * width * local,
        (own_rows, w_proj, triple, own_probs),
        (attended,),
    )
    sent = call(
        other_back_kernel,
        (shape((block, rows), low),) * 8,
        "v" * 7,
        4 * half * width * local,
        (other_rows, w_proj, triple, other_probs, query_own, key_own, value_own),
        (attended, pltpu.VMEM((2, 4, block, rows), low)),
    )

    def exchange(sent):
        return [sent[0]] + [flip(sent[q], q << 1) for q in (1, 2, 3)]

    def product(taken, after=()):
        return call(
            product_kernel,
            (shape((block // 2, width), jnp.float32), shape((block // 2, width), low)),
            "v" * 8 + "a" * len(after),
            8 * block * rows * width,
            (*taken, *normed_of, *after),
            (pltpu.VMEM((block, width), jnp.float32),),
        )

    far_taken = exchange(sent[:4])
    near_taken = exchange(sent[4:])
    far_keep, far_send = product(far_taken)
    far_came = flip(far_send, 1)
    far_sum = (far_keep + far_came.astype(jnp.float32)).astype(low)
    crossing = flip(far_sum, 8)
    near_keep, near_send = product(near_taken, (far_sum,))
    near_came = flip(near_send, 1)
    placed = call(
        place_kernel,
        shape((share_rows, 4 * width), low),
        "svvva",
        8 * rows * share_rows * width,
        (clip_tokens, positions, merged, other_merged, far_sum),
    )
    summed = near_keep + near_came.astype(jnp.float32) + crossing.astype(jnp.float32)
    return (placed, summed[None])


def solution(mesh):
    n_clip, n_seq = mesh.shape["clip"], mesh.shape["seq"]
    fast = n_clip == 2 * 4 * 2 and n_seq == 2
    body = functools.partial(fast_body, n_clip) if fast else general_body
    return jax.shard_map(
        body,
        mesh=mesh,
        in_specs=(
            P("clip", None),
            P("clip"),
            P("clip", None),
            P(),
            P(),
            P(None, None, "seq"),
            P(None, "seq"),
            P("seq", None),
            P(),
            P(),
            P(),
            P(("clip", "seq"), None),
        ),
        out_specs=(P(("clip", "seq"), None), P("seq", "clip", None)),
        check_vma=False,
    )
```

```python
import functools

import jax
import jax.numpy as jnp
from jax import lax
from jax.experimental import pallas as pl
from jax.experimental.pallas import tpu as pltpu
from jax.sharding import PartitionSpec as P


HEAD = 80


EPSILON = 1e-06


def normalize(values, gain_row, bias_row):
    center = values - jnp.mean(values, axis=-1, keepdims=True)
    inverse = lax.rsqrt(jnp.mean(center * center, axis=-1, keepdims=True) + EPSILON)
    unit_rows = center * inverse
    return (unit_rows * gain_row + bias_row, unit_rows, inverse)


def normalize_back(upstream, unit_rows, inverse, gain_row):
    scaled = upstream * gain_row
    return inverse * (
        scaled
        - jnp.mean(scaled, axis=-1, keepdims=True)
        - unit_rows * jnp.mean(scaled * unit_rows, axis=-1, keepdims=True)
    )


def leading(left, right):
    return lax.dot_general(
        left, right, (((0,), (0,)), ((), ())), preferred_element_type=jnp.float32
    )


def trailing(left, right):
    return lax.dot_general(
        left, right, (((1,), (1,)), ((), ())), preferred_element_type=jnp.float32
    )


def general_body(
    patches,
    clip_tokens,
    positions,
    norm_gain,
    norm_bias,
    w_qkv,
    b_qkv,
    w_proj,
    b_proj,
    merge_gain,
    merge_bias,
    grad_placed,
):
    block_rows = patches.shape[0]
    model_width = patches.shape[1]
    local_width = w_qkv.shape[2]
    local_heads = local_width // HEAD
    live_count = clip_tokens[0]
    places = positions[0]
    widened = patches.astype(jnp.float32)
    normed = normalize(widened, norm_gain, norm_bias)[0].astype(jnp.bfloat16)
    triple = jnp.dot(
        normed, w_qkv.reshape(model_width, 3 * local_width), preferred_element_type=jnp.float32
    )
    triple = (triple.reshape(block_rows, 3, local_width) + b_qkv).astype(jnp.bfloat16)
    query_rows = triple[:, 0].reshape(block_rows, local_heads, HEAD)
    key_rows = triple[:, 1].reshape(block_rows, local_heads, HEAD)
    value_rows = triple[:, 2].reshape(block_rows, local_heads, HEAD)
    scaling = HEAD ** (-0.5)
    scores = (
        jnp.einsum("qhd,khd->hqk", query_rows, key_rows, preferred_element_type=jnp.float32)
        * scaling
    )
    live_keys = jnp.arange(block_rows, dtype=jnp.int32) < 4 * live_count
    scores = jnp.where(live_keys[None, None, :], scores, -1e30)
    highest = jnp.max(scores, axis=-1, keepdims=True)
    powers = jnp.exp(scores - highest)
    weights = powers / jnp.sum(powers, axis=-1, keepdims=True)
    weights_low = weights.astype(jnp.bfloat16)
    attended = jnp.einsum(
        "hqk,khd->qhd", weights_low, value_rows, preferred_element_type=jnp.float32
    )
    attended = attended.reshape(block_rows, local_width).astype(jnp.bfloat16)
    partial_value = jnp.dot(attended, w_proj, preferred_element_type=jnp.float32)
    summed_share = lax.psum_scatter(
        partial_value.astype(jnp.bfloat16), "seq", scatter_dimension=0, tiled=True
    ).astype(jnp.float32)
    share_count = summed_share.shape[0]
    own_start = lax.axis_index("seq") * share_count
    own_patches = lax.dynamic_slice_in_dim(widened, own_start, share_count, 0)
    output_share = summed_share + b_proj + own_patches
    output = lax.all_gather(output_share.astype(jnp.bfloat16), "seq", axis=0, tiled=True).astype(
        output_share.dtype
    )
    merged_full, unit_rows, inverse = normalize(output, merge_gain, merge_bias)
    merged = merged_full.reshape(block_rows // 4, 4 * model_width).astype(jnp.bfloat16)
    live_tokens = jnp.arange(block_rows // 4, dtype=jnp.int32) < live_count
    share_rows = grad_placed.shape[0]
    rows_here = lax.axis_index("seq") * share_rows + jnp.arange(share_rows, dtype=jnp.int32)
    selector = ((places[None, :] == rows_here[:, None]) & live_tokens[None, :]).astype(jnp.bfloat16)
    placed = jnp.dot(selector, merged, preferred_element_type=jnp.float32).astype(jnp.bfloat16)
    own_grad = leading(selector, grad_placed)
    token_grad = lax.psum(own_grad.astype(jnp.bfloat16), "seq").astype(jnp.float32)
    upstream = token_grad.reshape(block_rows, model_width)
    row_grad = normalize_back(upstream, unit_rows, inverse, merge_gain).astype(jnp.bfloat16)
    attn_grad = lax.dot_general(
        row_grad, w_proj, (((1,), (1,)), ((), ())), preferred_element_type=jnp.float32
    )
    attn_grad = attn_grad.astype(jnp.bfloat16).reshape(block_rows, local_heads, HEAD)
    prob_grad = jnp.einsum(
        "qhd,khd->hqk", attn_grad, value_rows, preferred_element_type=jnp.float32
    )
    value_grad = jnp.einsum(
        "hqk,qhd->khd", weights_low, attn_grad, preferred_element_type=jnp.float32
    )
    score_grad = (
        weights * (prob_grad - jnp.sum(prob_grad * weights, axis=-1, keepdims=True)) * scaling
    )
    score_grad = score_grad.astype(jnp.bfloat16)
    query_grad = jnp.einsum(
        "hqk,khd->qhd", score_grad, key_rows, preferred_element_type=jnp.float32
    )
    key_grad = jnp.einsum(
        "hqk,qhd->khd", score_grad, query_rows, preferred_element_type=jnp.float32
    )
    triple_grad = jnp.stack([query_grad, key_grad, value_grad], axis=1)
    triple_grad = triple_grad.reshape(block_rows, 3 * local_width).astype(jnp.bfloat16)
    full_term = leading(triple_grad, normed)
    summed = lax.psum_scatter(full_term, "clip", scatter_dimension=0, tiled=True)
    return (placed, summed[None])


def place_masks(live_ref, places, share_rows, rows, first_row):
    tokens = places.shape[1]
    token = lax.broadcasted_iota(jnp.int32, (tokens, rows), 0)
    owner = (lax.broadcasted_iota(jnp.int32, (tokens, rows), 1) + first_row) // 4
    spread = jnp.where((token == owner) & (token < live_ref[0]), 1.0, 0.0)
    shifted = jnp.broadcast_to(places.astype(jnp.float32) + 1.0, (8, tokens))
    row = jnp.dot(shifted, spread, precision=lax.Precision.HIGHEST)[:1] - 1.0
    first = lax.axis_index("seq") * share_rows
    window = lax.broadcasted_iota(jnp.int32, (share_rows, rows), 0) + first
    patch = lax.broadcasted_iota(jnp.int32, (share_rows, rows), 1)
    hit = window.astype(jnp.float32) == row
    return [
        jnp.where(hit & (lax.rem(patch, 4) == k), 1.0, 0.0).astype(jnp.bfloat16) for k in range(4)
    ]


def begin(sources, targets, sems, first=0):
    copies = [
        pltpu.make_async_copy(source, target, sems.at[first + k])
        for k, (source, target) in enumerate(zip(sources, targets, strict=True))
    ]
    for copy in copies:
        copy.start()
    return copies


def half_start(half, own):
    seq = lax.axis_index("seq")
    return pl.multiple_of((seq if own else 1 - seq) * half, 128)


def prepare_kernel(
    live_ref,
    gain_hbm,
    bias_hbm,
    patches_hbm,
    places_hbm,
    grad_hbm,
    normed_hbm,
    keep_hbm,
    send_hbm,
    gain_ref,
    bias_ref,
    patches_ref,
    places_ref,
    grad_ref,
    normed_ref,
    keep_ref,
    send_ref,
    sems,
):
    half, width = send_ref.shape
    came = begin(
        (places_hbm, grad_hbm, gain_hbm, bias_hbm, patches_hbm),
        (places_ref, grad_ref, gain_ref, bias_ref, patches_ref),
        sems,
    )
    came[0].wait()
    masks = [
        place_masks(live_ref, places_ref[...], grad_ref.shape[0], half, half_start(half, own))
        for own in (False, True)
    ]
    came[1].wait()
    went = []
    for out_ref, out_hbm, masks_of in ((send_ref, send_hbm, masks[0]), (keep_ref, keep_hbm, masks[1])):
        total = None
        for k in range(4):
            term = leading(masks_of[k], grad_ref[:, k * width : (k + 1) * width])
            total = term if total is None else total + term
        out_ref[...] = total.astype(out_ref.dtype)
        went += begin((out_ref,), (out_hbm,), sems, 5 + len(went))
    for copy in came[2:]:
        copy.wait()
    normed_ref[...] = normalize(
        patches_ref[...].astype(jnp.float32), gain_ref[...][None, :], bias_ref[...][None, :]
    )[0].astype(jnp.bfloat16)
    went += begin((normed_ref,), (normed_hbm,), sems, 7)
    for copy in went:
        copy.wait()


def place_kernel(live_ref, places_ref, own_ref, other_ref, _, out_ref):
    half, width = own_ref.shape
    share_rows = out_ref.shape[0]
    own = place_masks(live_ref, places_ref[...], share_rows, half, half_start(half, True))
    other = place_masks(live_ref, places_ref[...], share_rows, half, half_start(half, False))
    for k in range(4):
        term = jnp.dot(own[k], own_ref[...], preferred_element_type=jnp.float32)
        term += jnp.dot(other[k], other_ref[...], preferred_element_type=jnp.float32)
        out_ref[:, k * width : (k + 1) * width] = term.astype(out_ref.dtype)


def attend(live_ref, triple_ref, start, probs_ref, attended_ref):
    half, rows = probs_ref.shape[1:]
    live = lax.broadcasted_iota(jnp.int32, (half, rows), 1) < 4 * live_ref[0]
    steep = HEAD ** (-0.5) * 1.4426950408889634
    for h in range(probs_ref.shape[0]):
        cols = slice(h * HEAD, (h + 1) * HEAD)
        scores = trailing(triple_ref[0, pl.ds(start, half), cols], triple_ref[1, :, cols])
        scores = jnp.where(live, scores, -1e30)
        powers = jnp.exp2((scores - jnp.max(scores, axis=-1, keepdims=True)) * steep)
        weights = powers * (1.0 / jnp.sum(powers, axis=-1, keepdims=True))
        weights = weights.astype(jnp.bfloat16)
        probs_ref[h] = weights
        attended_ref[:, cols] = jnp.dot(
            weights, triple_ref[2, :, cols], preferred_element_type=jnp.float32
        ).astype(jnp.bfloat16)


def first_kernel(
    live_ref,
    b_ref,
    normed_hbm,
    w_hbm,
    proj_hbm,
    triple_ref,
    probs_ref,
    send_ref,
    normed_ref,
    w_ref,
    proj_ref,
    attended_ref,
    sems,
):
    came = begin(
        (normed_hbm, w_hbm.at[0], w_hbm.at[1], w_hbm.at[2], proj_hbm),
        (normed_ref, w_ref.at[0], w_ref.at[1], w_ref.at[2], proj_ref),
        sems,
    )
    came[0].wait()
    for t in range(3):
        came[1 + t].wait()
        part = jnp.dot(normed_ref[...], w_ref[t], preferred_element_type=jnp.float32)
        triple_ref[t] = (part + b_ref[t : t + 1, :]).astype(jnp.bfloat16)
    start = half_start(send_ref.shape[0], False)
    attend(live_ref, triple_ref, start, probs_ref, attended_ref)
    came[4].wait()
    send_ref[...] = jnp.dot(
        attended_ref[...], proj_ref[...], preferred_element_type=jnp.float32
    ).astype(jnp.bfloat16)


def second_kernel(live_ref, triple_ref, proj_ref, probs_ref, keep_ref, attended_ref):
    start = half_start(keep_ref.shape[0], True)
    attend(live_ref, triple_ref, start, probs_ref, attended_ref)
    keep_ref[...] = jnp.dot(attended_ref[...], proj_ref[...], preferred_element_type=jnp.float32)


def middle_kernel(
    b_ref,
    gain_ref,
    bias_ref,
    keep_ref,
    came_ref,
    patches_ref,
    up_keep_ref,
    up_came_ref,
    merged_ref,
    back_ref,
):
    half = keep_ref.shape[0]
    gain = gain_ref[...][None, :]
    output = (
        keep_ref[...]
        + came_ref[...].astype(jnp.float32)
        + b_ref[...][None, :]
        + patches_ref[pl.ds(half_start(half, True), half), :].astype(jnp.float32)
    )
    merged, unit_rows, inverse = normalize(output, gain, bias_ref[...][None, :])
    merged_ref[...] = merged.astype(jnp.bfloat16)
    upstream = up_keep_ref[...].astype(jnp.float32) + up_came_ref[...].astype(jnp.float32)
    back_ref[...] = normalize_back(upstream, unit_rows, inverse, gain).astype(jnp.bfloat16)


def attend_back(row_ref, proj_ref, triple_ref, probs_ref, back_ref, start, put):
    half = row_ref.shape[0]
    back_ref[...] = trailing(row_ref[...], proj_ref[...]).astype(jnp.bfloat16)
    scaling = HEAD ** (-0.5)
    for h in range(probs_ref.shape[0]):
        cols = slice(h * HEAD, (h + 1) * HEAD)
        back = back_ref[:, cols]
        weights = probs_ref[h]
        prob_grad = trailing(back, triple_ref[2, :, cols])
        wide = weights.astype(jnp.float32)
        inner = jnp.sum(prob_grad * wide, axis=-1, keepdims=True)
        score_grad = (wide * (prob_grad - inner)).astype(jnp.bfloat16)
        query_grad = lax.dot_general(
            triple_ref[1, :, cols],
            score_grad,
            (((0,), (1,)), ((), ())),
            preferred_element_type=jnp.float32,
        )
        key_grad = leading(triple_ref[0, pl.ds(start, half), cols], score_grad)
        put(h, query_grad * scaling, key_grad * scaling, leading(back, weights))


def own_back_kernel(
    row_ref, proj_ref, triple_ref, probs_ref, query_ref, key_ref, value_ref, back_ref
):
    def put(h, query_grad, key_grad, value_grad):
        rows = slice(h * HEAD, (h + 1) * HEAD)
        query_ref[rows, :] = query_grad.astype(jnp.bfloat16)
        key_ref[rows, :] = key_grad
        value_ref[rows, :] = value_grad

    start = half_start(row_ref.shape[0], True)
    attend_back(row_ref, proj_ref, triple_ref, probs_ref, back_ref, start, put)


def other_back_kernel(
    row_ref, proj_ref, triple_ref, probs_ref, query_ref, key_ref, value_ref, *refs
):
    outs, (back_ref, slots_ref) = refs[:8], refs[8:]
    half = row_ref.shape[0]
    heads = probs_ref.shape[0]
    per_block = slots_ref.shape[2] // HEAD
    me = lax.axis_index("clip")
    turn = lax.bitwise_and(lax.shift_right_logical(me, 1), 3)
    away = 1 - lax.shift_right_logical(me, 3)
    mine, start = half_start(half, True), half_start(half, False)

    def where(t, h):
        piece = t * heads + h
        block, sub = piece // per_block, piece % per_block
        slot = lax.bitwise_xor(turn, block % 4)
        side = lax.bitwise_xor(away, block // 4)
        return side, slot, slice(sub * HEAD, (sub + 1) * HEAD)

    def put(h, query_grad, key_grad, value_grad):
        rows = slice(h * HEAD, (h + 1) * HEAD)
        side, slot, place = where(0, h)
        slots_ref[side, slot, place, pl.ds(mine, half)] = query_ref[rows, :]
        slots_ref[side, slot, place, pl.ds(start, half)] = query_grad.astype(jnp.bfloat16)
        side, slot, place = where(1, h)
        slots_ref[side, slot, place, :] = (key_ref[rows, :] + key_grad).astype(jnp.bfloat16)
        side, slot, place = where(2, h)
        slots_ref[side, slot, place, :] = (value_ref[rows, :] + value_grad).astype(jnp.bfloat16)

    attend_back(row_ref, proj_ref, triple_ref, probs_ref, back_ref, start, put)
    for k, out_ref in enumerate(outs):
        out_ref[...] = slots_ref[k // 4, k % 4]


def product_kernel(*refs):
    t_refs, n_refs = refs[:4], refs[4:8]
    keep_ref, send_ref, sum_ref = refs[-3:]
    half = keep_ref.shape[0]
    core = lax.bitwise_and(lax.axis_index("clip"), 1)
    total = None
    for t_ref, n_ref in zip(t_refs, n_refs, strict=True):
        term = jnp.dot(t_ref[...], n_ref[...], preferred_element_type=jnp.float32)
        total = term if total is None else total + term
    sum_ref[...] = total
    keep_ref[...] = sum_ref[pl.ds(pl.multiple_of(core * half, 8), half), :]
    other = sum_ref[pl.ds(pl.multiple_of((1 - core) * half, 8), half), :]
    send_ref[...] = other.astype(jnp.bfloat16)


def call(kernel, outs, kinds, flops, args, scratch=(), limit=30, out_kind="v"):
    spec = {
        "s": pl.BlockSpec(memory_space=pltpu.SMEM),
        "v": pl.BlockSpec(memory_space=pltpu.VMEM),
        "a": pl.BlockSpec(memory_space=pl.ANY),
    }
    return pl.pallas_call(
        kernel,
        out_shape=outs,
        in_specs=[spec[kind] for kind in kinds],
        out_specs=jax.tree.map(lambda _: spec[out_kind], outs),
        scratch_shapes=list(scratch),
        cost_estimate=pl.CostEstimate(flops=flops, bytes_accessed=4_000_000, transcendentals=0),
        compiler_params=pltpu.CompilerParams(vmem_limit_bytes=limit * 1024 * 1024),
    )(*args)


def fast_body(
    n_clip,
    patches,
    clip_tokens,
    positions,
    norm_gain,
    norm_bias,
    w_qkv,
    b_qkv,
    w_proj,
    b_proj,
    merge_gain,
    merge_bias,
    grad_placed,
):
    rows, width = patches.shape
    local = w_qkv.shape[2]
    heads = local // HEAD
    share_rows = grad_placed.shape[0]
    low = jnp.bfloat16
    shape = jax.ShapeDtypeStruct
    full = shape((rows, width), low)

    def swap(value):
        return lax.ppermute(value, "seq", [(0, 1), (1, 0)])

    def flip(value, bits):
        return lax.ppermute(value, "clip", [(i, i ^ bits) for i in range(n_clip)])

    half = rows // 2
    part, wide = shape((half, width), low), shape((half, width), jnp.float32)
    probs_half = shape((heads, half, rows), low)
    attended = pltpu.VMEM((half, local), low)
    block = 3 * local // 8
    normed, up_keep, up_send = call(
        prepare_kernel,
        (full, part, part),
        "saaaaa",
        8 * rows * share_rows * width,
        (clip_tokens, norm_gain, norm_bias, patches, positions, grad_placed),
        (
            pltpu.VMEM(norm_gain.shape, jnp.float32),
            pltpu.VMEM(norm_bias.shape, jnp.float32),
            pltpu.VMEM((rows, width), low),
            pltpu.VMEM(positions.shape, jnp.int32),
            pltpu.VMEM(grad_placed.shape, low),
            pltpu.VMEM((rows, width), low),
            pltpu.VMEM((half, width), low),
            pltpu.VMEM((half, width), low),
            pltpu.SemaphoreType.DMA((8,)),
        ),
        limit=62,
        out_kind="a",
    )
    up_came = swap(up_send)
    normed_of = [normed] + [flip(normed, q << 1) for q in (1, 2)]
    normed_of += [flip(normed, 3 << 1)]
    triple, other_probs, part_send = call(
        first_kernel,
        (shape((3, rows, local), low), probs_half, part),
        "svaaa",
        7 * rows * width * local,
        (clip_tokens, b_qkv, normed, jnp.transpose(w_qkv, (1, 0, 2)), w_proj),
        (
            pltpu.VMEM((rows, width), low),
            pltpu.VMEM((3, width, local), low),
            pltpu.VMEM((local, width), low),
            attended,
            pltpu.SemaphoreType.DMA((5,)),
        ),
        limit=51,
    )
    part_came = swap(part_send)
    own_probs, part_keep = call(
        second_kernel,
        (probs_half, wide),
        "svv",
        3 * half * width * local,
        (clip_tokens, triple, w_proj),
        (attended,),
    )
    merged, own_rows = call(
        middle_kernel,
        (part, part),
        "v" * 8,
        100 * half * width,
        (
            b_proj,
            merge_gain,
            merge_bias,
            part_keep,
            part_came,
            patches,
            up_keep,
            up_came,
        ),
    )
    other_rows = swap(own_rows)
    other_merged = swap(merged)
    query_own, key_own, value_own = call(
        own_back_kernel,
        (
            shape((local, half), low),
            shape((local, rows), jnp.float32),
            shape((local, rows), jnp.float32),
        ),
        "vvvv",
        4 * half * width * local,
        (own_rows, w_proj, triple, own_probs),
        (attended,),
    )
    sent = call(
        other_back_kernel,
        (shape((block, rows), low),) * 8,
        "v" * 7,
        4 * half * width * local,
        (other_rows, w_proj, triple, other_probs, query_own, key_own, value_own),
        (attended, pltpu.VMEM((2, 4, block, rows), low)),
    )

    def exchange(sent):
        return [sent[0]] + [flip(sent[q], q << 1) for q in (1, 2, 3)]

    def product(taken, after=()):
        return call(
            product_kernel,
            (shape((block // 2, width), jnp.float32), shape((block // 2, width), low)),
            "v" * 8 + "a" * len(after),
            8 * block * rows * width,
            (*taken, *normed_of, *after),
            (pltpu.VMEM((block, width), jnp.float32),),
        )

    far_taken = exchange(sent[:4])
    near_taken = exchange(sent[4:])
    far_keep, far_send = product(far_taken)
    far_came = flip(far_send, 1)
    far_sum = (far_keep + far_came.astype(jnp.float32)).astype(low)
    crossing = flip(far_sum, 8)
    near_keep, near_send = product(near_taken, (far_sum,))
    near_came = flip(near_send, 1)
    placed = call(
        place_kernel,
        shape((share_rows, 4 * width), low),
        "svvva",
        8 * rows * share_rows * width,
        (clip_tokens, positions, merged, other_merged, far_sum),
    )
    summed = near_keep + near_came.astype(jnp.float32) + crossing.astype(jnp.float32)
    return (placed, summed[None])


def solution(mesh):
    n_clip, n_seq = mesh.shape["clip"], mesh.shape["seq"]
    fast = n_clip == 2 * 4 * 2 and n_seq == 2
    body = functools.partial(fast_body, n_clip) if fast else general_body
    return jax.shard_map(
        body,
        mesh=mesh,
        in_specs=(
            P("clip", None),
            P("clip"),
            P("clip", None),
            P(),
            P(),
            P(None, None, "seq"),
            P(None, "seq"),
            P("seq", None),
            P(),
            P(),
            P(),
            P(("clip", "seq"), None),
        ),
        out_specs=(P(("clip", "seq"), None), P("seq", "clip", None)),
        check_vma=False,
    )
```

```python
import functools

import jax
import jax.numpy as jnp
from jax import lax
from jax.experimental import pallas as pl
from jax.experimental.pallas import tpu as pltpu
from jax.sharding import PartitionSpec as P


HEAD = 80


EPSILON = 1e-06


def normalize(values, gain_row, bias_row):
    center = values - jnp.mean(values, axis=-1, keepdims=True)
    inverse = lax.rsqrt(jnp.mean(center * center, axis=-1, keepdims=True) + EPSILON)
    unit_rows = center * inverse
    return (unit_rows * gain_row + bias_row, unit_rows, inverse)


def normalize_back(upstream, unit_rows, inverse, gain_row):
    scaled = upstream * gain_row
    return inverse * (
        scaled
        - jnp.mean(scaled, axis=-1, keepdims=True)
        - unit_rows * jnp.mean(scaled * unit_rows, axis=-1, keepdims=True)
    )


def leading(left, right):
    return lax.dot_general(
        left, right, (((0,), (0,)), ((), ())), preferred_element_type=jnp.float32
    )


def trailing(left, right):
    return lax.dot_general(
        left, right, (((1,), (1,)), ((), ())), preferred_element_type=jnp.float32
    )


def general_body(
    patches,
    clip_tokens,
    positions,
    norm_gain,
    norm_bias,
    w_qkv,
    b_qkv,
    w_proj,
    b_proj,
    merge_gain,
    merge_bias,
    grad_placed,
):
    block_rows = patches.shape[0]
    model_width = patches.shape[1]
    local_width = w_qkv.shape[2]
    local_heads = local_width // HEAD
    live_count = clip_tokens[0]
    places = positions[0]
    widened = patches.astype(jnp.float32)
    normed = normalize(widened, norm_gain, norm_bias)[0].astype(jnp.bfloat16)
    triple = jnp.dot(
        normed, w_qkv.reshape(model_width, 3 * local_width), preferred_element_type=jnp.float32
    )
    triple = (triple.reshape(block_rows, 3, local_width) + b_qkv).astype(jnp.bfloat16)
    query_rows = triple[:, 0].reshape(block_rows, local_heads, HEAD)
    key_rows = triple[:, 1].reshape(block_rows, local_heads, HEAD)
    value_rows = triple[:, 2].reshape(block_rows, local_heads, HEAD)
    scaling = HEAD ** (-0.5)
    scores = (
        jnp.einsum("qhd,khd->hqk", query_rows, key_rows, preferred_element_type=jnp.float32)
        * scaling
    )
    live_keys = jnp.arange(block_rows, dtype=jnp.int32) < 4 * live_count
    scores = jnp.where(live_keys[None, None, :], scores, -1e30)
    highest = jnp.max(scores, axis=-1, keepdims=True)
    powers = jnp.exp(scores - highest)
    weights = powers / jnp.sum(powers, axis=-1, keepdims=True)
    weights_low = weights.astype(jnp.bfloat16)
    attended = jnp.einsum(
        "hqk,khd->qhd", weights_low, value_rows, preferred_element_type=jnp.float32
    )
    attended = attended.reshape(block_rows, local_width).astype(jnp.bfloat16)
    partial_value = jnp.dot(attended, w_proj, preferred_element_type=jnp.float32)
    summed_share = lax.psum_scatter(
        partial_value.astype(jnp.bfloat16), "seq", scatter_dimension=0, tiled=True
    ).astype(jnp.float32)
    share_count = summed_share.shape[0]
    own_start = lax.axis_index("seq") * share_count
    own_patches = lax.dynamic_slice_in_dim(widened, own_start, share_count, 0)
    output_share = summed_share + b_proj + own_patches
    output = lax.all_gather(output_share.astype(jnp.bfloat16), "seq", axis=0, tiled=True).astype(
        output_share.dtype
    )
    merged_full, unit_rows, inverse = normalize(output, merge_gain, merge_bias)
    merged = merged_full.reshape(block_rows // 4, 4 * model_width).astype(jnp.bfloat16)
    live_tokens = jnp.arange(block_rows // 4, dtype=jnp.int32) < live_count
    share_rows = grad_placed.shape[0]
    rows_here = lax.axis_index("seq") * share_rows + jnp.arange(share_rows, dtype=jnp.int32)
    selector = ((places[None, :] == rows_here[:, None]) & live_tokens[None, :]).astype(jnp.bfloat16)
    placed = jnp.dot(selector, merged, preferred_element_type=jnp.float32).astype(jnp.bfloat16)
    own_grad = leading(selector, grad_placed)
    token_grad = lax.psum(own_grad.astype(jnp.bfloat16), "seq").astype(jnp.float32)
    upstream = token_grad.reshape(block_rows, model_width)
    row_grad = normalize_back(upstream, unit_rows, inverse, merge_gain).astype(jnp.bfloat16)
    attn_grad = lax.dot_general(
        row_grad, w_proj, (((1,), (1,)), ((), ())), preferred_element_type=jnp.float32
    )
    attn_grad = attn_grad.astype(jnp.bfloat16).reshape(block_rows, local_heads, HEAD)
    prob_grad = jnp.einsum(
        "qhd,khd->hqk", attn_grad, value_rows, preferred_element_type=jnp.float32
    )
    value_grad = jnp.einsum(
        "hqk,qhd->khd", weights_low, attn_grad, preferred_element_type=jnp.float32
    )
    score_grad = (
        weights * (prob_grad - jnp.sum(prob_grad * weights, axis=-1, keepdims=True)) * scaling
    )
    score_grad = score_grad.astype(jnp.bfloat16)
    query_grad = jnp.einsum(
        "hqk,khd->qhd", score_grad, key_rows, preferred_element_type=jnp.float32
    )
    key_grad = jnp.einsum(
        "hqk,qhd->khd", score_grad, query_rows, preferred_element_type=jnp.float32
    )
    triple_grad = jnp.stack([query_grad, key_grad, value_grad], axis=1)
    triple_grad = triple_grad.reshape(block_rows, 3 * local_width).astype(jnp.bfloat16)
    full_term = leading(triple_grad, normed)
    summed = lax.psum_scatter(full_term, "clip", scatter_dimension=0, tiled=True)
    return (placed, summed[None])


def place_masks(live_ref, places, share_rows, rows, first_row):
    tokens = places.shape[1]
    token = lax.broadcasted_iota(jnp.int32, (tokens, rows), 0)
    owner = (lax.broadcasted_iota(jnp.int32, (tokens, rows), 1) + first_row) // 4
    spread = jnp.where((token == owner) & (token < live_ref[0]), 1.0, 0.0)
    shifted = jnp.broadcast_to(places.astype(jnp.float32) + 1.0, (8, tokens))
    row = jnp.dot(shifted, spread, precision=lax.Precision.HIGHEST)[:1] - 1.0
    first = lax.axis_index("seq") * share_rows
    window = lax.broadcasted_iota(jnp.int32, (share_rows, rows), 0) + first
    patch = lax.broadcasted_iota(jnp.int32, (share_rows, rows), 1)
    hit = window.astype(jnp.float32) == row
    return [
        jnp.where(hit & (lax.rem(patch, 4) == k), 1.0, 0.0).astype(jnp.bfloat16) for k in range(4)
    ]


def begin(sources, targets, sems, first=0):
    copies = [
        pltpu.make_async_copy(source, target, sems.at[first + k])
        for k, (source, target) in enumerate(zip(sources, targets, strict=True))
    ]
    for copy in copies:
        copy.start()
    return copies


def half_start(half, own):
    seq = lax.axis_index("seq")
    return pl.multiple_of((seq if own else 1 - seq) * half, 128)


def norm_low(patches_ref, gain_ref, bias_ref):
    return normalize(
        patches_ref[...].astype(jnp.float32), gain_ref[...][None, :], bias_ref[...][None, :]
    )[0].astype(jnp.bfloat16)


def pull(live_ref, places_ref, grad_ref, out_ref, own):
    half, width = out_ref.shape
    masks = place_masks(
        live_ref, places_ref[...], grad_ref.shape[0], half, half_start(half, own)
    )
    total = None
    for k in range(4):
        term = leading(masks[k], grad_ref[:, k * width : (k + 1) * width])
        total = term if total is None else total + term
    out_ref[...] = total.astype(out_ref.dtype)


def prepare_kernel(
    live_ref,
    gain_hbm,
    bias_hbm,
    patches_hbm,
    places_hbm,
    grad_hbm,
    normed_hbm,
    send_hbm,
    gain_ref,
    bias_ref,
    patches_ref,
    places_ref,
    grad_ref,
    normed_ref,
    send_ref,
    sems,
):
    came = begin(
        (gain_hbm, bias_hbm, patches_hbm, places_hbm, grad_hbm),
        (gain_ref, bias_ref, patches_ref, places_ref, grad_ref),
        sems,
    )
    for copy in came[:3]:
        copy.wait()
    normed_ref[...] = norm_low(patches_ref, gain_ref, bias_ref)
    went = begin((normed_ref,), (normed_hbm,), sems, 5)
    for copy in came[3:]:
        copy.wait()
    pull(live_ref, places_ref, grad_ref, send_ref, False)
    went += begin((send_ref,), (send_hbm,), sems, 6)
    for copy in went:
        copy.wait()


def place_kernel(live_ref, places_ref, own_ref, other_ref, _, out_ref):
    half, width = own_ref.shape
    share_rows = out_ref.shape[0]
    own = place_masks(live_ref, places_ref[...], share_rows, half, half_start(half, True))
    other = place_masks(live_ref, places_ref[...], share_rows, half, half_start(half, False))
    for k in range(4):
        term = jnp.dot(own[k], own_ref[...], preferred_element_type=jnp.float32)
        term += jnp.dot(other[k], other_ref[...], preferred_element_type=jnp.float32)
        out_ref[:, k * width : (k + 1) * width] = term.astype(out_ref.dtype)


def attend(live_ref, triple_ref, start, probs_ref, attended_ref):
    half, rows = probs_ref.shape[1:]
    live = lax.broadcasted_iota(jnp.int32, (half, rows), 1) < 4 * live_ref[0]
    steep = HEAD ** (-0.5) * 1.4426950408889634
    for h in range(probs_ref.shape[0]):
        cols = slice(h * HEAD, (h + 1) * HEAD)
        scores = trailing(triple_ref[0, pl.ds(start, half), cols], triple_ref[1, :, cols])
        scores = jnp.where(live, scores, -1e30)
        powers = jnp.exp2((scores - jnp.max(scores, axis=-1, keepdims=True)) * steep)
        weights = powers * (1.0 / jnp.sum(powers, axis=-1, keepdims=True))
        weights = weights.astype(jnp.bfloat16)
        probs_ref[h] = weights
        attended_ref[:, cols] = jnp.dot(
            weights, triple_ref[2, :, cols], preferred_element_type=jnp.float32
        ).astype(jnp.bfloat16)


def first_kernel(
    live_ref,
    b_ref,
    gain_ref,
    bias_ref,
    patches_hbm,
    w_hbm,
    proj_hbm,
    triple_ref,
    probs_ref,
    send_ref,
    patches_ref,
    w_ref,
    proj_ref,
    attended_ref,
    normed_ref,
    sems,
):
    came = begin(
        (patches_hbm, w_hbm.at[0], w_hbm.at[1], w_hbm.at[2], proj_hbm),
        (patches_ref, w_ref.at[0], w_ref.at[1], w_ref.at[2], proj_ref),
        sems,
    )
    came[0].wait()
    normed_ref[...] = norm_low(patches_ref, gain_ref, bias_ref)
    for t in range(3):
        came[1 + t].wait()
        part = jnp.dot(normed_ref[...], w_ref[t], preferred_element_type=jnp.float32)
        triple_ref[t] = (part + b_ref[t : t + 1, :]).astype(jnp.bfloat16)
    start = half_start(send_ref.shape[0], False)
    attend(live_ref, triple_ref, start, probs_ref, attended_ref)
    came[4].wait()
    send_ref[...] = jnp.dot(
        attended_ref[...], proj_ref[...], preferred_element_type=jnp.float32
    ).astype(jnp.bfloat16)


def second_kernel(
    live_ref,
    places_ref,
    grad_ref,
    triple_ref,
    proj_ref,
    probs_ref,
    keep_ref,
    up_ref,
    attended_ref,
):
    start = half_start(keep_ref.shape[0], True)
    attend(live_ref, triple_ref, start, probs_ref, attended_ref)
    keep_ref[...] = jnp.dot(attended_ref[...], proj_ref[...], preferred_element_type=jnp.float32)
    pull(live_ref, places_ref, grad_ref, up_ref, True)


def middle_kernel(
    b_ref,
    gain_ref,
    bias_ref,
    keep_ref,
    came_ref,
    patches_ref,
    up_keep_ref,
    up_came_ref,
    merged_ref,
    back_ref,
):
    half = keep_ref.shape[0]
    gain = gain_ref[...][None, :]
    output = (
        keep_ref[...]
        + came_ref[...].astype(jnp.float32)
        + b_ref[...][None, :]
        + patches_ref[pl.ds(half_start(half, True), half), :].astype(jnp.float32)
    )
    merged, unit_rows, inverse = normalize(output, gain, bias_ref[...][None, :])
    merged_ref[...] = merged.astype(jnp.bfloat16)
    upstream = up_keep_ref[...].astype(jnp.float32) + up_came_ref[...].astype(jnp.float32)
    back_ref[...] = normalize_back(upstream, unit_rows, inverse, gain).astype(jnp.bfloat16)


def attend_back(row_ref, proj_ref, triple_ref, probs_ref, back_ref, start, put):
    half = row_ref.shape[0]
    back_ref[...] = trailing(row_ref[...], proj_ref[...]).astype(jnp.bfloat16)
    scaling = HEAD ** (-0.5)
    for h in range(probs_ref.shape[0]):
        cols = slice(h * HEAD, (h + 1) * HEAD)
        back = back_ref[:, cols]
        weights = probs_ref[h]
        prob_grad = trailing(back, triple_ref[2, :, cols])
        wide = weights.astype(jnp.float32)
        inner = jnp.sum(prob_grad * wide, axis=-1, keepdims=True)
        score_grad = (wide * (prob_grad - inner)).astype(jnp.bfloat16)
        query_grad = lax.dot_general(
            triple_ref[1, :, cols],
            score_grad,
            (((0,), (1,)), ((), ())),
            preferred_element_type=jnp.float32,
        )
        key_grad = leading(triple_ref[0, pl.ds(start, half), cols], score_grad)
        put(h, query_grad * scaling, key_grad * scaling, leading(back, weights))


def own_back_kernel(
    row_ref, proj_ref, triple_ref, probs_ref, query_ref, key_ref, value_ref, back_ref
):
    def put(h, query_grad, key_grad, value_grad):
        rows = slice(h * HEAD, (h + 1) * HEAD)
        query_ref[rows, :] = query_grad.astype(jnp.bfloat16)
        key_ref[rows, :] = key_grad
        value_ref[rows, :] = value_grad

    start = half_start(row_ref.shape[0], True)
    attend_back(row_ref, proj_ref, triple_ref, probs_ref, back_ref, start, put)


def other_back_kernel(
    row_ref, proj_ref, triple_ref, probs_ref, query_ref, key_ref, value_ref, *refs
):
    outs, (back_ref, slots_ref) = refs[:8], refs[8:]
    half = row_ref.shape[0]
    heads = probs_ref.shape[0]
    per_block = slots_ref.shape[2] // HEAD
    me = lax.axis_index("clip")
    turn = lax.bitwise_and(lax.shift_right_logical(me, 1), 3)
    away = 1 - lax.shift_right_logical(me, 3)
    mine, start = half_start(half, True), half_start(half, False)

    def where(t, h):
        piece = t * heads + h
        block, sub = piece // per_block, piece % per_block
        slot = lax.bitwise_xor(turn, block % 4)
        side = lax.bitwise_xor(away, block // 4)
        return side, slot, slice(sub * HEAD, (sub + 1) * HEAD)

    def put(h, query_grad, key_grad, value_grad):
        rows = slice(h * HEAD, (h + 1) * HEAD)
        side, slot, place = where(0, h)
        slots_ref[side, slot, place, pl.ds(mine, half)] = query_ref[rows, :]
        slots_ref[side, slot, place, pl.ds(start, half)] = query_grad.astype(jnp.bfloat16)
        side, slot, place = where(1, h)
        slots_ref[side, slot, place, :] = (key_ref[rows, :] + key_grad).astype(jnp.bfloat16)
        side, slot, place = where(2, h)
        slots_ref[side, slot, place, :] = (value_ref[rows, :] + value_grad).astype(jnp.bfloat16)

    attend_back(row_ref, proj_ref, triple_ref, probs_ref, back_ref, start, put)
    for k, out_ref in enumerate(outs):
        out_ref[...] = slots_ref[k // 4, k % 4]


def product_kernel(*refs):
    t_refs, n_refs = refs[:4], refs[4:8]
    keep_ref, send_ref, sum_ref = refs[-3:]
    half = keep_ref.shape[0]
    core = lax.bitwise_and(lax.axis_index("clip"), 1)
    total = None
    for t_ref, n_ref in zip(t_refs, n_refs, strict=True):
        term = jnp.dot(t_ref[...], n_ref[...], preferred_element_type=jnp.float32)
        total = term if total is None else total + term
    sum_ref[...] = total
    keep_ref[...] = sum_ref[pl.ds(pl.multiple_of(core * half, 8), half), :]
    other = sum_ref[pl.ds(pl.multiple_of((1 - core) * half, 8), half), :]
    send_ref[...] = other.astype(jnp.bfloat16)


def call(kernel, outs, kinds, flops, args, scratch=(), limit=30, out_kind="v"):
    spec = {
        "s": pl.BlockSpec(memory_space=pltpu.SMEM),
        "v": pl.BlockSpec(memory_space=pltpu.VMEM),
        "a": pl.BlockSpec(memory_space=pl.ANY),
    }
    return pl.pallas_call(
        kernel,
        out_shape=outs,
        in_specs=[spec[kind] for kind in kinds],
        out_specs=jax.tree.map(lambda _: spec[out_kind], outs),
        scratch_shapes=list(scratch),
        cost_estimate=pl.CostEstimate(flops=flops, bytes_accessed=4_000_000, transcendentals=0),
        compiler_params=pltpu.CompilerParams(vmem_limit_bytes=limit * 1024 * 1024),
    )(*args)


def fast_body(
    n_clip,
    patches,
    clip_tokens,
    positions,
    norm_gain,
    norm_bias,
    w_qkv,
    b_qkv,
    w_proj,
    b_proj,
    merge_gain,
    merge_bias,
    grad_placed,
):
    rows, width = patches.shape
    local = w_qkv.shape[2]
    heads = local // HEAD
    share_rows = grad_placed.shape[0]
    low = jnp.bfloat16
    shape = jax.ShapeDtypeStruct
    full = shape((rows, width), low)

    def swap(value):
        return lax.ppermute(value, "seq", [(0, 1), (1, 0)])

    def flip(value, bits):
        return lax.ppermute(value, "clip", [(i, i ^ bits) for i in range(n_clip)])

    half = rows // 2
    part, wide = shape((half, width), low), shape((half, width), jnp.float32)
    probs_half = shape((heads, half, rows), low)
    attended = pltpu.VMEM((half, local), low)
    block = 3 * local // 8
    normed, up_send = call(
        prepare_kernel,
        (full, part),
        "saaaaa",
        8 * rows * share_rows * width,
        (clip_tokens, norm_gain, norm_bias, patches, positions, grad_placed),
        (
            pltpu.VMEM(norm_gain.shape, jnp.float32),
            pltpu.VMEM(norm_bias.shape, jnp.float32),
            pltpu.VMEM((rows, width), low),
            pltpu.VMEM(positions.shape, jnp.int32),
            pltpu.VMEM(grad_placed.shape, low),
            pltpu.VMEM((rows, width), low),
            pltpu.VMEM((half, width), low),
            pltpu.SemaphoreType.DMA((7,)),
        ),
        limit=62,
        out_kind="a",
    )
    up_came = swap(up_send)
    normed_of = [normed] + [flip(normed, q << 1) for q in (1, 2)]
    normed_of += [flip(normed, 3 << 1)]
    triple, other_probs, part_send = call(
        first_kernel,
        (shape((3, rows, local), low), probs_half, part),
        "svvvaaa",
        7 * rows * width * local,
        (
            clip_tokens,
            b_qkv,
            norm_gain,
            norm_bias,
            patches,
            jnp.transpose(w_qkv, (1, 0, 2)),
            w_proj,
        ),
        (
            pltpu.VMEM((rows, width), low),
            pltpu.VMEM((3, width, local), low),
            pltpu.VMEM((local, width), low),
            attended,
            pltpu.VMEM((rows, width), low),
            pltpu.SemaphoreType.DMA((5,)),
        ),
        limit=51,
    )
    part_came = swap(part_send)
    own_probs, part_keep, up_keep = call(
        second_kernel,
        (probs_half, wide, part),
        "svvvv",
        3 * half * width * local,
        (clip_tokens, positions, grad_placed, triple, w_proj),
        (attended,),
    )
    merged, own_rows = call(
        middle_kernel,
        (part, part),
        "v" * 8,
        100 * half * width,
        (
            b_proj,
            merge_gain,
            merge_bias,
            part_keep,
            part_came,
            patches,
            up_keep,
            up_came,
        ),
    )
    other_rows = swap(own_rows)
    other_merged = swap(merged)
    query_own, key_own, value_own = call(
        own_back_kernel,
        (
            shape((local, half), low),
            shape((local, rows), jnp.float32),
            shape((local, rows), jnp.float32),
        ),
        "vvvv",
        4 * half * width * local,
        (own_rows, w_proj, triple, own_probs),
        (attended,),
    )
    sent = call(
        other_back_kernel,
        (shape((block, rows), low),) * 8,
        "v" * 7,
        4 * half * width * local,
        (other_rows, w_proj, triple, other_probs, query_own, key_own, value_own),
        (attended, pltpu.VMEM((2, 4, block, rows), low)),
    )

    def exchange(sent):
        return [sent[0]] + [flip(sent[q], q << 1) for q in (1, 2, 3)]

    def product(taken, after=()):
        return call(
            product_kernel,
            (shape((block // 2, width), jnp.float32), shape((block // 2, width), low)),
            "v" * 8 + "a" * len(after),
            8 * block * rows * width,
            (*taken, *normed_of, *after),
            (pltpu.VMEM((block, width), jnp.float32),),
        )

    far_taken = exchange(sent[:4])
    near_taken = exchange(sent[4:])
    far_keep, far_send = product(far_taken)
    far_came = flip(far_send, 1)
    far_sum = (far_keep + far_came.astype(jnp.float32)).astype(low)
    crossing = flip(far_sum, 8)
    near_keep, near_send = product(near_taken, (far_sum,))
    near_came = flip(near_send, 1)
    placed = call(
        place_kernel,
        shape((share_rows, 4 * width), low),
        "svvva",
        8 * rows * share_rows * width,
        (clip_tokens, positions, merged, other_merged, far_sum),
    )
    summed = near_keep + near_came.astype(jnp.float32) + crossing.astype(jnp.float32)
    return (placed, summed[None])


def solution(mesh):
    n_clip, n_seq = mesh.shape["clip"], mesh.shape["seq"]
    fast = n_clip == 2 * 4 * 2 and n_seq == 2
    body = functools.partial(fast_body, n_clip) if fast else general_body
    return jax.shard_map(
        body,
        mesh=mesh,
        in_specs=(
            P("clip", None),
            P("clip"),
            P("clip", None),
            P(),
            P(),
            P(None, None, "seq"),
            P(None, "seq"),
            P("seq", None),
            P(),
            P(),
            P(),
            P(("clip", "seq"), None),
        ),
        out_specs=(P(("clip", "seq"), None), P("seq", "clip", None)),
        check_vma=False,
    )
```

```python
import functools

import jax
import jax.numpy as jnp
from jax import lax
from jax.experimental import pallas as pl
from jax.experimental.pallas import tpu as pltpu
from jax.sharding import PartitionSpec as P


HEAD = 80


EPSILON = 1e-06


def normalize(values, gain_row, bias_row):
    center = values - jnp.mean(values, axis=-1, keepdims=True)
    inverse = lax.rsqrt(jnp.mean(center * center, axis=-1, keepdims=True) + EPSILON)
    unit_rows = center * inverse
    return (unit_rows * gain_row + bias_row, unit_rows, inverse)


def normalize_back(upstream, unit_rows, inverse, gain_row):
    scaled = upstream * gain_row
    return inverse * (
        scaled
        - jnp.mean(scaled, axis=-1, keepdims=True)
        - unit_rows * jnp.mean(scaled * unit_rows, axis=-1, keepdims=True)
    )


def leading(left, right):
    return lax.dot_general(
        left, right, (((0,), (0,)), ((), ())), preferred_element_type=jnp.float32
    )


def trailing(left, right):
    return lax.dot_general(
        left, right, (((1,), (1,)), ((), ())), preferred_element_type=jnp.float32
    )


def general_body(
    patches,
    clip_tokens,
    positions,
    norm_gain,
    norm_bias,
    w_qkv,
    b_qkv,
    w_proj,
    b_proj,
    merge_gain,
    merge_bias,
    grad_placed,
):
    block_rows = patches.shape[0]
    model_width = patches.shape[1]
    local_width = w_qkv.shape[2]
    local_heads = local_width // HEAD
    live_count = clip_tokens[0]
    places = positions[0]
    widened = patches.astype(jnp.float32)
    normed = normalize(widened, norm_gain, norm_bias)[0].astype(jnp.bfloat16)
    triple = jnp.dot(
        normed, w_qkv.reshape(model_width, 3 * local_width), preferred_element_type=jnp.float32
    )
    triple = (triple.reshape(block_rows, 3, local_width) + b_qkv).astype(jnp.bfloat16)
    query_rows = triple[:, 0].reshape(block_rows, local_heads, HEAD)
    key_rows = triple[:, 1].reshape(block_rows, local_heads, HEAD)
    value_rows = triple[:, 2].reshape(block_rows, local_heads, HEAD)
    scaling = HEAD ** (-0.5)
    scores = (
        jnp.einsum("qhd,khd->hqk", query_rows, key_rows, preferred_element_type=jnp.float32)
        * scaling
    )
    live_keys = jnp.arange(block_rows, dtype=jnp.int32) < 4 * live_count
    scores = jnp.where(live_keys[None, None, :], scores, -1e30)
    highest = jnp.max(scores, axis=-1, keepdims=True)
    powers = jnp.exp(scores - highest)
    weights = powers / jnp.sum(powers, axis=-1, keepdims=True)
    weights_low = weights.astype(jnp.bfloat16)
    attended = jnp.einsum(
        "hqk,khd->qhd", weights_low, value_rows, preferred_element_type=jnp.float32
    )
    attended = attended.reshape(block_rows, local_width).astype(jnp.bfloat16)
    partial_value = jnp.dot(attended, w_proj, preferred_element_type=jnp.float32)
    summed_share = lax.psum_scatter(
        partial_value.astype(jnp.bfloat16), "seq", scatter_dimension=0, tiled=True
    ).astype(jnp.float32)
    share_count = summed_share.shape[0]
    own_start = lax.axis_index("seq") * share_count
    own_patches = lax.dynamic_slice_in_dim(widened, own_start, share_count, 0)
    output_share = summed_share + b_proj + own_patches
    output = lax.all_gather(output_share.astype(jnp.bfloat16), "seq", axis=0, tiled=True).astype(
        output_share.dtype
    )
    merged_full, unit_rows, inverse = normalize(output, merge_gain, merge_bias)
    merged = merged_full.reshape(block_rows // 4, 4 * model_width).astype(jnp.bfloat16)
    live_tokens = jnp.arange(block_rows // 4, dtype=jnp.int32) < live_count
    share_rows = grad_placed.shape[0]
    rows_here = lax.axis_index("seq") * share_rows + jnp.arange(share_rows, dtype=jnp.int32)
    selector = ((places[None, :] == rows_here[:, None]) & live_tokens[None, :]).astype(jnp.bfloat16)
    placed = jnp.dot(selector, merged, preferred_element_type=jnp.float32).astype(jnp.bfloat16)
    own_grad = leading(selector, grad_placed)
    token_grad = lax.psum(own_grad.astype(jnp.bfloat16), "seq").astype(jnp.float32)
    upstream = token_grad.reshape(block_rows, model_width)
    row_grad = normalize_back(upstream, unit_rows, inverse, merge_gain).astype(jnp.bfloat16)
    attn_grad = lax.dot_general(
        row_grad, w_proj, (((1,), (1,)), ((), ())), preferred_element_type=jnp.float32
    )
    attn_grad = attn_grad.astype(jnp.bfloat16).reshape(block_rows, local_heads, HEAD)
    prob_grad = jnp.einsum(
        "qhd,khd->hqk", attn_grad, value_rows, preferred_element_type=jnp.float32
    )
    value_grad = jnp.einsum(
        "hqk,qhd->khd", weights_low, attn_grad, preferred_element_type=jnp.float32
    )
    score_grad = (
        weights * (prob_grad - jnp.sum(prob_grad * weights, axis=-1, keepdims=True)) * scaling
    )
    score_grad = score_grad.astype(jnp.bfloat16)
    query_grad = jnp.einsum(
        "hqk,khd->qhd", score_grad, key_rows, preferred_element_type=jnp.float32
    )
    key_grad = jnp.einsum(
        "hqk,qhd->khd", score_grad, query_rows, preferred_element_type=jnp.float32
    )
    triple_grad = jnp.stack([query_grad, key_grad, value_grad], axis=1)
    triple_grad = triple_grad.reshape(block_rows, 3 * local_width).astype(jnp.bfloat16)
    full_term = leading(triple_grad, normed)
    summed = lax.psum_scatter(full_term, "clip", scatter_dimension=0, tiled=True)
    return (placed, summed[None])


def place_masks(live_ref, places, share_rows, rows, first_row):
    tokens = places.shape[1]
    token = lax.broadcasted_iota(jnp.int32, (tokens, rows), 0)
    owner = (lax.broadcasted_iota(jnp.int32, (tokens, rows), 1) + first_row) // 4
    spread = jnp.where((token == owner) & (token < live_ref[0]), 1.0, 0.0)
    shifted = jnp.broadcast_to(places.astype(jnp.float32) + 1.0, (8, tokens))
    row = jnp.dot(shifted, spread, precision=lax.Precision.HIGHEST)[:1] - 1.0
    first = lax.axis_index("seq") * share_rows
    window = lax.broadcasted_iota(jnp.int32, (share_rows, rows), 0) + first
    patch = lax.broadcasted_iota(jnp.int32, (share_rows, rows), 1)
    hit = window.astype(jnp.float32) == row
    return [
        jnp.where(hit & (lax.rem(patch, 4) == k), 1.0, 0.0).astype(jnp.bfloat16) for k in range(4)
    ]


def begin(sources, targets, sems, first=0):
    copies = [
        pltpu.make_async_copy(source, target, sems.at[first + k])
        for k, (source, target) in enumerate(zip(sources, targets, strict=True))
    ]
    for copy in copies:
        copy.start()
    return copies


def half_start(half, own):
    seq = lax.axis_index("seq")
    return pl.multiple_of((seq if own else 1 - seq) * half, 128)


def norm_low(patches_ref, gain_ref, bias_ref):
    return normalize(
        patches_ref[...].astype(jnp.float32), gain_ref[...][None, :], bias_ref[...][None, :]
    )[0].astype(jnp.bfloat16)


def pull(live_ref, places_ref, grad_ref, out_ref, own):
    half, width = out_ref.shape
    masks = place_masks(
        live_ref, places_ref[...], grad_ref.shape[0], half, half_start(half, own)
    )
    total = None
    for k in range(4):
        term = leading(masks[k], grad_ref[:, k * width : (k + 1) * width])
        total = term if total is None else total + term
    out_ref[...] = total.astype(out_ref.dtype)


def prepare_kernel(
    live_ref,
    gain_hbm,
    bias_hbm,
    patches_hbm,
    places_hbm,
    grad_hbm,
    normed_hbm,
    send_hbm,
    gain_ref,
    bias_ref,
    patches_ref,
    places_ref,
    grad_ref,
    normed_ref,
    send_ref,
    sems,
):
    came = begin(
        (gain_hbm, bias_hbm, patches_hbm, places_hbm, grad_hbm),
        (gain_ref, bias_ref, patches_ref, places_ref, grad_ref),
        sems,
    )
    for copy in came[:3]:
        copy.wait()
    normed_ref[...] = norm_low(patches_ref, gain_ref, bias_ref)
    went = begin((normed_ref,), (normed_hbm,), sems, 5)
    for copy in came[3:]:
        copy.wait()
    pull(live_ref, places_ref, grad_ref, send_ref, False)
    went += begin((send_ref,), (send_hbm,), sems, 6)
    for copy in went:
        copy.wait()


def place_kernel(live_ref, places_ref, own_ref, other_ref, _, out_ref):
    half, width = own_ref.shape
    share_rows = out_ref.shape[0]
    own = place_masks(live_ref, places_ref[...], share_rows, half, half_start(half, True))
    other = place_masks(live_ref, places_ref[...], share_rows, half, half_start(half, False))
    for k in range(4):
        term = jnp.dot(own[k], own_ref[...], preferred_element_type=jnp.float32)
        term += jnp.dot(other[k], other_ref[...], preferred_element_type=jnp.float32)
        out_ref[:, k * width : (k + 1) * width] = term.astype(out_ref.dtype)


def attend(live_ref, query_ref, pair_ref, probs_ref, attended_ref):
    half, rows = probs_ref.shape[1:]
    live = lax.broadcasted_iota(jnp.int32, (half, rows), 1) < 4 * live_ref[0]
    steep = HEAD ** (-0.5) * 1.4426950408889634
    for h in range(probs_ref.shape[0]):
        cols = slice(h * HEAD, (h + 1) * HEAD)
        scores = trailing(query_ref[:, cols], pair_ref[0, :, cols])
        scores = jnp.where(live, scores, -1e30)
        powers = jnp.exp2((scores - jnp.max(scores, axis=-1, keepdims=True)) * steep)
        weights = powers * (1.0 / jnp.sum(powers, axis=-1, keepdims=True))
        weights = weights.astype(jnp.bfloat16)
        probs_ref[h] = weights
        attended_ref[:, cols] = jnp.dot(
            weights, pair_ref[1, :, cols], preferred_element_type=jnp.float32
        ).astype(jnp.bfloat16)


def first_kernel(
    live_ref,
    b_ref,
    gain_ref,
    bias_ref,
    patches_hbm,
    w_hbm,
    proj_hbm,
    query_ref,
    pair_ref,
    own_ref,
    wq_ref,
    probs_ref,
    send_ref,
    patches_ref,
    w_ref,
    proj_ref,
    attended_ref,
    normed_ref,
    sems,
):
    came = begin(
        (patches_hbm, w_hbm.at[0], w_hbm.at[1], w_hbm.at[2], proj_hbm),
        (patches_ref, wq_ref, w_ref.at[0], w_ref.at[1], proj_ref),
        sems,
    )
    came[0].wait()
    normed_ref[...] = norm_low(patches_ref, gain_ref, bias_ref)
    half = send_ref.shape[0]
    start = half_start(half, False)
    came[1].wait()
    part = jnp.dot(
        normed_ref[pl.ds(start, half), :], wq_ref[...], preferred_element_type=jnp.float32
    )
    query_ref[...] = (part + b_ref[0:1, :]).astype(jnp.bfloat16)
    own_ref[...] = normed_ref[pl.ds(half_start(half, True), half), :]
    for t in (1, 2):
        came[1 + t].wait()
        part = jnp.dot(normed_ref[...], w_ref[t - 1], preferred_element_type=jnp.float32)
        pair_ref[t - 1] = (part + b_ref[t : t + 1, :]).astype(jnp.bfloat16)
    attend(live_ref, query_ref, pair_ref, probs_ref, attended_ref)
    came[4].wait()
    send_ref[...] = jnp.dot(
        attended_ref[...], proj_ref[...], preferred_element_type=jnp.float32
    ).astype(jnp.bfloat16)


def second_kernel(
    live_ref,
    places_ref,
    grad_ref,
    b_ref,
    own_ref,
    w_ref,
    pair_ref,
    proj_ref,
    query_ref,
    probs_ref,
    keep_ref,
    up_ref,
    attended_ref,
):
    pull(live_ref, places_ref, grad_ref, up_ref, True)
    part = jnp.dot(own_ref[...], w_ref[...], preferred_element_type=jnp.float32)
    query_ref[...] = (part + b_ref[0:1, :]).astype(jnp.bfloat16)
    attend(live_ref, query_ref, pair_ref, probs_ref, attended_ref)
    keep_ref[...] = jnp.dot(attended_ref[...], proj_ref[...], preferred_element_type=jnp.float32)


def middle_kernel(
    b_ref,
    gain_ref,
    bias_ref,
    keep_ref,
    came_ref,
    patches_ref,
    up_keep_ref,
    up_came_ref,
    merged_ref,
    back_ref,
):
    half = keep_ref.shape[0]
    gain = gain_ref[...][None, :]
    output = (
        keep_ref[...]
        + came_ref[...].astype(jnp.float32)
        + b_ref[...][None, :]
        + patches_ref[pl.ds(half_start(half, True), half), :].astype(jnp.float32)
    )
    merged, unit_rows, inverse = normalize(output, gain, bias_ref[...][None, :])
    merged_ref[...] = merged.astype(jnp.bfloat16)
    upstream = up_keep_ref[...].astype(jnp.float32) + up_came_ref[...].astype(jnp.float32)
    back_ref[...] = normalize_back(upstream, unit_rows, inverse, gain).astype(jnp.bfloat16)


def attend_back(row_ref, proj_ref, query_ref, pair_ref, probs_ref, back_ref, put):
    back_ref[...] = trailing(row_ref[...], proj_ref[...]).astype(jnp.bfloat16)
    scaling = HEAD ** (-0.5)
    for h in range(probs_ref.shape[0]):
        cols = slice(h * HEAD, (h + 1) * HEAD)
        back = back_ref[:, cols]
        weights = probs_ref[h]
        prob_grad = trailing(back, pair_ref[1, :, cols])
        wide = weights.astype(jnp.float32)
        inner = jnp.sum(prob_grad * wide, axis=-1, keepdims=True)
        score_grad = (wide * (prob_grad - inner)).astype(jnp.bfloat16)
        query_grad = lax.dot_general(
            pair_ref[0, :, cols],
            score_grad,
            (((0,), (1,)), ((), ())),
            preferred_element_type=jnp.float32,
        )
        key_grad = leading(query_ref[:, cols], score_grad)
        put(h, query_grad * scaling, key_grad * scaling, leading(back, weights))


def own_back_kernel(
    row_ref, proj_ref, q_ref, pair_ref, probs_ref, query_ref, key_ref, value_ref, back_ref
):
    def put(h, query_grad, key_grad, value_grad):
        rows = slice(h * HEAD, (h + 1) * HEAD)
        query_ref[rows, :] = query_grad.astype(jnp.bfloat16)
        key_ref[rows, :] = key_grad
        value_ref[rows, :] = value_grad

    attend_back(row_ref, proj_ref, q_ref, pair_ref, probs_ref, back_ref, put)


def other_back_kernel(
    row_ref, proj_ref, q_ref, pair_ref, probs_ref, query_ref, key_ref, value_ref, *refs
):
    outs, (back_ref, slots_ref) = refs[:8], refs[8:]
    half = row_ref.shape[0]
    heads = probs_ref.shape[0]
    per_block = slots_ref.shape[2] // HEAD
    me = lax.axis_index("clip")
    turn = lax.bitwise_and(lax.shift_right_logical(me, 1), 3)
    away = 1 - lax.shift_right_logical(me, 3)
    mine, start = half_start(half, True), half_start(half, False)

    def where(t, h):
        piece = t * heads + h
        block, sub = piece // per_block, piece % per_block
        slot = lax.bitwise_xor(turn, block % 4)
        side = lax.bitwise_xor(away, block // 4)
        return side, slot, slice(sub * HEAD, (sub + 1) * HEAD)

    def put(h, query_grad, key_grad, value_grad):
        rows = slice(h * HEAD, (h + 1) * HEAD)
        side, slot, place = where(0, h)
        slots_ref[side, slot, place, pl.ds(mine, half)] = query_ref[rows, :]
        slots_ref[side, slot, place, pl.ds(start, half)] = query_grad.astype(jnp.bfloat16)
        side, slot, place = where(1, h)
        slots_ref[side, slot, place, :] = (key_ref[rows, :] + key_grad).astype(jnp.bfloat16)
        side, slot, place = where(2, h)
        slots_ref[side, slot, place, :] = (value_ref[rows, :] + value_grad).astype(jnp.bfloat16)

    attend_back(row_ref, proj_ref, q_ref, pair_ref, probs_ref, back_ref, put)
    for k, out_ref in enumerate(outs):
        out_ref[...] = slots_ref[k // 4, k % 4]


def product_kernel(*refs):
    t_refs, n_refs = refs[:4], refs[4:8]
    keep_ref, send_ref, sum_ref = refs[-3:]
    half = keep_ref.shape[0]
    core = lax.bitwise_and(lax.axis_index("clip"), 1)
    total = None
    for t_ref, n_ref in zip(t_refs, n_refs, strict=True):
        term = jnp.dot(t_ref[...], n_ref[...], preferred_element_type=jnp.float32)
        total = term if total is None else total + term
    sum_ref[...] = total
    keep_ref[...] = sum_ref[pl.ds(pl.multiple_of(core * half, 8), half), :]
    other = sum_ref[pl.ds(pl.multiple_of((1 - core) * half, 8), half), :]
    send_ref[...] = other.astype(jnp.bfloat16)


def call(kernel, outs, kinds, flops, args, scratch=(), limit=30, out_kind="v"):
    spec = {
        "s": pl.BlockSpec(memory_space=pltpu.SMEM),
        "v": pl.BlockSpec(memory_space=pltpu.VMEM),
        "a": pl.BlockSpec(memory_space=pl.ANY),
    }
    return pl.pallas_call(
        kernel,
        out_shape=outs,
        in_specs=[spec[kind] for kind in kinds],
        out_specs=jax.tree.map(lambda _: spec[out_kind], outs),
        scratch_shapes=list(scratch),
        cost_estimate=pl.CostEstimate(flops=flops, bytes_accessed=4_000_000, transcendentals=0),
        compiler_params=pltpu.CompilerParams(vmem_limit_bytes=limit * 1024 * 1024),
    )(*args)


def fast_body(
    n_clip,
    patches,
    clip_tokens,
    positions,
    norm_gain,
    norm_bias,
    w_qkv,
    b_qkv,
    w_proj,
    b_proj,
    merge_gain,
    merge_bias,
    grad_placed,
):
    rows, width = patches.shape
    local = w_qkv.shape[2]
    heads = local // HEAD
    share_rows = grad_placed.shape[0]
    low = jnp.bfloat16
    shape = jax.ShapeDtypeStruct
    full = shape((rows, width), low)

    def swap(value):
        return lax.ppermute(value, "seq", [(0, 1), (1, 0)])

    def flip(value, bits):
        return lax.ppermute(value, "clip", [(i, i ^ bits) for i in range(n_clip)])

    half = rows // 2
    part, wide = shape((half, width), low), shape((half, width), jnp.float32)
    probs_half = shape((heads, half, rows), low)
    query = shape((half, local), low)
    attended = pltpu.VMEM((half, local), low)
    block = 3 * local // 8
    normed, up_send = call(
        prepare_kernel,
        (full, part),
        "saaaaa",
        8 * rows * share_rows * width,
        (clip_tokens, norm_gain, norm_bias, patches, positions, grad_placed),
        (
            pltpu.VMEM(norm_gain.shape, jnp.float32),
            pltpu.VMEM(norm_bias.shape, jnp.float32),
            pltpu.VMEM((rows, width), low),
            pltpu.VMEM(positions.shape, jnp.int32),
            pltpu.VMEM(grad_placed.shape, low),
            pltpu.VMEM((rows, width), low),
            pltpu.VMEM((half, width), low),
            pltpu.SemaphoreType.DMA((7,)),
        ),
        limit=62,
        out_kind="a",
    )
    up_came = swap(up_send)
    normed_of = [normed] + [flip(normed, q << 1) for q in (1, 2)]
    normed_of += [flip(normed, 3 << 1)]
    other_query, pair, own_normed, w_query, other_probs, part_send = call(
        first_kernel,
        (query, shape((2, rows, local), low), part, shape((width, local), low), probs_half, part),
        "svvvaaa",
        7 * rows * width * local,
        (
            clip_tokens,
            b_qkv,
            norm_gain,
            norm_bias,
            patches,
            jnp.transpose(w_qkv, (1, 0, 2)),
            w_proj,
        ),
        (
            pltpu.VMEM((rows, width), low),
            pltpu.VMEM((2, width, local), low),
            pltpu.VMEM((local, width), low),
            attended,
            pltpu.VMEM((rows, width), low),
            pltpu.SemaphoreType.DMA((5,)),
        ),
        limit=49,
    )
    part_came = swap(part_send)
    own_query, own_probs, part_keep, up_keep = call(
        second_kernel,
        (query, probs_half, wide, part),
        "svvvvvvv",
        5 * half * width * local,
        (
            clip_tokens,
            positions,
            grad_placed,
            b_qkv,
            own_normed,
            w_query,
            pair,
            w_proj,
        ),
        (attended,),
    )
    merged, own_rows = call(
        middle_kernel,
        (part, part),
        "v" * 8,
        100 * half * width,
        (
            b_proj,
            merge_gain,
            merge_bias,
            part_keep,
            part_came,
            patches,
            up_keep,
            up_came,
        ),
    )
    other_rows = swap(own_rows)
    other_merged = swap(merged)
    query_own, key_own, value_own = call(
        own_back_kernel,
        (
            shape((local, half), low),
            shape((local, rows), jnp.float32),
            shape((local, rows), jnp.float32),
        ),
        "vvvvv",
        4 * half * width * local,
        (own_rows, w_proj, own_query, pair, own_probs),
        (attended,),
    )
    sent = call(
        other_back_kernel,
        (shape((block, rows), low),) * 8,
        "v" * 8,
        4 * half * width * local,
        (
            other_rows,
            w_proj,
            other_query,
            pair,
            other_probs,
            query_own,
            key_own,
            value_own,
        ),
        (attended, pltpu.VMEM((2, 4, block, rows), low)),
    )

    def exchange(sent):
        return [sent[0]] + [flip(sent[q], q << 1) for q in (1, 2, 3)]

    def product(taken, after=()):
        return call(
            product_kernel,
            (shape((block // 2, width), jnp.float32), shape((block // 2, width), low)),
            "v" * 8 + "a" * len(after),
            8 * block * rows * width,
            (*taken, *normed_of, *after),
            (pltpu.VMEM((block, width), jnp.float32),),
        )

    far_taken = exchange(sent[:4])
    near_taken = exchange(sent[4:])
    far_keep, far_send = product(far_taken)
    far_came = flip(far_send, 1)
    far_sum = (far_keep + far_came.astype(jnp.float32)).astype(low)
    crossing = flip(far_sum, 8)
    near_keep, near_send = product(near_taken, (far_sum,))
    near_came = flip(near_send, 1)
    placed = call(
        place_kernel,
        shape((share_rows, 4 * width), low),
        "svvva",
        8 * rows * share_rows * width,
        (clip_tokens, positions, merged, other_merged, far_sum),
    )
    summed = near_keep + near_came.astype(jnp.float32) + crossing.astype(jnp.float32)
    return (placed, summed[None])


def solution(mesh):
    n_clip, n_seq = mesh.shape["clip"], mesh.shape["seq"]
    fast = n_clip == 2 * 4 * 2 and n_seq == 2
    body = functools.partial(fast_body, n_clip) if fast else general_body
    return jax.shard_map(
        body,
        mesh=mesh,
        in_specs=(
            P("clip", None),
            P("clip"),
            P("clip", None),
            P(),
            P(),
            P(None, None, "seq"),
            P(None, "seq"),
            P("seq", None),
            P(),
            P(),
            P(),
            P(("clip", "seq"), None),
        ),
        out_specs=(P(("clip", "seq"), None), P("seq", "clip", None)),
        check_vma=False,
    )
```

```python
import functools

import jax
import jax.numpy as jnp
from jax import lax
from jax.experimental import pallas as pl
from jax.experimental.pallas import tpu as pltpu
from jax.sharding import PartitionSpec as P


HEAD = 80


EPSILON = 1e-06


def normalize(values, gain_row, bias_row):
    center = values - jnp.mean(values, axis=-1, keepdims=True)
    inverse = lax.rsqrt(jnp.mean(center * center, axis=-1, keepdims=True) + EPSILON)
    unit_rows = center * inverse
    return (unit_rows * gain_row + bias_row, unit_rows, inverse)


def normalize_back(upstream, unit_rows, inverse, gain_row):
    scaled = upstream * gain_row
    return inverse * (
        scaled
        - jnp.mean(scaled, axis=-1, keepdims=True)
        - unit_rows * jnp.mean(scaled * unit_rows, axis=-1, keepdims=True)
    )


def leading(left, right):
    return lax.dot_general(
        left, right, (((0,), (0,)), ((), ())), preferred_element_type=jnp.float32
    )


def trailing(left, right):
    return lax.dot_general(
        left, right, (((1,), (1,)), ((), ())), preferred_element_type=jnp.float32
    )


def general_body(
    patches,
    clip_tokens,
    positions,
    norm_gain,
    norm_bias,
    w_qkv,
    b_qkv,
    w_proj,
    b_proj,
    merge_gain,
    merge_bias,
    grad_placed,
):
    block_rows = patches.shape[0]
    model_width = patches.shape[1]
    local_width = w_qkv.shape[2]
    local_heads = local_width // HEAD
    live_count = clip_tokens[0]
    places = positions[0]
    widened = patches.astype(jnp.float32)
    normed = normalize(widened, norm_gain, norm_bias)[0].astype(jnp.bfloat16)
    triple = jnp.dot(
        normed, w_qkv.reshape(model_width, 3 * local_width), preferred_element_type=jnp.float32
    )
    triple = (triple.reshape(block_rows, 3, local_width) + b_qkv).astype(jnp.bfloat16)
    query_rows = triple[:, 0].reshape(block_rows, local_heads, HEAD)
    key_rows = triple[:, 1].reshape(block_rows, local_heads, HEAD)
    value_rows = triple[:, 2].reshape(block_rows, local_heads, HEAD)
    scaling = HEAD ** (-0.5)
    scores = (
        jnp.einsum("qhd,khd->hqk", query_rows, key_rows, preferred_element_type=jnp.float32)
        * scaling
    )
    live_keys = jnp.arange(block_rows, dtype=jnp.int32) < 4 * live_count
    scores = jnp.where(live_keys[None, None, :], scores, -1e30)
    highest = jnp.max(scores, axis=-1, keepdims=True)
    powers = jnp.exp(scores - highest)
    weights = powers / jnp.sum(powers, axis=-1, keepdims=True)
    weights_low = weights.astype(jnp.bfloat16)
    attended = jnp.einsum(
        "hqk,khd->qhd", weights_low, value_rows, preferred_element_type=jnp.float32
    )
    attended = attended.reshape(block_rows, local_width).astype(jnp.bfloat16)
    partial_value = jnp.dot(attended, w_proj, preferred_element_type=jnp.float32)
    summed_share = lax.psum_scatter(
        partial_value.astype(jnp.bfloat16), "seq", scatter_dimension=0, tiled=True
    ).astype(jnp.float32)
    share_count = summed_share.shape[0]
    own_start = lax.axis_index("seq") * share_count
    own_patches = lax.dynamic_slice_in_dim(widened, own_start, share_count, 0)
    output_share = summed_share + b_proj + own_patches
    output = lax.all_gather(output_share.astype(jnp.bfloat16), "seq", axis=0, tiled=True).astype(
        output_share.dtype
    )
    merged_full, unit_rows, inverse = normalize(output, merge_gain, merge_bias)
    merged = merged_full.reshape(block_rows // 4, 4 * model_width).astype(jnp.bfloat16)
    live_tokens = jnp.arange(block_rows // 4, dtype=jnp.int32) < live_count
    share_rows = grad_placed.shape[0]
    rows_here = lax.axis_index("seq") * share_rows + jnp.arange(share_rows, dtype=jnp.int32)
    selector = ((places[None, :] == rows_here[:, None]) & live_tokens[None, :]).astype(jnp.bfloat16)
    placed = jnp.dot(selector, merged, preferred_element_type=jnp.float32).astype(jnp.bfloat16)
    own_grad = leading(selector, grad_placed)
    token_grad = lax.psum(own_grad.astype(jnp.bfloat16), "seq").astype(jnp.float32)
    upstream = token_grad.reshape(block_rows, model_width)
    row_grad = normalize_back(upstream, unit_rows, inverse, merge_gain).astype(jnp.bfloat16)
    attn_grad = lax.dot_general(
        row_grad, w_proj, (((1,), (1,)), ((), ())), preferred_element_type=jnp.float32
    )
    attn_grad = attn_grad.astype(jnp.bfloat16).reshape(block_rows, local_heads, HEAD)
    prob_grad = jnp.einsum(
        "qhd,khd->hqk", attn_grad, value_rows, preferred_element_type=jnp.float32
    )
    value_grad = jnp.einsum(
        "hqk,qhd->khd", weights_low, attn_grad, preferred_element_type=jnp.float32
    )
    score_grad = (
        weights * (prob_grad - jnp.sum(prob_grad * weights, axis=-1, keepdims=True)) * scaling
    )
    score_grad = score_grad.astype(jnp.bfloat16)
    query_grad = jnp.einsum(
        "hqk,khd->qhd", score_grad, key_rows, preferred_element_type=jnp.float32
    )
    key_grad = jnp.einsum(
        "hqk,qhd->khd", score_grad, query_rows, preferred_element_type=jnp.float32
    )
    triple_grad = jnp.stack([query_grad, key_grad, value_grad], axis=1)
    triple_grad = triple_grad.reshape(block_rows, 3 * local_width).astype(jnp.bfloat16)
    full_term = leading(triple_grad, normed)
    summed = lax.psum_scatter(full_term, "clip", scatter_dimension=0, tiled=True)
    return (placed, summed[None])


def place_masks(live_ref, places, share_rows, rows, first_row):
    tokens = places.shape[1]
    token = lax.broadcasted_iota(jnp.int32, (tokens, rows), 0)
    owner = (lax.broadcasted_iota(jnp.int32, (tokens, rows), 1) + first_row) // 4
    spread = jnp.where((token == owner) & (token < live_ref[0]), 1.0, 0.0)
    shifted = jnp.broadcast_to(places.astype(jnp.float32) + 1.0, (8, tokens))
    row = jnp.dot(shifted, spread, precision=lax.Precision.HIGHEST)[:1] - 1.0
    first = lax.axis_index("seq") * share_rows
    window = lax.broadcasted_iota(jnp.int32, (share_rows, rows), 0) + first
    patch = lax.broadcasted_iota(jnp.int32, (share_rows, rows), 1)
    hit = window.astype(jnp.float32) == row
    return [
        jnp.where(hit & (lax.rem(patch, 4) == k), 1.0, 0.0).astype(jnp.bfloat16) for k in range(4)
    ]


def begin(sources, targets, sems, first=0):
    copies = [
        pltpu.make_async_copy(source, target, sems.at[first + k])
        for k, (source, target) in enumerate(zip(sources, targets, strict=True))
    ]
    for copy in copies:
        copy.start()
    return copies


def half_start(half, own):
    seq = lax.axis_index("seq")
    return pl.multiple_of((seq if own else 1 - seq) * half, 128)


def norm_low(patches_ref, gain_ref, bias_ref):
    return normalize(
        patches_ref[...].astype(jnp.float32), gain_ref[...][None, :], bias_ref[...][None, :]
    )[0].astype(jnp.bfloat16)


def pull(live_ref, places_ref, grad_ref, out_ref, own):
    half, width = out_ref.shape
    masks = place_masks(
        live_ref, places_ref[...], grad_ref.shape[0], half, half_start(half, own)
    )
    total = None
    for k in range(4):
        term = leading(masks[k], grad_ref[:, k * width : (k + 1) * width])
        total = term if total is None else total + term
    out_ref[...] = total.astype(out_ref.dtype)


def pull_kernel(live_ref, places_hbm, grad_hbm, send_hbm, places_ref, grad_ref, send_ref, sems):
    came = begin((places_hbm, grad_hbm), (places_ref, grad_ref), sems)
    for copy in came:
        copy.wait()
    pull(live_ref, places_ref, grad_ref, send_ref, False)
    begin((send_ref,), (send_hbm,), sems, 2)[0].wait()


def norm_kernel(gain_ref, bias_ref, patches_ref, normed_ref):
    normed_ref[...] = norm_low(patches_ref, gain_ref, bias_ref)


def place_kernel(live_ref, places_ref, own_ref, other_ref, _, out_ref):
    half, width = own_ref.shape
    share_rows = out_ref.shape[0]
    own = place_masks(live_ref, places_ref[...], share_rows, half, half_start(half, True))
    other = place_masks(live_ref, places_ref[...], share_rows, half, half_start(half, False))
    for k in range(4):
        term = jnp.dot(own[k], own_ref[...], preferred_element_type=jnp.float32)
        term += jnp.dot(other[k], other_ref[...], preferred_element_type=jnp.float32)
        out_ref[:, k * width : (k + 1) * width] = term.astype(out_ref.dtype)


def attend(live_ref, query_ref, pair_ref, probs_ref, attended_ref):
    half, rows = probs_ref.shape[1:]
    live = lax.broadcasted_iota(jnp.int32, (half, rows), 1) < 4 * live_ref[0]
    steep = HEAD ** (-0.5) * 1.4426950408889634
    for h in range(probs_ref.shape[0]):
        cols = slice(h * HEAD, (h + 1) * HEAD)
        scores = trailing(query_ref[:, cols], pair_ref[0, :, cols])
        scores = jnp.where(live, scores, -1e30)
        powers = jnp.exp2((scores - jnp.max(scores, axis=-1, keepdims=True)) * steep)
        weights = powers * (1.0 / jnp.sum(powers, axis=-1, keepdims=True))
        weights = weights.astype(jnp.bfloat16)
        probs_ref[h] = weights
        attended_ref[:, cols] = jnp.dot(
            weights, pair_ref[1, :, cols], preferred_element_type=jnp.float32
        ).astype(jnp.bfloat16)


def first_kernel(
    live_ref,
    b_ref,
    normed_ref,
    w_hbm,
    proj_hbm,
    query_ref,
    pair_ref,
    own_ref,
    wq_ref,
    probs_ref,
    send_ref,
    w_ref,
    proj_ref,
    attended_ref,
    sems,
):
    came = begin(
        (w_hbm.at[0], w_hbm.at[1], w_hbm.at[2], proj_hbm),
        (wq_ref, w_ref.at[0], w_ref.at[1], proj_ref),
        sems,
    )
    half = send_ref.shape[0]
    start = half_start(half, False)
    own_ref[...] = normed_ref[pl.ds(half_start(half, True), half), :]
    came[0].wait()
    part = jnp.dot(
        normed_ref[pl.ds(start, half), :], wq_ref[...], preferred_element_type=jnp.float32
    )
    query_ref[...] = (part + b_ref[0:1, :]).astype(jnp.bfloat16)
    for t in (1, 2):
        came[t].wait()
        part = jnp.dot(normed_ref[...], w_ref[t - 1], preferred_element_type=jnp.float32)
        pair_ref[t - 1] = (part + b_ref[t : t + 1, :]).astype(jnp.bfloat16)
    attend(live_ref, query_ref, pair_ref, probs_ref, attended_ref)
    came[3].wait()
    send_ref[...] = jnp.dot(
        attended_ref[...], proj_ref[...], preferred_element_type=jnp.float32
    ).astype(jnp.bfloat16)


def second_kernel(
    live_ref,
    places_ref,
    grad_ref,
    b_ref,
    own_ref,
    w_ref,
    pair_ref,
    proj_ref,
    query_ref,
    probs_ref,
    keep_ref,
    up_ref,
    attended_ref,
):
    pull(live_ref, places_ref, grad_ref, up_ref, True)
    part = jnp.dot(own_ref[...], w_ref[...], preferred_element_type=jnp.float32)
    query_ref[...] = (part + b_ref[0:1, :]).astype(jnp.bfloat16)
    attend(live_ref, query_ref, pair_ref, probs_ref, attended_ref)
    keep_ref[...] = jnp.dot(attended_ref[...], proj_ref[...], preferred_element_type=jnp.float32)


def middle_kernel(
    b_ref,
    gain_ref,
    bias_ref,
    keep_ref,
    came_ref,
    patches_ref,
    up_keep_ref,
    up_came_ref,
    merged_ref,
    back_ref,
):
    half = keep_ref.shape[0]
    gain = gain_ref[...][None, :]
    output = (
        keep_ref[...]
        + came_ref[...].astype(jnp.float32)
        + b_ref[...][None, :]
        + patches_ref[pl.ds(half_start(half, True), half), :].astype(jnp.float32)
    )
    merged, unit_rows, inverse = normalize(output, gain, bias_ref[...][None, :])
    merged_ref[...] = merged.astype(jnp.bfloat16)
    upstream = up_keep_ref[...].astype(jnp.float32) + up_came_ref[...].astype(jnp.float32)
    back_ref[...] = normalize_back(upstream, unit_rows, inverse, gain).astype(jnp.bfloat16)


def attend_back(row_ref, proj_ref, query_ref, pair_ref, probs_ref, back_ref, put):
    back_ref[...] = trailing(row_ref[...], proj_ref[...]).astype(jnp.bfloat16)
    scaling = HEAD ** (-0.5)
    for h in range(probs_ref.shape[0]):
        cols = slice(h * HEAD, (h + 1) * HEAD)
        back = back_ref[:, cols]
        weights = probs_ref[h]
        prob_grad = trailing(back, pair_ref[1, :, cols])
        wide = weights.astype(jnp.float32)
        inner = jnp.sum(prob_grad * wide, axis=-1, keepdims=True)
        score_grad = (wide * (prob_grad - inner)).astype(jnp.bfloat16)
        query_grad = lax.dot_general(
            pair_ref[0, :, cols],
            score_grad,
            (((0,), (1,)), ((), ())),
            preferred_element_type=jnp.float32,
        )
        key_grad = leading(query_ref[:, cols], score_grad)
        put(h, query_grad * scaling, key_grad * scaling, leading(back, weights))


def own_back_kernel(
    row_ref, proj_ref, q_ref, pair_ref, probs_ref, query_ref, key_ref, value_ref, back_ref
):
    def put(h, query_grad, key_grad, value_grad):
        rows = slice(h * HEAD, (h + 1) * HEAD)
        query_ref[rows, :] = query_grad.astype(jnp.bfloat16)
        key_ref[rows, :] = key_grad
        value_ref[rows, :] = value_grad

    attend_back(row_ref, proj_ref, q_ref, pair_ref, probs_ref, back_ref, put)


def other_back_kernel(
    row_ref, proj_ref, q_ref, pair_ref, probs_ref, query_ref, key_ref, value_ref, *refs
):
    outs, (back_ref, slots_ref) = refs[:8], refs[8:]
    half = row_ref.shape[0]
    heads = probs_ref.shape[0]
    per_block = slots_ref.shape[2] // HEAD
    me = lax.axis_index("clip")
    turn = lax.bitwise_and(lax.shift_right_logical(me, 1), 3)
    away = 1 - lax.shift_right_logical(me, 3)
    mine, start = half_start(half, True), half_start(half, False)

    def where(t, h):
        piece = t * heads + h
        block, sub = piece // per_block, piece % per_block
        slot = lax.bitwise_xor(turn, block % 4)
        side = lax.bitwise_xor(away, block // 4)
        return side, slot, slice(sub * HEAD, (sub + 1) * HEAD)

    def put(h, query_grad, key_grad, value_grad):
        rows = slice(h * HEAD, (h + 1) * HEAD)
        side, slot, place = where(0, h)
        slots_ref[side, slot, place, pl.ds(mine, half)] = query_ref[rows, :]
        slots_ref[side, slot, place, pl.ds(start, half)] = query_grad.astype(jnp.bfloat16)
        side, slot, place = where(1, h)
        slots_ref[side, slot, place, :] = (key_ref[rows, :] + key_grad).astype(jnp.bfloat16)
        side, slot, place = where(2, h)
        slots_ref[side, slot, place, :] = (value_ref[rows, :] + value_grad).astype(jnp.bfloat16)

    attend_back(row_ref, proj_ref, q_ref, pair_ref, probs_ref, back_ref, put)
    for k, out_ref in enumerate(outs):
        out_ref[...] = slots_ref[k // 4, k % 4]


def product_kernel(t0, t1, t2, t3, n0, n1, n2, n3_low, n3_high, *refs):
    keep_ref, send_ref, sum_ref = refs[-3:]
    half = keep_ref.shape[0]
    core = lax.bitwise_and(lax.axis_index("clip"), 1)
    cut = n3_low.shape[0]
    total = None
    for t, n in (
        (t0[...], n0),
        (t1[...], n1),
        (t2[...], n2),
        (t3[:, :cut], n3_low),
        (t3[:, cut:], n3_high),
    ):
        term = jnp.dot(t, n[...], preferred_element_type=jnp.float32)
        total = term if total is None else total + term
    sum_ref[...] = total
    keep_ref[...] = sum_ref[pl.ds(pl.multiple_of(core * half, 8), half), :]
    other = sum_ref[pl.ds(pl.multiple_of((1 - core) * half, 8), half), :]
    send_ref[...] = other.astype(jnp.bfloat16)


def call(kernel, outs, kinds, flops, args, scratch=(), limit=30, out_kind="v"):
    spec = {
        "s": pl.BlockSpec(memory_space=pltpu.SMEM),
        "v": pl.BlockSpec(memory_space=pltpu.VMEM),
        "a": pl.BlockSpec(memory_space=pl.ANY),
    }
    return pl.pallas_call(
        kernel,
        out_shape=outs,
        in_specs=[spec[kind] for kind in kinds],
        out_specs=jax.tree.map(lambda _: spec[out_kind], outs),
        scratch_shapes=list(scratch),
        cost_estimate=pl.CostEstimate(flops=flops, bytes_accessed=4_000_000, transcendentals=0),
        compiler_params=pltpu.CompilerParams(vmem_limit_bytes=limit * 1024 * 1024),
    )(*args)


def fast_body(
    n_clip,
    patches,
    clip_tokens,
    positions,
    norm_gain,
    norm_bias,
    w_qkv,
    b_qkv,
    w_proj,
    b_proj,
    merge_gain,
    merge_bias,
    grad_placed,
):
    rows, width = patches.shape
    local = w_qkv.shape[2]
    heads = local // HEAD
    share_rows = grad_placed.shape[0]
    low = jnp.bfloat16
    shape = jax.ShapeDtypeStruct
    full = shape((rows, width), low)

    def swap(value):
        return lax.ppermute(value, "seq", [(0, 1), (1, 0)])

    def flip(value, bits):
        return lax.ppermute(value, "clip", [(i, i ^ bits) for i in range(n_clip)])

    half = rows // 2
    part, wide = shape((half, width), low), shape((half, width), jnp.float32)
    probs_half = shape((heads, half, rows), low)
    query = shape((half, local), low)
    attended = pltpu.VMEM((half, local), low)
    block = 3 * local // 8
    up_send = call(
        pull_kernel,
        part,
        "saa",
        4 * rows * share_rows * width,
        (clip_tokens, positions, grad_placed),
        (
            pltpu.VMEM(positions.shape, jnp.int32),
            pltpu.VMEM(grad_placed.shape, low),
            pltpu.VMEM((half, width), low),
            pltpu.SemaphoreType.DMA((3,)),
        ),
        limit=62,
        out_kind="a",
    )
    up_came = swap(up_send)
    normed = call(norm_kernel, full, "vvv", 100 * rows * width, (norm_gain, norm_bias, patches))
    normed_of = [normed] + [flip(normed, q << 1) for q in (1, 2)]
    normed_of += [flip(normed_of[2][:half], 1 << 1), flip(normed_of[1][half:], 2 << 1)]
    other_query, pair, own_normed, w_query, other_probs, part_send = call(
        first_kernel,
        (query, shape((2, rows, local), low), part, shape((width, local), low), probs_half, part),
        "svvaa",
        7 * rows * width * local,
        (
            clip_tokens,
            b_qkv,
            normed,
            jnp.transpose(w_qkv, (1, 0, 2)),
            w_proj,
        ),
        (
            pltpu.VMEM((2, width, local), low),
            pltpu.VMEM((local, width), low),
            attended,
            pltpu.SemaphoreType.DMA((4,)),
        ),
        limit=49,
    )
    part_came = swap(part_send)
    own_query, own_probs, part_keep, up_keep = call(
        second_kernel,
        (query, probs_half, wide, part),
        "svvvvvvv",
        5 * half * width * local,
        (
            clip_tokens,
            positions,
            grad_placed,
            b_qkv,
            own_normed,
            w_query,
            pair,
            w_proj,
        ),
        (attended,),
    )
    merged, own_rows = call(
        middle_kernel,
        (part, part),
        "v" * 8,
        100 * half * width,
        (
            b_proj,
            merge_gain,
            merge_bias,
            part_keep,
            part_came,
            patches,
            up_keep,
            up_came,
        ),
    )
    other_rows = swap(own_rows)
    other_merged = swap(merged)
    query_own, key_own, value_own = call(
        own_back_kernel,
        (
            shape((local, half), low),
            shape((local, rows), jnp.float32),
            shape((local, rows), jnp.float32),
        ),
        "vvvvv",
        4 * half * width * local,
        (own_rows, w_proj, own_query, pair, own_probs),
        (attended,),
    )
    sent = call(
        other_back_kernel,
        (shape((block, rows), low),) * 8,
        "v" * 8,
        4 * half * width * local,
        (
            other_rows,
            w_proj,
            other_query,
            pair,
            other_probs,
            query_own,
            key_own,
            value_own,
        ),
        (attended, pltpu.VMEM((2, 4, block, rows), low)),
    )

    def exchange(sent):
        diagonal = flip(sent[3], 3 << 1)
        return [sent[0]] + [flip(sent[q], q << 1) for q in (1, 2)] + [diagonal]

    def product(taken, after=()):
        return call(
            product_kernel,
            (shape((block // 2, width), jnp.float32), shape((block // 2, width), low)),
            "v" * 9 + "a" * len(after),
            8 * block * rows * width,
            (*taken, *normed_of, *after),
            (pltpu.VMEM((block, width), jnp.float32),),
        )

    far_taken = exchange(sent[:4])
    near_taken = exchange(sent[4:])
    far_keep, far_send = product(far_taken)
    far_came = flip(far_send, 1)
    far_sum = (far_keep + far_came.astype(jnp.float32)).astype(low)
    crossing = flip(far_sum, 8)
    near_keep, near_send = product(near_taken, (far_sum,))
    near_came = flip(near_send, 1)
    placed = call(
        place_kernel,
        shape((share_rows, 4 * width), low),
        "svvva",
        8 * rows * share_rows * width,
        (clip_tokens, positions, merged, other_merged, far_sum),
    )
    summed = near_keep + near_came.astype(jnp.float32) + crossing.astype(jnp.float32)
    return (placed, summed[None])


def solution(mesh):
    n_clip, n_seq = mesh.shape["clip"], mesh.shape["seq"]
    fast = n_clip == 2 * 4 * 2 and n_seq == 2
    body = functools.partial(fast_body, n_clip) if fast else general_body
    return jax.shard_map(
        body,
        mesh=mesh,
        in_specs=(
            P("clip", None),
            P("clip"),
            P("clip", None),
            P(),
            P(),
            P(None, None, "seq"),
            P(None, "seq"),
            P("seq", None),
            P(),
            P(),
            P(),
            P(("clip", "seq"), None),
        ),
        out_specs=(P(("clip", "seq"), None), P("seq", "clip", None)),
        check_vma=False,
    )
```

```python
import functools

import jax
import jax.numpy as jnp
from jax import lax
from jax.experimental import pallas as pl
from jax.experimental.pallas import tpu as pltpu
from jax.sharding import PartitionSpec as P


HEAD = 80


EPSILON = 1e-06


def normalize(values, gain_row, bias_row):
    center = values - jnp.mean(values, axis=-1, keepdims=True)
    inverse = lax.rsqrt(jnp.mean(center * center, axis=-1, keepdims=True) + EPSILON)
    unit_rows = center * inverse
    return (unit_rows * gain_row + bias_row, unit_rows, inverse)


def normalize_back(upstream, unit_rows, inverse, gain_row):
    scaled = upstream * gain_row
    return inverse * (
        scaled
        - jnp.mean(scaled, axis=-1, keepdims=True)
        - unit_rows * jnp.mean(scaled * unit_rows, axis=-1, keepdims=True)
    )


def leading(left, right):
    return lax.dot_general(
        left, right, (((0,), (0,)), ((), ())), preferred_element_type=jnp.float32
    )


def trailing(left, right):
    return lax.dot_general(
        left, right, (((1,), (1,)), ((), ())), preferred_element_type=jnp.float32
    )


def general_body(
    patches,
    clip_tokens,
    positions,
    norm_gain,
    norm_bias,
    w_qkv,
    b_qkv,
    w_proj,
    b_proj,
    merge_gain,
    merge_bias,
    grad_placed,
):
    block_rows = patches.shape[0]
    model_width = patches.shape[1]
    local_width = w_qkv.shape[2]
    local_heads = local_width // HEAD
    live_count = clip_tokens[0]
    places = positions[0]
    widened = patches.astype(jnp.float32)
    normed = normalize(widened, norm_gain, norm_bias)[0].astype(jnp.bfloat16)
    triple = jnp.dot(
        normed, w_qkv.reshape(model_width, 3 * local_width), preferred_element_type=jnp.float32
    )
    triple = (triple.reshape(block_rows, 3, local_width) + b_qkv).astype(jnp.bfloat16)
    query_rows = triple[:, 0].reshape(block_rows, local_heads, HEAD)
    key_rows = triple[:, 1].reshape(block_rows, local_heads, HEAD)
    value_rows = triple[:, 2].reshape(block_rows, local_heads, HEAD)
    scaling = HEAD ** (-0.5)
    scores = (
        jnp.einsum("qhd,khd->hqk", query_rows, key_rows, preferred_element_type=jnp.float32)
        * scaling
    )
    live_keys = jnp.arange(block_rows, dtype=jnp.int32) < 4 * live_count
    scores = jnp.where(live_keys[None, None, :], scores, -1e30)
    highest = jnp.max(scores, axis=-1, keepdims=True)
    powers = jnp.exp(scores - highest)
    weights = powers / jnp.sum(powers, axis=-1, keepdims=True)
    weights_low = weights.astype(jnp.bfloat16)
    attended = jnp.einsum(
        "hqk,khd->qhd", weights_low, value_rows, preferred_element_type=jnp.float32
    )
    attended = attended.reshape(block_rows, local_width).astype(jnp.bfloat16)
    partial_value = jnp.dot(attended, w_proj, preferred_element_type=jnp.float32)
    summed_share = lax.psum_scatter(
        partial_value.astype(jnp.bfloat16), "seq", scatter_dimension=0, tiled=True
    ).astype(jnp.float32)
    share_count = summed_share.shape[0]
    own_start = lax.axis_index("seq") * share_count
    own_patches = lax.dynamic_slice_in_dim(widened, own_start, share_count, 0)
    output_share = summed_share + b_proj + own_patches
    output = lax.all_gather(output_share.astype(jnp.bfloat16), "seq", axis=0, tiled=True).astype(
        output_share.dtype
    )
    merged_full, unit_rows, inverse = normalize(output, merge_gain, merge_bias)
    merged = merged_full.reshape(block_rows // 4, 4 * model_width).astype(jnp.bfloat16)
    live_tokens = jnp.arange(block_rows // 4, dtype=jnp.int32) < live_count
    share_rows = grad_placed.shape[0]
    rows_here = lax.axis_index("seq") * share_rows + jnp.arange(share_rows, dtype=jnp.int32)
    selector = ((places[None, :] == rows_here[:, None]) & live_tokens[None, :]).astype(jnp.bfloat16)
    placed = jnp.dot(selector, merged, preferred_element_type=jnp.float32).astype(jnp.bfloat16)
    own_grad = leading(selector, grad_placed)
    token_grad = lax.psum(own_grad.astype(jnp.bfloat16), "seq").astype(jnp.float32)
    upstream = token_grad.reshape(block_rows, model_width)
    row_grad = normalize_back(upstream, unit_rows, inverse, merge_gain).astype(jnp.bfloat16)
    attn_grad = lax.dot_general(
        row_grad, w_proj, (((1,), (1,)), ((), ())), preferred_element_type=jnp.float32
    )
    attn_grad = attn_grad.astype(jnp.bfloat16).reshape(block_rows, local_heads, HEAD)
    prob_grad = jnp.einsum(
        "qhd,khd->hqk", attn_grad, value_rows, preferred_element_type=jnp.float32
    )
    value_grad = jnp.einsum(
        "hqk,qhd->khd", weights_low, attn_grad, preferred_element_type=jnp.float32
    )
    score_grad = (
        weights * (prob_grad - jnp.sum(prob_grad * weights, axis=-1, keepdims=True)) * scaling
    )
    score_grad = score_grad.astype(jnp.bfloat16)
    query_grad = jnp.einsum(
        "hqk,khd->qhd", score_grad, key_rows, preferred_element_type=jnp.float32
    )
    key_grad = jnp.einsum(
        "hqk,qhd->khd", score_grad, query_rows, preferred_element_type=jnp.float32
    )
    triple_grad = jnp.stack([query_grad, key_grad, value_grad], axis=1)
    triple_grad = triple_grad.reshape(block_rows, 3 * local_width).astype(jnp.bfloat16)
    full_term = leading(triple_grad, normed)
    summed = lax.psum_scatter(full_term, "clip", scatter_dimension=0, tiled=True)
    return (placed, summed[None])


def place_masks(live_ref, places, share_rows, rows, first_row):
    tokens = places.shape[1]
    token = lax.broadcasted_iota(jnp.int32, (tokens, rows), 0)
    owner = (lax.broadcasted_iota(jnp.int32, (tokens, rows), 1) + first_row) // 4
    spread = jnp.where((token == owner) & (token < live_ref[0]), 1.0, 0.0)
    shifted = jnp.broadcast_to(places.astype(jnp.float32) + 1.0, (8, tokens))
    row = jnp.dot(shifted, spread, precision=lax.Precision.HIGHEST)[:1] - 1.0
    first = lax.axis_index("seq") * share_rows
    window = lax.broadcasted_iota(jnp.int32, (share_rows, rows), 0) + first
    patch = lax.broadcasted_iota(jnp.int32, (share_rows, rows), 1)
    hit = window.astype(jnp.float32) == row
    return [
        jnp.where(hit & (lax.rem(patch, 4) == k), 1.0, 0.0).astype(jnp.bfloat16) for k in range(4)
    ]


def begin(sources, targets, sems, first=0):
    copies = [
        pltpu.make_async_copy(source, target, sems.at[first + k])
        for k, (source, target) in enumerate(zip(sources, targets, strict=True))
    ]
    for copy in copies:
        copy.start()
    return copies


def half_start(half, own):
    seq = lax.axis_index("seq")
    return pl.multiple_of((seq if own else 1 - seq) * half, 128)


def norm_low(patches_ref, gain_ref, bias_ref):
    return normalize(
        patches_ref[...].astype(jnp.float32), gain_ref[...][None, :], bias_ref[...][None, :]
    )[0].astype(jnp.bfloat16)


def pull(live_ref, places_ref, grad_ref, out_ref, own):
    half, width = out_ref.shape
    masks = place_masks(
        live_ref, places_ref[...], grad_ref.shape[0], half, half_start(half, own)
    )
    total = None
    for k in range(4):
        term = leading(masks[k], grad_ref[:, k * width : (k + 1) * width])
        total = term if total is None else total + term
    out_ref[...] = total.astype(out_ref.dtype)


def pull_kernel(live_ref, places_hbm, grad_hbm, send_ref, places_ref, grad_ref, sems):
    half, width = send_ref.shape
    came = begin((places_hbm,), (places_ref,), sems)
    blocks = [slice(k * width, (k + 1) * width) for k in range(4)]
    came += begin(
        [grad_hbm.at[:, block] for block in blocks],
        [grad_ref.at[:, block] for block in blocks],
        sems,
        1,
    )
    came[0].wait()
    masks = place_masks(
        live_ref, places_ref[...], grad_ref.shape[0], half, half_start(half, False)
    )
    total = None
    for k in range(4):
        came[1 + k].wait()
        term = leading(masks[k], grad_ref[:, blocks[k]])
        total = term if total is None else total + term
    send_ref[...] = total.astype(send_ref.dtype)


def norm_kernel(gain_ref, bias_ref, patches_ref, normed_ref):
    normed_ref[...] = norm_low(patches_ref, gain_ref, bias_ref)


def place_kernel(live_ref, places_ref, own_ref, other_ref, _, out_ref):
    half, width = own_ref.shape
    share_rows = out_ref.shape[0]
    own = place_masks(live_ref, places_ref[...], share_rows, half, half_start(half, True))
    other = place_masks(live_ref, places_ref[...], share_rows, half, half_start(half, False))
    for k in range(4):
        term = jnp.dot(own[k], own_ref[...], preferred_element_type=jnp.float32)
        term += jnp.dot(other[k], other_ref[...], preferred_element_type=jnp.float32)
        out_ref[:, k * width : (k + 1) * width] = term.astype(out_ref.dtype)


def attend(live_ref, query_ref, pair_ref, probs_ref, attended_ref):
    half, rows = probs_ref.shape[1:]
    live = lax.broadcasted_iota(jnp.int32, (half, rows), 1) < 4 * live_ref[0]
    steep = HEAD ** (-0.5) * 1.4426950408889634
    for h in range(probs_ref.shape[0]):
        cols = slice(h * HEAD, (h + 1) * HEAD)
        scores = trailing(query_ref[:, cols], pair_ref[0, :, cols])
        scores = jnp.where(live, scores, -1e30)
        powers = jnp.exp2((scores - jnp.max(scores, axis=-1, keepdims=True)) * steep)
        weights = powers * (1.0 / jnp.sum(powers, axis=-1, keepdims=True))
        weights = weights.astype(jnp.bfloat16)
        probs_ref[h] = weights
        attended_ref[:, cols] = jnp.dot(
            weights, pair_ref[1, :, cols], preferred_element_type=jnp.float32
        ).astype(jnp.bfloat16)


def first_kernel(
    live_ref,
    b_ref,
    normed_ref,
    w_hbm,
    proj_hbm,
    query_ref,
    pair_ref,
    own_ref,
    wq_ref,
    probs_ref,
    send_ref,
    w_ref,
    proj_ref,
    attended_ref,
    sems,
):
    came = begin(
        (w_hbm.at[0], w_hbm.at[1], w_hbm.at[2], proj_hbm),
        (wq_ref, w_ref.at[0], w_ref.at[1], proj_ref),
        sems,
    )
    half = send_ref.shape[0]
    start = half_start(half, False)
    own_ref[...] = normed_ref[pl.ds(half_start(half, True), half), :]
    came[0].wait()
    part = jnp.dot(
        normed_ref[pl.ds(start, half), :], wq_ref[...], preferred_element_type=jnp.float32
    )
    query_ref[...] = (part + b_ref[0:1, :]).astype(jnp.bfloat16)
    for t in (1, 2):
        came[t].wait()
        part = jnp.dot(normed_ref[...], w_ref[t - 1], preferred_element_type=jnp.float32)
        pair_ref[t - 1] = (part + b_ref[t : t + 1, :]).astype(jnp.bfloat16)
    attend(live_ref, query_ref, pair_ref, probs_ref, attended_ref)
    came[3].wait()
    send_ref[...] = jnp.dot(
        attended_ref[...], proj_ref[...], preferred_element_type=jnp.float32
    ).astype(jnp.bfloat16)


def second_kernel(
    live_ref,
    places_ref,
    grad_ref,
    b_ref,
    own_ref,
    w_ref,
    pair_ref,
    proj_ref,
    query_ref,
    probs_ref,
    keep_ref,
    up_ref,
    attended_ref,
):
    pull(live_ref, places_ref, grad_ref, up_ref, True)
    part = jnp.dot(own_ref[...], w_ref[...], preferred_element_type=jnp.float32)
    query_ref[...] = (part + b_ref[0:1, :]).astype(jnp.bfloat16)
    attend(live_ref, query_ref, pair_ref, probs_ref, attended_ref)
    keep_ref[...] = jnp.dot(attended_ref[...], proj_ref[...], preferred_element_type=jnp.float32)


def middle_kernel(
    b_ref,
    gain_ref,
    bias_ref,
    keep_ref,
    came_ref,
    patches_ref,
    up_keep_ref,
    up_came_ref,
    merged_ref,
    back_ref,
):
    half = keep_ref.shape[0]
    gain = gain_ref[...][None, :]
    output = (
        keep_ref[...]
        + came_ref[...].astype(jnp.float32)
        + b_ref[...][None, :]
        + patches_ref[pl.ds(half_start(half, True), half), :].astype(jnp.float32)
    )
    merged, unit_rows, inverse = normalize(output, gain, bias_ref[...][None, :])
    merged_ref[...] = merged.astype(jnp.bfloat16)
    upstream = up_keep_ref[...].astype(jnp.float32) + up_came_ref[...].astype(jnp.float32)
    back_ref[...] = normalize_back(upstream, unit_rows, inverse, gain).astype(jnp.bfloat16)


def attend_back(row_ref, proj_ref, query_ref, pair_ref, probs_ref, back_ref, put):
    back_ref[...] = trailing(row_ref[...], proj_ref[...]).astype(jnp.bfloat16)
    scaling = HEAD ** (-0.5)
    for h in range(probs_ref.shape[0]):
        cols = slice(h * HEAD, (h + 1) * HEAD)
        back = back_ref[:, cols]
        weights = probs_ref[h]
        prob_grad = trailing(back, pair_ref[1, :, cols])
        wide = weights.astype(jnp.float32)
        inner = jnp.sum(prob_grad * wide, axis=-1, keepdims=True)
        score_grad = (wide * (prob_grad - inner)).astype(jnp.bfloat16)
        query_grad = lax.dot_general(
            pair_ref[0, :, cols],
            score_grad,
            (((0,), (1,)), ((), ())),
            preferred_element_type=jnp.float32,
        )
        key_grad = leading(query_ref[:, cols], score_grad)
        put(h, query_grad * scaling, key_grad * scaling, leading(back, weights))


def own_back_kernel(
    row_ref, proj_ref, q_ref, pair_ref, probs_ref, query_ref, key_ref, value_ref, back_ref
):
    def put(h, query_grad, key_grad, value_grad):
        rows = slice(h * HEAD, (h + 1) * HEAD)
        query_ref[rows, :] = query_grad.astype(jnp.bfloat16)
        key_ref[rows, :] = key_grad
        value_ref[rows, :] = value_grad

    attend_back(row_ref, proj_ref, q_ref, pair_ref, probs_ref, back_ref, put)


def other_back_kernel(
    row_ref, proj_ref, q_ref, pair_ref, probs_ref, query_ref, key_ref, value_ref, *refs
):
    outs, (back_ref, slots_ref) = refs[:8], refs[8:]
    half = row_ref.shape[0]
    heads = probs_ref.shape[0]
    per_block = slots_ref.shape[2] // HEAD
    me = lax.axis_index("clip")
    turn = lax.bitwise_and(lax.shift_right_logical(me, 1), 3)
    away = 1 - lax.shift_right_logical(me, 3)
    mine, start = half_start(half, True), half_start(half, False)

    def where(t, h):
        piece = t * heads + h
        block, sub = piece // per_block, piece % per_block
        slot = lax.bitwise_xor(turn, block % 4)
        side = lax.bitwise_xor(away, block // 4)
        return side, slot, slice(sub * HEAD, (sub + 1) * HEAD)

    def put(h, query_grad, key_grad, value_grad):
        rows = slice(h * HEAD, (h + 1) * HEAD)
        side, slot, place = where(0, h)
        slots_ref[side, slot, place, pl.ds(mine, half)] = query_ref[rows, :]
        slots_ref[side, slot, place, pl.ds(start, half)] = query_grad.astype(jnp.bfloat16)
        side, slot, place = where(1, h)
        slots_ref[side, slot, place, :] = (key_ref[rows, :] + key_grad).astype(jnp.bfloat16)
        side, slot, place = where(2, h)
        slots_ref[side, slot, place, :] = (value_ref[rows, :] + value_grad).astype(jnp.bfloat16)

    attend_back(row_ref, proj_ref, q_ref, pair_ref, probs_ref, back_ref, put)
    for k, out_ref in enumerate(outs):
        out_ref[...] = slots_ref[k // 4, k % 4]


def product_kernel(t0, t1, t2, t3, n0, n1, n2, n3_low, n3_high, *refs):
    keep_ref, send_ref, sum_ref, n3 = refs[-4:]
    half = keep_ref.shape[0]
    core = lax.bitwise_and(lax.axis_index("clip"), 1)
    cut = n3_low.shape[0]
    n3[:cut, :] = n3_low[...]
    n3[cut:, :] = n3_high[...]
    total = None
    for t, n in ((t0, n0), (t1, n1), (t2, n2), (t3, n3)):
        term = jnp.dot(t[...], n[...], preferred_element_type=jnp.float32)
        total = term if total is None else total + term
    sum_ref[...] = total
    keep_ref[...] = sum_ref[pl.ds(pl.multiple_of(core * half, 8), half), :]
    other = sum_ref[pl.ds(pl.multiple_of((1 - core) * half, 8), half), :]
    send_ref[...] = other.astype(jnp.bfloat16)


def call(kernel, outs, kinds, flops, args, scratch=(), limit=30):
    spec = {
        "s": pl.BlockSpec(memory_space=pltpu.SMEM),
        "v": pl.BlockSpec(memory_space=pltpu.VMEM),
        "a": pl.BlockSpec(memory_space=pl.ANY),
    }
    return pl.pallas_call(
        kernel,
        out_shape=outs,
        in_specs=[spec[kind] for kind in kinds],
        out_specs=jax.tree.map(lambda _: spec["v"], outs),
        scratch_shapes=list(scratch),
        cost_estimate=pl.CostEstimate(flops=flops, bytes_accessed=4_000_000, transcendentals=0),
        compiler_params=pltpu.CompilerParams(vmem_limit_bytes=limit * 1024 * 1024),
    )(*args)


def fast_body(
    n_clip,
    patches,
    clip_tokens,
    positions,
    norm_gain,
    norm_bias,
    w_qkv,
    b_qkv,
    w_proj,
    b_proj,
    merge_gain,
    merge_bias,
    grad_placed,
):
    rows, width = patches.shape
    local = w_qkv.shape[2]
    heads = local // HEAD
    share_rows = grad_placed.shape[0]
    low = jnp.bfloat16
    shape = jax.ShapeDtypeStruct
    full = shape((rows, width), low)

    def swap(value):
        return lax.ppermute(value, "seq", [(0, 1), (1, 0)])

    def flip(value, bits):
        return lax.ppermute(value, "clip", [(i, i ^ bits) for i in range(n_clip)])

    half = rows // 2
    part, wide = shape((half, width), low), shape((half, width), jnp.float32)
    probs_half = shape((heads, half, rows), low)
    query = shape((half, local), low)
    attended = pltpu.VMEM((half, local), low)
    block = 3 * local // 8
    up_send = call(
        pull_kernel,
        part,
        "saa",
        4 * rows * share_rows * width,
        (clip_tokens, positions, grad_placed),
        (
            pltpu.VMEM(positions.shape, jnp.int32),
            pltpu.VMEM(grad_placed.shape, low),
            pltpu.SemaphoreType.DMA((5,)),
        ),
        limit=62,
    )
    up_came = swap(up_send)
    normed = call(norm_kernel, full, "vvv", 100 * rows * width, (norm_gain, norm_bias, patches))
    normed_of = [normed] + [flip(normed, q << 1) for q in (1, 2)]
    normed_of += [flip(normed_of[2][:half], 1 << 1), flip(normed_of[1][half:], 2 << 1)]
    other_query, pair, own_normed, w_query, other_probs, part_send = call(
        first_kernel,
        (query, shape((2, rows, local), low), part, shape((width, local), low), probs_half, part),
        "svvaa",
        7 * rows * width * local,
        (
            clip_tokens,
            b_qkv,
            normed,
            jnp.transpose(w_qkv, (1, 0, 2)),
            w_proj,
        ),
        (
            pltpu.VMEM((2, width, local), low),
            pltpu.VMEM((local, width), low),
            attended,
            pltpu.SemaphoreType.DMA((4,)),
        ),
        limit=49,
    )
    part_came = swap(part_send)
    own_query, own_probs, part_keep, up_keep = call(
        second_kernel,
        (query, probs_half, wide, part),
        "svvvvvvv",
        5 * half * width * local,
        (
            clip_tokens,
            positions,
            grad_placed,
            b_qkv,
            own_normed,
            w_query,
            pair,
            w_proj,
        ),
        (attended,),
    )
    merged, own_rows = call(
        middle_kernel,
        (part, part),
        "v" * 8,
        100 * half * width,
        (
            b_proj,
            merge_gain,
            merge_bias,
            part_keep,
            part_came,
            patches,
            up_keep,
            up_came,
        ),
    )
    other_rows = swap(own_rows)
    other_merged = swap(merged)
    query_own, key_own, value_own = call(
        own_back_kernel,
        (
            shape((local, half), low),
            shape((local, rows), jnp.float32),
            shape((local, rows), jnp.float32),
        ),
        "vvvvv",
        4 * half * width * local,
        (own_rows, w_proj, own_query, pair, own_probs),
        (attended,),
    )
    sent = call(
        other_back_kernel,
        (shape((block, rows), low),) * 8,
        "v" * 8,
        4 * half * width * local,
        (
            other_rows,
            w_proj,
            other_query,
            pair,
            other_probs,
            query_own,
            key_own,
            value_own,
        ),
        (attended, pltpu.VMEM((2, 4, block, rows), low)),
    )

    def exchange(sent):
        diagonal = flip(sent[3], 3 << 1)
        return [sent[0]] + [flip(sent[q], q << 1) for q in (1, 2)] + [diagonal]

    def product(taken, after=()):
        return call(
            product_kernel,
            (shape((block // 2, width), jnp.float32), shape((block // 2, width), low)),
            "v" * 9 + "a" * len(after),
            8 * block * rows * width,
            (*taken, *normed_of, *after),
            (pltpu.VMEM((block, width), jnp.float32), pltpu.VMEM((rows, width), low)),
        )

    far_taken = exchange(sent[:4])
    near_taken = exchange(sent[4:])
    far_keep, far_send = product(far_taken)
    far_came = flip(far_send, 1)
    far_sum = (far_keep + far_came.astype(jnp.float32)).astype(low)
    crossing = flip(far_sum, 8)
    near_keep, near_send = product(near_taken, (far_sum,))
    near_came = flip(near_send, 1)
    placed = call(
        place_kernel,
        shape((share_rows, 4 * width), low),
        "svvva",
        8 * rows * share_rows * width,
        (clip_tokens, positions, merged, other_merged, far_sum),
    )
    summed = near_keep + near_came.astype(jnp.float32) + crossing.astype(jnp.float32)
    return (placed, summed[None])


def solution(mesh):
    n_clip, n_seq = mesh.shape["clip"], mesh.shape["seq"]
    fast = n_clip == 2 * 4 * 2 and n_seq == 2
    body = functools.partial(fast_body, n_clip) if fast else general_body
    return jax.shard_map(
        body,
        mesh=mesh,
        in_specs=(
            P("clip", None),
            P("clip"),
            P("clip", None),
            P(),
            P(),
            P(None, None, "seq"),
            P(None, "seq"),
            P("seq", None),
            P(),
            P(),
            P(),
            P(("clip", "seq"), None),
        ),
        out_specs=(P(("clip", "seq"), None), P("seq", "clip", None)),
        check_vma=False,
    )
```

```python
import functools

import jax
import jax.numpy as jnp
from jax import lax
from jax.experimental import pallas as pl
from jax.experimental.pallas import tpu as pltpu
from jax.sharding import PartitionSpec as P


HEAD = 80


EPSILON = 1e-06


def normalize(values, gain_row, bias_row):
    center = values - jnp.mean(values, axis=-1, keepdims=True)
    inverse = lax.rsqrt(jnp.mean(center * center, axis=-1, keepdims=True) + EPSILON)
    unit_rows = center * inverse
    return (unit_rows * gain_row + bias_row, unit_rows, inverse)


def normalize_back(upstream, unit_rows, inverse, gain_row):
    scaled = upstream * gain_row
    return inverse * (
        scaled
        - jnp.mean(scaled, axis=-1, keepdims=True)
        - unit_rows * jnp.mean(scaled * unit_rows, axis=-1, keepdims=True)
    )


def leading(left, right):
    return lax.dot_general(
        left, right, (((0,), (0,)), ((), ())), preferred_element_type=jnp.float32
    )


def trailing(left, right):
    return lax.dot_general(
        left, right, (((1,), (1,)), ((), ())), preferred_element_type=jnp.float32
    )


def general_body(
    patches,
    clip_tokens,
    positions,
    norm_gain,
    norm_bias,
    w_qkv,
    b_qkv,
    w_proj,
    b_proj,
    merge_gain,
    merge_bias,
    grad_placed,
):
    block_rows = patches.shape[0]
    model_width = patches.shape[1]
    local_width = w_qkv.shape[2]
    local_heads = local_width // HEAD
    live_count = clip_tokens[0]
    places = positions[0]
    widened = patches.astype(jnp.float32)
    normed = normalize(widened, norm_gain, norm_bias)[0].astype(jnp.bfloat16)
    triple = jnp.dot(
        normed, w_qkv.reshape(model_width, 3 * local_width), preferred_element_type=jnp.float32
    )
    triple = (triple.reshape(block_rows, 3, local_width) + b_qkv).astype(jnp.bfloat16)
    query_rows = triple[:, 0].reshape(block_rows, local_heads, HEAD)
    key_rows = triple[:, 1].reshape(block_rows, local_heads, HEAD)
    value_rows = triple[:, 2].reshape(block_rows, local_heads, HEAD)
    scaling = HEAD ** (-0.5)
    scores = (
        jnp.einsum("qhd,khd->hqk", query_rows, key_rows, preferred_element_type=jnp.float32)
        * scaling
    )
    live_keys = jnp.arange(block_rows, dtype=jnp.int32) < 4 * live_count
    scores = jnp.where(live_keys[None, None, :], scores, -1e30)
    highest = jnp.max(scores, axis=-1, keepdims=True)
    powers = jnp.exp(scores - highest)
    weights = powers / jnp.sum(powers, axis=-1, keepdims=True)
    weights_low = weights.astype(jnp.bfloat16)
    attended = jnp.einsum(
        "hqk,khd->qhd", weights_low, value_rows, preferred_element_type=jnp.float32
    )
    attended = attended.reshape(block_rows, local_width).astype(jnp.bfloat16)
    partial_value = jnp.dot(attended, w_proj, preferred_element_type=jnp.float32)
    summed_share = lax.psum_scatter(
        partial_value.astype(jnp.bfloat16), "seq", scatter_dimension=0, tiled=True
    ).astype(jnp.float32)
    share_count = summed_share.shape[0]
    own_start = lax.axis_index("seq") * share_count
    own_patches = lax.dynamic_slice_in_dim(widened, own_start, share_count, 0)
    output_share = summed_share + b_proj + own_patches
    output = lax.all_gather(output_share.astype(jnp.bfloat16), "seq", axis=0, tiled=True).astype(
        output_share.dtype
    )
    merged_full, unit_rows, inverse = normalize(output, merge_gain, merge_bias)
    merged = merged_full.reshape(block_rows // 4, 4 * model_width).astype(jnp.bfloat16)
    live_tokens = jnp.arange(block_rows // 4, dtype=jnp.int32) < live_count
    share_rows = grad_placed.shape[0]
    rows_here = lax.axis_index("seq") * share_rows + jnp.arange(share_rows, dtype=jnp.int32)
    selector = ((places[None, :] == rows_here[:, None]) & live_tokens[None, :]).astype(jnp.bfloat16)
    placed = jnp.dot(selector, merged, preferred_element_type=jnp.float32).astype(jnp.bfloat16)
    own_grad = leading(selector, grad_placed)
    token_grad = lax.psum(own_grad.astype(jnp.bfloat16), "seq").astype(jnp.float32)
    upstream = token_grad.reshape(block_rows, model_width)
    row_grad = normalize_back(upstream, unit_rows, inverse, merge_gain).astype(jnp.bfloat16)
    attn_grad = lax.dot_general(
        row_grad, w_proj, (((1,), (1,)), ((), ())), preferred_element_type=jnp.float32
    )
    attn_grad = attn_grad.astype(jnp.bfloat16).reshape(block_rows, local_heads, HEAD)
    prob_grad = jnp.einsum(
        "qhd,khd->hqk", attn_grad, value_rows, preferred_element_type=jnp.float32
    )
    value_grad = jnp.einsum(
        "hqk,qhd->khd", weights_low, attn_grad, preferred_element_type=jnp.float32
    )
    score_grad = (
        weights * (prob_grad - jnp.sum(prob_grad * weights, axis=-1, keepdims=True)) * scaling
    )
    score_grad = score_grad.astype(jnp.bfloat16)
    query_grad = jnp.einsum(
        "hqk,khd->qhd", score_grad, key_rows, preferred_element_type=jnp.float32
    )
    key_grad = jnp.einsum(
        "hqk,qhd->khd", score_grad, query_rows, preferred_element_type=jnp.float32
    )
    triple_grad = jnp.stack([query_grad, key_grad, value_grad], axis=1)
    triple_grad = triple_grad.reshape(block_rows, 3 * local_width).astype(jnp.bfloat16)
    full_term = leading(triple_grad, normed)
    summed = lax.psum_scatter(full_term, "clip", scatter_dimension=0, tiled=True)
    return (placed, summed[None])


def place_masks(live_ref, places, share_rows, rows, first_row):
    tokens = places.shape[1]
    token = lax.broadcasted_iota(jnp.int32, (tokens, rows), 0)
    owner = (lax.broadcasted_iota(jnp.int32, (tokens, rows), 1) + first_row) // 4
    spread = jnp.where((token == owner) & (token < live_ref[0]), 1.0, 0.0)
    shifted = jnp.broadcast_to(places.astype(jnp.float32) + 1.0, (8, tokens))
    row = jnp.dot(shifted, spread, precision=lax.Precision.HIGHEST)[:1] - 1.0
    first = lax.axis_index("seq") * share_rows
    window = lax.broadcasted_iota(jnp.int32, (share_rows, rows), 0) + first
    patch = lax.broadcasted_iota(jnp.int32, (share_rows, rows), 1)
    hit = window.astype(jnp.float32) == row
    return [
        jnp.where(hit & (lax.rem(patch, 4) == k), 1.0, 0.0).astype(jnp.bfloat16) for k in range(4)
    ]


def begin(sources, targets, sems, first=0):
    copies = [
        pltpu.make_async_copy(source, target, sems.at[first + k])
        for k, (source, target) in enumerate(zip(sources, targets, strict=True))
    ]
    for copy in copies:
        copy.start()
    return copies


def half_start(half, own):
    seq = lax.axis_index("seq")
    return pl.multiple_of((seq if own else 1 - seq) * half, 128)


def norm_low(patches_ref, gain_ref, bias_ref):
    return normalize(
        patches_ref[...].astype(jnp.float32), gain_ref[...][None, :], bias_ref[...][None, :]
    )[0].astype(jnp.bfloat16)


def pull(live_ref, places_ref, grad_ref, out_ref, own):
    half, width = out_ref.shape
    masks = place_masks(
        live_ref, places_ref[...], grad_ref.shape[0], half, half_start(half, own)
    )
    total = None
    for k in range(4):
        term = leading(masks[k], grad_ref[:, k * width : (k + 1) * width])
        total = term if total is None else total + term
    out_ref[...] = total.astype(out_ref.dtype)


def pull_kernel(
    live_hbm, places_hbm, grad_hbm, send_ref, live_ref, places_ref, grad_ref, sems
):
    half, width = send_ref.shape
    counted = begin((live_hbm,), (live_ref,), sems, 5)
    came = begin((places_hbm,), (places_ref,), sems)
    blocks = [slice(k * width, (k + 1) * width) for k in range(4)]
    came += begin(
        [grad_hbm.at[:, block] for block in blocks],
        [grad_ref.at[:, block] for block in blocks],
        sems,
        1,
    )
    counted[0].wait()
    came[0].wait()
    masks = place_masks(
        live_ref, places_ref[...], grad_ref.shape[0], half, half_start(half, False)
    )
    total = None
    for k in range(4):
        came[1 + k].wait()
        term = leading(masks[k], grad_ref[:, blocks[k]])
        total = term if total is None else total + term
    send_ref[...] = total.astype(send_ref.dtype)


def norm_kernel(gain_ref, bias_ref, patches_ref, normed_ref):
    normed_ref[...] = norm_low(patches_ref, gain_ref, bias_ref)


def place_kernel(live_ref, places_ref, own_ref, other_ref, _, out_ref):
    half, width = own_ref.shape
    share_rows = out_ref.shape[0]
    own = place_masks(live_ref, places_ref[...], share_rows, half, half_start(half, True))
    other = place_masks(live_ref, places_ref[...], share_rows, half, half_start(half, False))
    for k in range(4):
        term = jnp.dot(own[k], own_ref[...], preferred_element_type=jnp.float32)
        term += jnp.dot(other[k], other_ref[...], preferred_element_type=jnp.float32)
        out_ref[:, k * width : (k + 1) * width] = term.astype(out_ref.dtype)


def attend(live_ref, query_ref, pair_ref, probs_ref, attended_ref):
    half, rows = probs_ref.shape[1:]
    live = lax.broadcasted_iota(jnp.int32, (half, rows), 1) < 4 * live_ref[0]
    steep = HEAD ** (-0.5) * 1.4426950408889634
    for h in range(probs_ref.shape[0]):
        cols = slice(h * HEAD, (h + 1) * HEAD)
        scores = trailing(query_ref[:, cols], pair_ref[0, :, cols])
        scores = jnp.where(live, scores, -1e30)
        powers = jnp.exp2((scores - jnp.max(scores, axis=-1, keepdims=True)) * steep)
        weights = powers * (1.0 / jnp.sum(powers, axis=-1, keepdims=True))
        weights = weights.astype(jnp.bfloat16)
        probs_ref[h] = weights
        attended_ref[:, cols] = jnp.dot(
            weights, pair_ref[1, :, cols], preferred_element_type=jnp.float32
        ).astype(jnp.bfloat16)


def first_kernel(
    live_hbm,
    b_ref,
    normed_ref,
    w_hbm,
    proj_hbm,
    query_ref,
    pair_ref,
    own_ref,
    wq_ref,
    probs_ref,
    send_ref,
    live_ref,
    w_ref,
    proj_ref,
    attended_ref,
    sems,
):
    came = begin(
        (w_hbm.at[0], w_hbm.at[1], w_hbm.at[2], proj_hbm, live_hbm),
        (wq_ref, w_ref.at[0], w_ref.at[1], proj_ref, live_ref),
        sems,
    )
    half = send_ref.shape[0]
    start = half_start(half, False)
    own_ref[...] = normed_ref[pl.ds(half_start(half, True), half), :]
    came[0].wait()
    part = jnp.dot(
        normed_ref[pl.ds(start, half), :], wq_ref[...], preferred_element_type=jnp.float32
    )
    query_ref[...] = (part + b_ref[0:1, :]).astype(jnp.bfloat16)
    for t in (1, 2):
        came[t].wait()
        part = jnp.dot(normed_ref[...], w_ref[t - 1], preferred_element_type=jnp.float32)
        pair_ref[t - 1] = (part + b_ref[t : t + 1, :]).astype(jnp.bfloat16)
    came[4].wait()
    attend(live_ref, query_ref, pair_ref, probs_ref, attended_ref)
    came[3].wait()
    send_ref[...] = jnp.dot(
        attended_ref[...], proj_ref[...], preferred_element_type=jnp.float32
    ).astype(jnp.bfloat16)


def second_kernel(
    live_ref,
    places_ref,
    grad_ref,
    b_ref,
    own_ref,
    w_ref,
    pair_ref,
    proj_ref,
    query_ref,
    probs_ref,
    keep_ref,
    up_ref,
    attended_ref,
):
    pull(live_ref, places_ref, grad_ref, up_ref, True)
    part = jnp.dot(own_ref[...], w_ref[...], preferred_element_type=jnp.float32)
    query_ref[...] = (part + b_ref[0:1, :]).astype(jnp.bfloat16)
    attend(live_ref, query_ref, pair_ref, probs_ref, attended_ref)
    keep_ref[...] = jnp.dot(attended_ref[...], proj_ref[...], preferred_element_type=jnp.float32)


def middle_kernel(
    b_ref,
    gain_ref,
    bias_ref,
    keep_ref,
    came_ref,
    patches_ref,
    up_keep_ref,
    up_came_ref,
    merged_ref,
    back_ref,
):
    half = keep_ref.shape[0]
    gain = gain_ref[...][None, :]
    output = (
        keep_ref[...]
        + came_ref[...].astype(jnp.float32)
        + b_ref[...][None, :]
        + patches_ref[pl.ds(half_start(half, True), half), :].astype(jnp.float32)
    )
    merged, unit_rows, inverse = normalize(output, gain, bias_ref[...][None, :])
    merged_ref[...] = merged.astype(jnp.bfloat16)
    upstream = up_keep_ref[...].astype(jnp.float32) + up_came_ref[...].astype(jnp.float32)
    back_ref[...] = normalize_back(upstream, unit_rows, inverse, gain).astype(jnp.bfloat16)


def attend_back(row_ref, proj_ref, query_ref, pair_ref, probs_ref, back_ref, put):
    back_ref[...] = trailing(row_ref[...], proj_ref[...]).astype(jnp.bfloat16)
    scaling = HEAD ** (-0.5)
    for h in range(probs_ref.shape[0]):
        cols = slice(h * HEAD, (h + 1) * HEAD)
        back = back_ref[:, cols]
        weights = probs_ref[h]
        prob_grad = trailing(back, pair_ref[1, :, cols])
        wide = weights.astype(jnp.float32)
        inner = jnp.sum(prob_grad * wide, axis=-1, keepdims=True)
        score_grad = (wide * (prob_grad - inner)).astype(jnp.bfloat16)
        query_grad = lax.dot_general(
            pair_ref[0, :, cols],
            score_grad,
            (((0,), (1,)), ((), ())),
            preferred_element_type=jnp.float32,
        )
        key_grad = leading(query_ref[:, cols], score_grad)
        put(h, query_grad * scaling, key_grad * scaling, leading(back, weights))


def own_back_kernel(
    row_ref, proj_ref, q_ref, pair_ref, probs_ref, query_ref, key_ref, value_ref, back_ref
):
    def put(h, query_grad, key_grad, value_grad):
        rows = slice(h * HEAD, (h + 1) * HEAD)
        query_ref[rows, :] = query_grad.astype(jnp.bfloat16)
        key_ref[rows, :] = key_grad
        value_ref[rows, :] = value_grad

    attend_back(row_ref, proj_ref, q_ref, pair_ref, probs_ref, back_ref, put)


def other_back_kernel(
    row_ref, proj_ref, q_ref, pair_ref, probs_ref, query_ref, key_ref, value_ref, *refs
):
    outs, (back_ref, slots_ref) = refs[:8], refs[8:]
    half = row_ref.shape[0]
    heads = probs_ref.shape[0]
    per_block = slots_ref.shape[2] // HEAD
    me = lax.axis_index("clip")
    turn = lax.bitwise_and(lax.shift_right_logical(me, 1), 3)
    away = 1 - lax.shift_right_logical(me, 3)
    mine, start = half_start(half, True), half_start(half, False)

    def where(t, h):
        piece = t * heads + h
        block, sub = piece // per_block, piece % per_block
        slot = lax.bitwise_xor(turn, block % 4)
        side = lax.bitwise_xor(away, block // 4)
        return side, slot, slice(sub * HEAD, (sub + 1) * HEAD)

    def put(h, query_grad, key_grad, value_grad):
        rows = slice(h * HEAD, (h + 1) * HEAD)
        side, slot, place = where(0, h)
        slots_ref[side, slot, place, pl.ds(mine, half)] = query_ref[rows, :]
        slots_ref[side, slot, place, pl.ds(start, half)] = query_grad.astype(jnp.bfloat16)
        side, slot, place = where(1, h)
        slots_ref[side, slot, place, :] = (key_ref[rows, :] + key_grad).astype(jnp.bfloat16)
        side, slot, place = where(2, h)
        slots_ref[side, slot, place, :] = (value_ref[rows, :] + value_grad).astype(jnp.bfloat16)

    attend_back(row_ref, proj_ref, q_ref, pair_ref, probs_ref, back_ref, put)
    for k, out_ref in enumerate(outs):
        out_ref[...] = slots_ref[k // 4, k % 4]


def product_kernel(t0, t1, t2, t3, n0, n1, n2, n3_low, n3_high, *refs):
    keep_ref, send_ref, sum_ref, n3 = refs[-4:]
    half = keep_ref.shape[0]
    core = lax.bitwise_and(lax.axis_index("clip"), 1)
    cut = n3_low.shape[0]
    n3[:cut, :] = n3_low[...]
    n3[cut:, :] = n3_high[...]
    total = None
    for t, n in ((t0, n0), (t1, n1), (t2, n2), (t3, n3)):
        term = jnp.dot(t[...], n[...], preferred_element_type=jnp.float32)
        total = term if total is None else total + term
    sum_ref[...] = total
    keep_ref[...] = sum_ref[pl.ds(pl.multiple_of(core * half, 8), half), :]
    other = sum_ref[pl.ds(pl.multiple_of((1 - core) * half, 8), half), :]
    send_ref[...] = other.astype(jnp.bfloat16)


def call(kernel, outs, kinds, flops, args, scratch=(), limit=30):
    spec = {
        "s": pl.BlockSpec(memory_space=pltpu.SMEM),
        "v": pl.BlockSpec(memory_space=pltpu.VMEM),
        "a": pl.BlockSpec(memory_space=pl.ANY),
    }
    return pl.pallas_call(
        kernel,
        out_shape=outs,
        in_specs=[spec[kind] for kind in kinds],
        out_specs=jax.tree.map(lambda _: spec["v"], outs),
        scratch_shapes=list(scratch),
        cost_estimate=pl.CostEstimate(flops=flops, bytes_accessed=4_000_000, transcendentals=0),
        compiler_params=pltpu.CompilerParams(vmem_limit_bytes=limit * 1024 * 1024),
    )(*args)


def fast_body(
    n_clip,
    patches,
    clip_tokens,
    positions,
    norm_gain,
    norm_bias,
    w_qkv,
    b_qkv,
    w_proj,
    b_proj,
    merge_gain,
    merge_bias,
    grad_placed,
):
    rows, width = patches.shape
    local = w_qkv.shape[2]
    heads = local // HEAD
    share_rows = grad_placed.shape[0]
    low = jnp.bfloat16
    shape = jax.ShapeDtypeStruct
    full = shape((rows, width), low)

    def swap(value):
        return lax.ppermute(value, "seq", [(0, 1), (1, 0)])

    def flip(value, bits):
        return lax.ppermute(value, "clip", [(i, i ^ bits) for i in range(n_clip)])

    counted = jnp.minimum(clip_tokens, rows // 4)
    half = rows // 2
    part, wide = shape((half, width), low), shape((half, width), jnp.float32)
    probs_half = shape((heads, half, rows), low)
    query = shape((half, local), low)
    attended = pltpu.VMEM((half, local), low)
    block = 3 * local // 8
    up_send = call(
        pull_kernel,
        part,
        "aaa",
        4 * rows * share_rows * width,
        (clip_tokens, positions, grad_placed),
        (
            pltpu.SMEM((1,), jnp.int32),
            pltpu.VMEM(positions.shape, jnp.int32),
            pltpu.VMEM(grad_placed.shape, low),
            pltpu.SemaphoreType.DMA((6,)),
        ),
        limit=62,
    )
    up_came = swap(up_send)
    normed = call(norm_kernel, full, "vvv", 100 * rows * width, (norm_gain, norm_bias, patches))
    normed_of = [normed] + [flip(normed, q << 1) for q in (1, 2)]
    normed_of += [flip(normed_of[2][:half], 1 << 1), flip(normed_of[1][half:], 2 << 1)]
    other_query, pair, own_normed, w_query, other_probs, part_send = call(
        first_kernel,
        (query, shape((2, rows, local), low), part, shape((width, local), low), probs_half, part),
        "avvaa",
        7 * rows * width * local,
        (
            clip_tokens,
            b_qkv,
            normed,
            jnp.transpose(w_qkv, (1, 0, 2)),
            w_proj,
        ),
        (
            pltpu.SMEM((1,), jnp.int32),
            pltpu.VMEM((2, width, local), low),
            pltpu.VMEM((local, width), low),
            attended,
            pltpu.SemaphoreType.DMA((5,)),
        ),
        limit=49,
    )
    part_came = swap(part_send)
    own_query, own_probs, part_keep, up_keep = call(
        second_kernel,
        (query, probs_half, wide, part),
        "svvvvvvv",
        5 * half * width * local,
        (
            counted,
            positions,
            grad_placed,
            b_qkv,
            own_normed,
            w_query,
            pair,
            w_proj,
        ),
        (attended,),
    )
    merged, own_rows = call(
        middle_kernel,
        (part, part),
        "v" * 8,
        100 * half * width,
        (
            b_proj,
            merge_gain,
            merge_bias,
            part_keep,
            part_came,
            patches,
            up_keep,
            up_came,
        ),
    )
    other_rows = swap(own_rows)
    other_merged = swap(merged)
    query_own, key_own, value_own = call(
        own_back_kernel,
        (
            shape((local, half), low),
            shape((local, rows), jnp.float32),
            shape((local, rows), jnp.float32),
        ),
        "vvvvv",
        4 * half * width * local,
        (own_rows, w_proj, own_query, pair, own_probs),
        (attended,),
    )
    sent = call(
        other_back_kernel,
        (shape((block, rows), low),) * 8,
        "v" * 8,
        4 * half * width * local,
        (
            other_rows,
            w_proj,
            other_query,
            pair,
            other_probs,
            query_own,
            key_own,
            value_own,
        ),
        (attended, pltpu.VMEM((2, 4, block, rows), low)),
    )

    def exchange(sent):
        diagonal = flip(sent[3], 3 << 1)
        return [sent[0]] + [flip(sent[q], q << 1) for q in (1, 2)] + [diagonal]

    def product(taken, after=()):
        return call(
            product_kernel,
            (shape((block // 2, width), jnp.float32), shape((block // 2, width), low)),
            "v" * 9 + "a" * len(after),
            8 * block * rows * width,
            (*taken, *normed_of, *after),
            (pltpu.VMEM((block, width), jnp.float32), pltpu.VMEM((rows, width), low)),
        )

    far_taken = exchange(sent[:4])
    near_taken = exchange(sent[4:])
    far_keep, far_send = product(far_taken)
    far_came = flip(far_send, 1)
    far_sum = (far_keep + far_came.astype(jnp.float32)).astype(low)
    crossing = flip(far_sum, 8)
    near_keep, near_send = product(near_taken, (far_sum,))
    near_came = flip(near_send, 1)
    placed = call(
        place_kernel,
        shape((share_rows, 4 * width), low),
        "svvva",
        8 * rows * share_rows * width,
        (counted, positions, merged, other_merged, far_sum),
    )
    summed = near_keep + near_came.astype(jnp.float32) + crossing.astype(jnp.float32)
    return (placed, summed[None])


def solution(mesh):
    n_clip, n_seq = mesh.shape["clip"], mesh.shape["seq"]
    fast = n_clip == 2 * 4 * 2 and n_seq == 2
    body = functools.partial(fast_body, n_clip) if fast else general_body
    return jax.shard_map(
        body,
        mesh=mesh,
        in_specs=(
            P("clip", None),
            P("clip"),
            P("clip", None),
            P(),
            P(),
            P(None, None, "seq"),
            P(None, "seq"),
            P("seq", None),
            P(),
            P(),
            P(),
            P(("clip", "seq"), None),
        ),
        out_specs=(P(("clip", "seq"), None), P("seq", "clip", None)),
        check_vma=False,
    )
```

```python
import functools

import jax
import jax.numpy as jnp
from jax import lax
from jax.experimental import pallas as pl
from jax.experimental.pallas import tpu as pltpu
from jax.sharding import PartitionSpec as P


HEAD = 80


EPSILON = 1e-06


def normalize(values, gain_row, bias_row):
    center = values - jnp.mean(values, axis=-1, keepdims=True)
    inverse = lax.rsqrt(jnp.mean(center * center, axis=-1, keepdims=True) + EPSILON)
    unit_rows = center * inverse
    return (unit_rows * gain_row + bias_row, unit_rows, inverse)


def normalize_back(upstream, unit_rows, inverse, gain_row):
    scaled = upstream * gain_row
    return inverse * (
        scaled
        - jnp.mean(scaled, axis=-1, keepdims=True)
        - unit_rows * jnp.mean(scaled * unit_rows, axis=-1, keepdims=True)
    )


def leading(left, right):
    return lax.dot_general(
        left, right, (((0,), (0,)), ((), ())), preferred_element_type=jnp.float32
    )


def trailing(left, right):
    return lax.dot_general(
        left, right, (((1,), (1,)), ((), ())), preferred_element_type=jnp.float32
    )


def general_body(
    patches,
    clip_tokens,
    positions,
    norm_gain,
    norm_bias,
    w_qkv,
    b_qkv,
    w_proj,
    b_proj,
    merge_gain,
    merge_bias,
    grad_placed,
):
    block_rows = patches.shape[0]
    model_width = patches.shape[1]
    local_width = w_qkv.shape[2]
    local_heads = local_width // HEAD
    live_count = clip_tokens[0]
    places = positions[0]
    widened = patches.astype(jnp.float32)
    normed = normalize(widened, norm_gain, norm_bias)[0].astype(jnp.bfloat16)
    triple = jnp.dot(
        normed, w_qkv.reshape(model_width, 3 * local_width), preferred_element_type=jnp.float32
    )
    triple = (triple.reshape(block_rows, 3, local_width) + b_qkv).astype(jnp.bfloat16)
    query_rows = triple[:, 0].reshape(block_rows, local_heads, HEAD)
    key_rows = triple[:, 1].reshape(block_rows, local_heads, HEAD)
    value_rows = triple[:, 2].reshape(block_rows, local_heads, HEAD)
    scaling = HEAD ** (-0.5)
    scores = (
        jnp.einsum("qhd,khd->hqk", query_rows, key_rows, preferred_element_type=jnp.float32)
        * scaling
    )
    live_keys = jnp.arange(block_rows, dtype=jnp.int32) < 4 * live_count
    scores = jnp.where(live_keys[None, None, :], scores, -1e30)
    highest = jnp.max(scores, axis=-1, keepdims=True)
    powers = jnp.exp(scores - highest)
    weights = powers / jnp.sum(powers, axis=-1, keepdims=True)
    weights_low = weights.astype(jnp.bfloat16)
    attended = jnp.einsum(
        "hqk,khd->qhd", weights_low, value_rows, preferred_element_type=jnp.float32
    )
    attended = attended.reshape(block_rows, local_width).astype(jnp.bfloat16)
    partial_value = jnp.dot(attended, w_proj, preferred_element_type=jnp.float32)
    summed_share = lax.psum_scatter(
        partial_value.astype(jnp.bfloat16), "seq", scatter_dimension=0, tiled=True
    ).astype(jnp.float32)
    share_count = summed_share.shape[0]
    own_start = lax.axis_index("seq") * share_count
    own_patches = lax.dynamic_slice_in_dim(widened, own_start, share_count, 0)
    output_share = summed_share + b_proj + own_patches
    output = lax.all_gather(output_share.astype(jnp.bfloat16), "seq", axis=0, tiled=True).astype(
        output_share.dtype
    )
    merged_full, unit_rows, inverse = normalize(output, merge_gain, merge_bias)
    merged = merged_full.reshape(block_rows // 4, 4 * model_width).astype(jnp.bfloat16)
    live_tokens = jnp.arange(block_rows // 4, dtype=jnp.int32) < live_count
    share_rows = grad_placed.shape[0]
    rows_here = lax.axis_index("seq") * share_rows + jnp.arange(share_rows, dtype=jnp.int32)
    selector = ((places[None, :] == rows_here[:, None]) & live_tokens[None, :]).astype(jnp.bfloat16)
    placed = jnp.dot(selector, merged, preferred_element_type=jnp.float32).astype(jnp.bfloat16)
    own_grad = leading(selector, grad_placed)
    token_grad = lax.psum(own_grad.astype(jnp.bfloat16), "seq").astype(jnp.float32)
    upstream = token_grad.reshape(block_rows, model_width)
    row_grad = normalize_back(upstream, unit_rows, inverse, merge_gain).astype(jnp.bfloat16)
    attn_grad = lax.dot_general(
        row_grad, w_proj, (((1,), (1,)), ((), ())), preferred_element_type=jnp.float32
    )
    attn_grad = attn_grad.astype(jnp.bfloat16).reshape(block_rows, local_heads, HEAD)
    prob_grad = jnp.einsum(
        "qhd,khd->hqk", attn_grad, value_rows, preferred_element_type=jnp.float32
    )
    value_grad = jnp.einsum(
        "hqk,qhd->khd", weights_low, attn_grad, preferred_element_type=jnp.float32
    )
    score_grad = (
        weights * (prob_grad - jnp.sum(prob_grad * weights, axis=-1, keepdims=True)) * scaling
    )
    score_grad = score_grad.astype(jnp.bfloat16)
    query_grad = jnp.einsum(
        "hqk,khd->qhd", score_grad, key_rows, preferred_element_type=jnp.float32
    )
    key_grad = jnp.einsum(
        "hqk,qhd->khd", score_grad, query_rows, preferred_element_type=jnp.float32
    )
    triple_grad = jnp.stack([query_grad, key_grad, value_grad], axis=1)
    triple_grad = triple_grad.reshape(block_rows, 3 * local_width).astype(jnp.bfloat16)
    full_term = leading(triple_grad, normed)
    summed = lax.psum_scatter(full_term, "clip", scatter_dimension=0, tiled=True)
    return (placed, summed[None])


def place_masks(live_ref, places, share_rows, rows, first_row):
    tokens = places.shape[1]
    token = lax.broadcasted_iota(jnp.int32, (tokens, rows), 0)
    owner = (lax.broadcasted_iota(jnp.int32, (tokens, rows), 1) + first_row) // 4
    spread = jnp.where((token == owner) & (token < live_ref[0]), 1.0, 0.0)
    shifted = jnp.broadcast_to(places.astype(jnp.float32) + 1.0, (8, tokens))
    row = jnp.dot(shifted, spread, precision=lax.Precision.HIGHEST)[:1] - 1.0
    first = lax.axis_index("seq") * share_rows
    window = lax.broadcasted_iota(jnp.int32, (share_rows, rows), 0) + first
    patch = lax.broadcasted_iota(jnp.int32, (share_rows, rows), 1)
    hit = window.astype(jnp.float32) == row
    return [
        jnp.where(hit & (lax.rem(patch, 4) == k), 1.0, 0.0).astype(jnp.bfloat16) for k in range(4)
    ]


def begin(sources, targets, sems, first=0):
    copies = [
        pltpu.make_async_copy(source, target, sems.at[first + k])
        for k, (source, target) in enumerate(zip(sources, targets, strict=True))
    ]
    for copy in copies:
        copy.start()
    return copies


def half_start(half, own):
    seq = lax.axis_index("seq")
    return pl.multiple_of((seq if own else 1 - seq) * half, 128)


def norm_low(patches_ref, gain_ref, bias_ref):
    return normalize(
        patches_ref[...].astype(jnp.float32), gain_ref[...][None, :], bias_ref[...][None, :]
    )[0].astype(jnp.bfloat16)


def pull(live_ref, places_ref, grad_ref, out_ref, own):
    half, width = out_ref.shape
    masks = place_masks(
        live_ref, places_ref[...], grad_ref.shape[0], half, half_start(half, own)
    )
    total = None
    for k in range(4):
        term = leading(masks[k], grad_ref[:, k * width : (k + 1) * width])
        total = term if total is None else total + term
    out_ref[...] = total.astype(out_ref.dtype)


def pull_kernel(
    live_hbm, places_hbm, grad_hbm, send_ref, live_ref, places_ref, grad_ref, sems
):
    half, width = send_ref.shape
    counted = begin((live_hbm,), (live_ref,), sems, 5)
    came = begin((places_hbm,), (places_ref,), sems)
    blocks = [slice(k * width, (k + 1) * width) for k in range(4)]
    came += begin(
        [grad_hbm.at[:, block] for block in blocks],
        [grad_ref.at[:, block] for block in blocks],
        sems,
        1,
    )
    counted[0].wait()
    came[0].wait()
    masks = place_masks(
        live_ref, places_ref[...], grad_ref.shape[0], half, half_start(half, False)
    )
    total = None
    for k in range(4):
        came[1 + k].wait()
        term = leading(masks[k], grad_ref[:, blocks[k]])
        total = term if total is None else total + term
    send_ref[...] = total.astype(send_ref.dtype)


def norm_kernel(gain_ref, bias_ref, patches_ref, normed_ref):
    normed_ref[...] = norm_low(patches_ref, gain_ref, bias_ref)


def place_kernel(live_ref, places_ref, own_ref, other_ref, _, out_ref):
    half, width = own_ref.shape
    share_rows = out_ref.shape[0]
    own = place_masks(live_ref, places_ref[...], share_rows, half, half_start(half, True))
    other = place_masks(live_ref, places_ref[...], share_rows, half, half_start(half, False))
    for k in range(4):
        term = jnp.dot(own[k], own_ref[...], preferred_element_type=jnp.float32)
        term += jnp.dot(other[k], other_ref[...], preferred_element_type=jnp.float32)
        out_ref[:, k * width : (k + 1) * width] = term.astype(out_ref.dtype)


def attend(live_ref, query_ref, pair_ref, probs_ref, attended_ref):
    half, rows = probs_ref.shape[1:]
    live = lax.broadcasted_iota(jnp.int32, (half, rows), 1) < 4 * live_ref[0]
    steep = HEAD ** (-0.5) * 1.4426950408889634
    for h in range(probs_ref.shape[0]):
        cols = slice(h * HEAD, (h + 1) * HEAD)
        scores = trailing(query_ref[:, cols], pair_ref[0, :, cols])
        scores = jnp.where(live, scores, -1e30)
        powers = jnp.exp2((scores - jnp.max(scores, axis=-1, keepdims=True)) * steep)
        weights = powers * (1.0 / jnp.sum(powers, axis=-1, keepdims=True))
        weights = weights.astype(jnp.bfloat16)
        probs_ref[h] = weights
        attended_ref[:, cols] = jnp.dot(
            weights, pair_ref[1, :, cols], preferred_element_type=jnp.float32
        ).astype(jnp.bfloat16)


def first_kernel(
    live_hbm,
    b_ref,
    normed_ref,
    w_hbm,
    proj_hbm,
    query_ref,
    pair_ref,
    own_ref,
    wq_ref,
    probs_ref,
    send_ref,
    live_ref,
    w_ref,
    proj_ref,
    attended_ref,
    sems,
):
    came = begin(
        (w_hbm.at[0], w_hbm.at[1], w_hbm.at[2], proj_hbm, live_hbm),
        (wq_ref, w_ref.at[0], w_ref.at[1], proj_ref, live_ref),
        sems,
    )
    half = send_ref.shape[0]
    start = half_start(half, False)
    own_ref[...] = normed_ref[pl.ds(half_start(half, True), half), :]
    came[0].wait()
    part = jnp.dot(
        normed_ref[pl.ds(start, half), :], wq_ref[...], preferred_element_type=jnp.float32
    )
    query_ref[...] = (part + b_ref[0:1, :]).astype(jnp.bfloat16)
    for t in (1, 2):
        came[t].wait()
        part = jnp.dot(normed_ref[...], w_ref[t - 1], preferred_element_type=jnp.float32)
        pair_ref[t - 1] = (part + b_ref[t : t + 1, :]).astype(jnp.bfloat16)
    came[4].wait()
    attend(live_ref, query_ref, pair_ref, probs_ref, attended_ref)
    came[3].wait()
    send_ref[...] = jnp.dot(
        attended_ref[...], proj_ref[...], preferred_element_type=jnp.float32
    ).astype(jnp.bfloat16)


def second_kernel(
    live_ref,
    places_ref,
    grad_ref,
    b_ref,
    own_ref,
    w_ref,
    pair_ref,
    proj_ref,
    query_ref,
    probs_ref,
    keep_ref,
    up_ref,
    turned_ref,
    attended_ref,
):
    turned_ref[...] = proj_ref[...].T
    pull(live_ref, places_ref, grad_ref, up_ref, True)
    part = jnp.dot(own_ref[...], w_ref[...], preferred_element_type=jnp.float32)
    query_ref[...] = (part + b_ref[0:1, :]).astype(jnp.bfloat16)
    attend(live_ref, query_ref, pair_ref, probs_ref, attended_ref)
    keep_ref[...] = jnp.dot(attended_ref[...], proj_ref[...], preferred_element_type=jnp.float32)


def middle_kernel(
    b_ref,
    gain_ref,
    bias_ref,
    keep_ref,
    came_ref,
    patches_ref,
    up_keep_ref,
    up_came_ref,
    merged_ref,
    back_ref,
):
    half = keep_ref.shape[0]
    gain = gain_ref[...][None, :]
    output = (
        keep_ref[...]
        + came_ref[...].astype(jnp.float32)
        + b_ref[...][None, :]
        + patches_ref[pl.ds(half_start(half, True), half), :].astype(jnp.float32)
    )
    merged, unit_rows, inverse = normalize(output, gain, bias_ref[...][None, :])
    merged_ref[...] = merged.astype(jnp.bfloat16)
    upstream = up_keep_ref[...].astype(jnp.float32) + up_came_ref[...].astype(jnp.float32)
    back_ref[...] = normalize_back(upstream, unit_rows, inverse, gain).astype(jnp.bfloat16)


def attend_back(row_ref, turned_ref, query_ref, pair_ref, probs_ref, back_ref, put):
    back_ref[...] = jnp.dot(
        row_ref[...], turned_ref[...], preferred_element_type=jnp.float32
    ).astype(jnp.bfloat16)
    scaling = HEAD ** (-0.5)
    for h in range(probs_ref.shape[0]):
        cols = slice(h * HEAD, (h + 1) * HEAD)
        back = back_ref[:, cols]
        weights = probs_ref[h]
        prob_grad = trailing(back, pair_ref[1, :, cols])
        wide = weights.astype(jnp.float32)
        inner = jnp.sum(prob_grad * wide, axis=-1, keepdims=True)
        score_grad = (wide * (prob_grad - inner)).astype(jnp.bfloat16)
        query_grad = jnp.dot(
            score_grad, pair_ref[0, :, cols], preferred_element_type=jnp.float32
        )
        key_grad = leading(query_ref[:, cols], score_grad)
        put(h, (query_grad * scaling).T, key_grad * scaling, leading(back, weights))


def own_back_kernel(
    row_ref, turned_ref, q_ref, pair_ref, probs_ref, query_ref, key_ref, value_ref, back_ref
):
    def put(h, query_grad, key_grad, value_grad):
        rows = slice(h * HEAD, (h + 1) * HEAD)
        query_ref[rows, :] = query_grad.astype(jnp.bfloat16)
        key_ref[rows, :] = key_grad
        value_ref[rows, :] = value_grad

    attend_back(row_ref, turned_ref, q_ref, pair_ref, probs_ref, back_ref, put)


def other_back_kernel(
    row_ref, turned_ref, q_ref, pair_ref, probs_ref, query_ref, key_ref, value_ref, *refs
):
    outs, (back_ref, slots_ref) = refs[:8], refs[8:]
    half = row_ref.shape[0]
    heads = probs_ref.shape[0]
    per_block = slots_ref.shape[2] // HEAD
    me = lax.axis_index("clip")
    turn = lax.bitwise_and(lax.shift_right_logical(me, 1), 3)
    away = 1 - lax.shift_right_logical(me, 3)
    mine, start = half_start(half, True), half_start(half, False)

    def where(t, h):
        piece = t * heads + h
        block, sub = piece // per_block, piece % per_block
        slot = lax.bitwise_xor(turn, block % 4)
        side = lax.bitwise_xor(away, block // 4)
        return side, slot, slice(sub * HEAD, (sub + 1) * HEAD)

    def put(h, query_grad, key_grad, value_grad):
        rows = slice(h * HEAD, (h + 1) * HEAD)
        side, slot, place = where(0, h)
        slots_ref[side, slot, place, pl.ds(mine, half)] = query_ref[rows, :]
        slots_ref[side, slot, place, pl.ds(start, half)] = query_grad.astype(jnp.bfloat16)
        side, slot, place = where(1, h)
        slots_ref[side, slot, place, :] = (key_ref[rows, :] + key_grad).astype(jnp.bfloat16)
        side, slot, place = where(2, h)
        slots_ref[side, slot, place, :] = (value_ref[rows, :] + value_grad).astype(jnp.bfloat16)

    attend_back(row_ref, turned_ref, q_ref, pair_ref, probs_ref, back_ref, put)
    for k, out_ref in enumerate(outs):
        out_ref[...] = slots_ref[k // 4, k % 4]


def product_kernel(t0, t1, t2, t3, n0, n1, n2, n3_low, n3_high, *refs):
    keep_ref, send_ref, sum_ref, n3 = refs[-4:]
    half = keep_ref.shape[0]
    core = lax.bitwise_and(lax.axis_index("clip"), 1)
    cut = n3_low.shape[0]
    n3[:cut, :] = n3_low[...]
    n3[cut:, :] = n3_high[...]
    total = None
    for t, n in ((t0, n0), (t1, n1), (t2, n2), (t3, n3)):
        term = jnp.dot(t[...], n[...], preferred_element_type=jnp.float32)
        total = term if total is None else total + term
    sum_ref[...] = total
    keep_ref[...] = sum_ref[pl.ds(pl.multiple_of(core * half, 8), half), :]
    other = sum_ref[pl.ds(pl.multiple_of((1 - core) * half, 8), half), :]
    send_ref[...] = other.astype(jnp.bfloat16)


def call(kernel, outs, kinds, flops, args, scratch=(), limit=30):
    spec = {
        "s": pl.BlockSpec(memory_space=pltpu.SMEM),
        "v": pl.BlockSpec(memory_space=pltpu.VMEM),
        "a": pl.BlockSpec(memory_space=pl.ANY),
    }
    return pl.pallas_call(
        kernel,
        out_shape=outs,
        in_specs=[spec[kind] for kind in kinds],
        out_specs=jax.tree.map(lambda _: spec["v"], outs),
        scratch_shapes=list(scratch),
        cost_estimate=pl.CostEstimate(flops=flops, bytes_accessed=4_000_000, transcendentals=0),
        compiler_params=pltpu.CompilerParams(vmem_limit_bytes=limit * 1024 * 1024),
    )(*args)


def fast_body(
    n_clip,
    patches,
    clip_tokens,
    positions,
    norm_gain,
    norm_bias,
    w_qkv,
    b_qkv,
    w_proj,
    b_proj,
    merge_gain,
    merge_bias,
    grad_placed,
):
    rows, width = patches.shape
    local = w_qkv.shape[2]
    heads = local // HEAD
    share_rows = grad_placed.shape[0]
    low = jnp.bfloat16
    shape = jax.ShapeDtypeStruct
    full = shape((rows, width), low)

    def swap(value):
        return lax.ppermute(value, "seq", [(0, 1), (1, 0)])

    def flip(value, bits):
        return lax.ppermute(value, "clip", [(i, i ^ bits) for i in range(n_clip)])

    counted = jnp.minimum(clip_tokens, rows // 4)
    half = rows // 2
    part, wide = shape((half, width), low), shape((half, width), jnp.float32)
    probs_half = shape((heads, half, rows), low)
    query = shape((half, local), low)
    attended = pltpu.VMEM((half, local), low)
    block = 3 * local // 8
    up_send = call(
        pull_kernel,
        part,
        "aaa",
        4 * rows * share_rows * width,
        (clip_tokens, positions, grad_placed),
        (
            pltpu.SMEM((1,), jnp.int32),
            pltpu.VMEM(positions.shape, jnp.int32),
            pltpu.VMEM(grad_placed.shape, low),
            pltpu.SemaphoreType.DMA((6,)),
        ),
        limit=62,
    )
    up_came = swap(up_send)
    normed = call(norm_kernel, full, "vvv", 100 * rows * width, (norm_gain, norm_bias, patches))
    normed_of = [normed] + [flip(normed, q << 1) for q in (1, 2)]
    normed_of += [flip(normed_of[2][:half], 1 << 1), flip(normed_of[1][half:], 2 << 1)]
    other_query, pair, own_normed, w_query, other_probs, part_send = call(
        first_kernel,
        (query, shape((2, rows, local), low), part, shape((width, local), low), probs_half, part),
        "avvaa",
        7 * rows * width * local,
        (
            clip_tokens,
            b_qkv,
            normed,
            jnp.transpose(w_qkv, (1, 0, 2)),
            w_proj,
        ),
        (
            pltpu.SMEM((1,), jnp.int32),
            pltpu.VMEM((2, width, local), low),
            pltpu.VMEM((local, width), low),
            attended,
            pltpu.SemaphoreType.DMA((5,)),
        ),
        limit=49,
    )
    part_came = swap(part_send)
    own_query, own_probs, part_keep, up_keep, turned = call(
        second_kernel,
        (query, probs_half, wide, part, shape((width, local), low)),
        "svvvvvvv",
        5 * half * width * local,
        (
            counted,
            positions,
            grad_placed,
            b_qkv,
            own_normed,
            w_query,
            pair,
            w_proj,
        ),
        (attended,),
    )
    merged, own_rows = call(
        middle_kernel,
        (part, part),
        "v" * 8,
        100 * half * width,
        (
            b_proj,
            merge_gain,
            merge_bias,
            part_keep,
            part_came,
            patches,
            up_keep,
            up_came,
        ),
    )
    other_rows = swap(own_rows)
    other_merged = swap(merged)
    query_own, key_own, value_own = call(
        own_back_kernel,
        (
            shape((local, half), low),
            shape((local, rows), jnp.float32),
            shape((local, rows), jnp.float32),
        ),
        "vvvvv",
        4 * half * width * local,
        (own_rows, turned, own_query, pair, own_probs),
        (attended,),
    )
    sent = call(
        other_back_kernel,
        (shape((block, rows), low),) * 8,
        "v" * 8,
        4 * half * width * local,
        (
            other_rows,
            turned,
            other_query,
            pair,
            other_probs,
            query_own,
            key_own,
            value_own,
        ),
        (attended, pltpu.VMEM((2, 4, block, rows), low)),
    )

    def exchange(sent):
        diagonal = flip(sent[3], 3 << 1)
        return [sent[0]] + [flip(sent[q], q << 1) for q in (1, 2)] + [diagonal]

    def product(taken, after=()):
        return call(
            product_kernel,
            (shape((block // 2, width), jnp.float32), shape((block // 2, width), low)),
            "v" * 9 + "a" * len(after),
            8 * block * rows * width,
            (*taken, *normed_of, *after),
            (pltpu.VMEM((block, width), jnp.float32), pltpu.VMEM((rows, width), low)),
        )

    far_taken = exchange(sent[:4])
    near_taken = exchange(sent[4:])
    far_keep, far_send = product(far_taken)
    far_came = flip(far_send, 1)
    far_sum = (far_keep + far_came.astype(jnp.float32)).astype(low)
    crossing = flip(far_sum, 8)
    near_keep, near_send = product(near_taken, (far_sum,))
    near_came = flip(near_send, 1)
    placed = call(
        place_kernel,
        shape((share_rows, 4 * width), low),
        "svvva",
        8 * rows * share_rows * width,
        (counted, positions, merged, other_merged, far_sum),
    )
    summed = near_keep + near_came.astype(jnp.float32) + crossing.astype(jnp.float32)
    return (placed, summed[None])


def solution(mesh):
    n_clip, n_seq = mesh.shape["clip"], mesh.shape["seq"]
    fast = n_clip == 2 * 4 * 2 and n_seq == 2
    body = functools.partial(fast_body, n_clip) if fast else general_body
    return jax.shard_map(
        body,
        mesh=mesh,
        in_specs=(
            P("clip", None),
            P("clip"),
            P("clip", None),
            P(),
            P(),
            P(None, None, "seq"),
            P(None, "seq"),
            P("seq", None),
            P(),
            P(),
            P(),
            P(("clip", "seq"), None),
        ),
        out_specs=(P(("clip", "seq"), None), P("seq", "clip", None)),
        check_vma=False,
    )
```

```python
import functools

import jax
import jax.numpy as jnp
from jax import lax
from jax.experimental import pallas as pl
from jax.experimental.pallas import tpu as pltpu
from jax.sharding import PartitionSpec as P


HEAD = 80


EPSILON = 1e-06


def normalize(values, gain_row, bias_row):
    center = values - jnp.mean(values, axis=-1, keepdims=True)
    inverse = lax.rsqrt(jnp.mean(center * center, axis=-1, keepdims=True) + EPSILON)
    unit_rows = center * inverse
    return (unit_rows * gain_row + bias_row, unit_rows, inverse)


def normalize_back(upstream, unit_rows, inverse, gain_row):
    scaled = upstream * gain_row
    return inverse * (
        scaled
        - jnp.mean(scaled, axis=-1, keepdims=True)
        - unit_rows * jnp.mean(scaled * unit_rows, axis=-1, keepdims=True)
    )


def leading(left, right):
    return lax.dot_general(
        left, right, (((0,), (0,)), ((), ())), preferred_element_type=jnp.float32
    )


def trailing(left, right):
    return lax.dot_general(
        left, right, (((1,), (1,)), ((), ())), preferred_element_type=jnp.float32
    )


def general_body(
    patches,
    clip_tokens,
    positions,
    norm_gain,
    norm_bias,
    w_qkv,
    b_qkv,
    w_proj,
    b_proj,
    merge_gain,
    merge_bias,
    grad_placed,
):
    block_rows = patches.shape[0]
    model_width = patches.shape[1]
    local_width = w_qkv.shape[2]
    local_heads = local_width // HEAD
    live_count = clip_tokens[0]
    places = positions[0]
    widened = patches.astype(jnp.float32)
    normed = normalize(widened, norm_gain, norm_bias)[0].astype(jnp.bfloat16)
    triple = jnp.dot(
        normed, w_qkv.reshape(model_width, 3 * local_width), preferred_element_type=jnp.float32
    )
    triple = (triple.reshape(block_rows, 3, local_width) + b_qkv).astype(jnp.bfloat16)
    query_rows = triple[:, 0].reshape(block_rows, local_heads, HEAD)
    key_rows = triple[:, 1].reshape(block_rows, local_heads, HEAD)
    value_rows = triple[:, 2].reshape(block_rows, local_heads, HEAD)
    scaling = HEAD ** (-0.5)
    scores = (
        jnp.einsum("qhd,khd->hqk", query_rows, key_rows, preferred_element_type=jnp.float32)
        * scaling
    )
    live_keys = jnp.arange(block_rows, dtype=jnp.int32) < 4 * live_count
    scores = jnp.where(live_keys[None, None, :], scores, -1e30)
    highest = jnp.max(scores, axis=-1, keepdims=True)
    powers = jnp.exp(scores - highest)
    weights = powers / jnp.sum(powers, axis=-1, keepdims=True)
    weights_low = weights.astype(jnp.bfloat16)
    attended = jnp.einsum(
        "hqk,khd->qhd", weights_low, value_rows, preferred_element_type=jnp.float32
    )
    attended = attended.reshape(block_rows, local_width).astype(jnp.bfloat16)
    partial_value = jnp.dot(attended, w_proj, preferred_element_type=jnp.float32)
    summed_share = lax.psum_scatter(
        partial_value.astype(jnp.bfloat16), "seq", scatter_dimension=0, tiled=True
    ).astype(jnp.float32)
    share_count = summed_share.shape[0]
    own_start = lax.axis_index("seq") * share_count
    own_patches = lax.dynamic_slice_in_dim(widened, own_start, share_count, 0)
    output_share = summed_share + b_proj + own_patches
    output = lax.all_gather(output_share.astype(jnp.bfloat16), "seq", axis=0, tiled=True).astype(
        output_share.dtype
    )
    merged_full, unit_rows, inverse = normalize(output, merge_gain, merge_bias)
    merged = merged_full.reshape(block_rows // 4, 4 * model_width).astype(jnp.bfloat16)
    live_tokens = jnp.arange(block_rows // 4, dtype=jnp.int32) < live_count
    share_rows = grad_placed.shape[0]
    rows_here = lax.axis_index("seq") * share_rows + jnp.arange(share_rows, dtype=jnp.int32)
    selector = ((places[None, :] == rows_here[:, None]) & live_tokens[None, :]).astype(jnp.bfloat16)
    placed = jnp.dot(selector, merged, preferred_element_type=jnp.float32).astype(jnp.bfloat16)
    own_grad = leading(selector, grad_placed)
    token_grad = lax.psum(own_grad.astype(jnp.bfloat16), "seq").astype(jnp.float32)
    upstream = token_grad.reshape(block_rows, model_width)
    row_grad = normalize_back(upstream, unit_rows, inverse, merge_gain).astype(jnp.bfloat16)
    attn_grad = lax.dot_general(
        row_grad, w_proj, (((1,), (1,)), ((), ())), preferred_element_type=jnp.float32
    )
    attn_grad = attn_grad.astype(jnp.bfloat16).reshape(block_rows, local_heads, HEAD)
    prob_grad = jnp.einsum(
        "qhd,khd->hqk", attn_grad, value_rows, preferred_element_type=jnp.float32
    )
    value_grad = jnp.einsum(
        "hqk,qhd->khd", weights_low, attn_grad, preferred_element_type=jnp.float32
    )
    score_grad = (
        weights * (prob_grad - jnp.sum(prob_grad * weights, axis=-1, keepdims=True)) * scaling
    )
    score_grad = score_grad.astype(jnp.bfloat16)
    query_grad = jnp.einsum(
        "hqk,khd->qhd", score_grad, key_rows, preferred_element_type=jnp.float32
    )
    key_grad = jnp.einsum(
        "hqk,qhd->khd", score_grad, query_rows, preferred_element_type=jnp.float32
    )
    triple_grad = jnp.stack([query_grad, key_grad, value_grad], axis=1)
    triple_grad = triple_grad.reshape(block_rows, 3 * local_width).astype(jnp.bfloat16)
    full_term = leading(triple_grad, normed)
    summed = lax.psum_scatter(full_term, "clip", scatter_dimension=0, tiled=True)
    return (placed, summed[None])


def place_masks(live_ref, places, share_rows, rows, first_row):
    tokens = places.shape[1]
    token = lax.broadcasted_iota(jnp.int32, (tokens, rows), 0)
    owner = (lax.broadcasted_iota(jnp.int32, (tokens, rows), 1) + first_row) // 4
    spread = jnp.where((token == owner) & (token < live_ref[0]), 1.0, 0.0)
    shifted = jnp.broadcast_to(places.astype(jnp.float32) + 1.0, (8, tokens))
    row = jnp.dot(shifted, spread, precision=lax.Precision.HIGHEST)[:1] - 1.0
    first = lax.axis_index("seq") * share_rows
    window = lax.broadcasted_iota(jnp.int32, (share_rows, rows), 0) + first
    patch = lax.broadcasted_iota(jnp.int32, (share_rows, rows), 1)
    hit = window.astype(jnp.float32) == row
    return [
        jnp.where(hit & (lax.rem(patch, 4) == k), 1.0, 0.0).astype(jnp.bfloat16) for k in range(4)
    ]


def begin(sources, targets, sems, first=0):
    copies = [
        pltpu.make_async_copy(source, target, sems.at[first + k])
        for k, (source, target) in enumerate(zip(sources, targets, strict=True))
    ]
    for copy in copies:
        copy.start()
    return copies


def half_start(half, own):
    seq = lax.axis_index("seq")
    return pl.multiple_of((seq if own else 1 - seq) * half, 128)


def norm_low(patches_ref, gain_ref, bias_ref):
    return normalize(
        patches_ref[...].astype(jnp.float32), gain_ref[...][None, :], bias_ref[...][None, :]
    )[0].astype(jnp.bfloat16)


def pull(live_ref, places_ref, grad_ref, out_ref, own):
    half, width = out_ref.shape
    masks = place_masks(
        live_ref, places_ref[...], grad_ref.shape[0], half, half_start(half, own)
    )
    total = None
    for k in range(4):
        term = leading(masks[k], grad_ref[:, k * width : (k + 1) * width])
        total = term if total is None else total + term
    out_ref[...] = total.astype(out_ref.dtype)


def pull_kernel(live_ref, places_hbm, grad_hbm, send_ref, places_ref, grad_ref, sems):
    half, width = send_ref.shape
    came = begin((places_hbm,), (places_ref,), sems)
    blocks = [slice(k * width, (k + 1) * width) for k in range(4)]
    came += begin(
        [grad_hbm.at[:, block] for block in blocks],
        [grad_ref.at[:, block] for block in blocks],
        sems,
        1,
    )
    came[0].wait()
    masks = place_masks(
        live_ref, places_ref[...], grad_ref.shape[0], half, half_start(half, False)
    )
    total = None
    for k in range(4):
        came[1 + k].wait()
        term = leading(masks[k], grad_ref[:, blocks[k]])
        total = term if total is None else total + term
    send_ref[...] = total.astype(send_ref.dtype)


def norm_kernel(gain_ref, bias_ref, patches_ref, normed_ref):
    normed_ref[...] = norm_low(patches_ref, gain_ref, bias_ref)


def place_kernel(live_ref, places_ref, own_ref, other_ref, _, out_ref):
    half, width = own_ref.shape
    share_rows = out_ref.shape[0]
    own = place_masks(live_ref, places_ref[...], share_rows, half, half_start(half, True))
    other = place_masks(live_ref, places_ref[...], share_rows, half, half_start(half, False))
    for k in range(4):
        term = jnp.dot(own[k], own_ref[...], preferred_element_type=jnp.float32)
        term += jnp.dot(other[k], other_ref[...], preferred_element_type=jnp.float32)
        out_ref[:, k * width : (k + 1) * width] = term.astype(out_ref.dtype)


def attend(live_ref, query_ref, pair_ref, probs_ref, attended_ref):
    half, rows = probs_ref.shape[1:]
    live = lax.broadcasted_iota(jnp.int32, (half, rows), 1) < 4 * live_ref[0]
    steep = HEAD ** (-0.5) * 1.4426950408889634
    for h in range(probs_ref.shape[0]):
        cols = slice(h * HEAD, (h + 1) * HEAD)
        scores = trailing(query_ref[:, cols], pair_ref[0, :, cols])
        scores = jnp.where(live, scores, -1e30)
        powers = jnp.exp2((scores - jnp.max(scores, axis=-1, keepdims=True)) * steep)
        weights = powers * (1.0 / jnp.sum(powers, axis=-1, keepdims=True))
        weights = weights.astype(jnp.bfloat16)
        probs_ref[h] = weights
        attended_ref[:, cols] = jnp.dot(
            weights, pair_ref[1, :, cols], preferred_element_type=jnp.float32
        ).astype(jnp.bfloat16)


def first_kernel(
    live_ref,
    b_ref,
    normed_ref,
    w_hbm,
    proj_hbm,
    query_ref,
    pair_ref,
    own_ref,
    wq_ref,
    probs_ref,
    send_ref,
    w_ref,
    proj_ref,
    attended_ref,
    sems,
):
    came = begin(
        (w_hbm.at[0], w_hbm.at[1], w_hbm.at[2], proj_hbm),
        (wq_ref, w_ref.at[0], w_ref.at[1], proj_ref),
        sems,
    )
    half = send_ref.shape[0]
    start = half_start(half, False)
    own_ref[...] = normed_ref[pl.ds(half_start(half, True), half), :]
    came[0].wait()
    part = jnp.dot(
        normed_ref[pl.ds(start, half), :], wq_ref[...], preferred_element_type=jnp.float32
    )
    query_ref[...] = (part + b_ref[0:1, :]).astype(jnp.bfloat16)
    for t in (1, 2):
        came[t].wait()
        part = jnp.dot(normed_ref[...], w_ref[t - 1], preferred_element_type=jnp.float32)
        pair_ref[t - 1] = (part + b_ref[t : t + 1, :]).astype(jnp.bfloat16)
    attend(live_ref, query_ref, pair_ref, probs_ref, attended_ref)
    came[3].wait()
    send_ref[...] = jnp.dot(
        attended_ref[...], proj_ref[...], preferred_element_type=jnp.float32
    ).astype(jnp.bfloat16)


def second_kernel(
    live_ref,
    places_ref,
    grad_ref,
    b_ref,
    own_ref,
    w_ref,
    pair_ref,
    proj_ref,
    query_ref,
    probs_ref,
    keep_ref,
    up_ref,
    turned_ref,
    attended_ref,
):
    turned_ref[...] = proj_ref[...].T
    pull(live_ref, places_ref, grad_ref, up_ref, True)
    part = jnp.dot(own_ref[...], w_ref[...], preferred_element_type=jnp.float32)
    query_ref[...] = (part + b_ref[0:1, :]).astype(jnp.bfloat16)
    attend(live_ref, query_ref, pair_ref, probs_ref, attended_ref)
    keep_ref[...] = jnp.dot(attended_ref[...], proj_ref[...], preferred_element_type=jnp.float32)


def middle_kernel(
    b_ref,
    gain_ref,
    bias_ref,
    keep_ref,
    came_ref,
    patches_ref,
    up_keep_ref,
    up_came_ref,
    merged_ref,
    back_ref,
):
    half = keep_ref.shape[0]
    gain = gain_ref[...][None, :]
    output = (
        keep_ref[...]
        + came_ref[...].astype(jnp.float32)
        + b_ref[...][None, :]
        + patches_ref[pl.ds(half_start(half, True), half), :].astype(jnp.float32)
    )
    merged, unit_rows, inverse = normalize(output, gain, bias_ref[...][None, :])
    merged_ref[...] = merged.astype(jnp.bfloat16)
    upstream = up_keep_ref[...].astype(jnp.float32) + up_came_ref[...].astype(jnp.float32)
    back_ref[...] = normalize_back(upstream, unit_rows, inverse, gain).astype(jnp.bfloat16)


def attend_back(row_ref, turned_ref, query_ref, pair_ref, probs_ref, back_ref, put):
    back_ref[...] = jnp.dot(
        row_ref[...], turned_ref[...], preferred_element_type=jnp.float32
    ).astype(jnp.bfloat16)
    scaling = HEAD ** (-0.5)
    for h in range(probs_ref.shape[0]):
        cols = slice(h * HEAD, (h + 1) * HEAD)
        back = back_ref[:, cols]
        weights = probs_ref[h]
        prob_grad = trailing(back, pair_ref[1, :, cols])
        wide = weights.astype(jnp.float32)
        inner = jnp.sum(prob_grad * wide, axis=-1, keepdims=True)
        score_grad = (wide * (prob_grad - inner)).astype(jnp.bfloat16)
        query_grad = jnp.dot(
            score_grad, pair_ref[0, :, cols], preferred_element_type=jnp.float32
        )
        key_grad = leading(query_ref[:, cols], score_grad)
        put(h, (query_grad * scaling).T, key_grad * scaling, leading(back, weights))


def own_back_kernel(
    row_ref, turned_ref, q_ref, pair_ref, probs_ref, query_ref, key_ref, value_ref, back_ref
):
    def put(h, query_grad, key_grad, value_grad):
        rows = slice(h * HEAD, (h + 1) * HEAD)
        query_ref[rows, :] = query_grad.astype(jnp.bfloat16)
        key_ref[rows, :] = key_grad
        value_ref[rows, :] = value_grad

    attend_back(row_ref, turned_ref, q_ref, pair_ref, probs_ref, back_ref, put)


def other_back_kernel(
    row_ref, turned_ref, q_ref, pair_ref, probs_ref, query_ref, key_ref, value_ref, *refs
):
    outs, (back_ref, slots_ref) = refs[:8], refs[8:]
    half = row_ref.shape[0]
    heads = probs_ref.shape[0]
    per_block = slots_ref.shape[2] // HEAD
    me = lax.axis_index("clip")
    turn = lax.bitwise_and(lax.shift_right_logical(me, 1), 3)
    away = 1 - lax.shift_right_logical(me, 3)
    mine, start = half_start(half, True), half_start(half, False)

    def where(t, h):
        piece = t * heads + h
        block, sub = piece // per_block, piece % per_block
        slot = lax.bitwise_xor(turn, block % 4)
        side = lax.bitwise_xor(away, block // 4)
        return side, slot, slice(sub * HEAD, (sub + 1) * HEAD)

    def put(h, query_grad, key_grad, value_grad):
        rows = slice(h * HEAD, (h + 1) * HEAD)
        side, slot, place = where(0, h)
        slots_ref[side, slot, place, pl.ds(mine, half)] = query_ref[rows, :]
        slots_ref[side, slot, place, pl.ds(start, half)] = query_grad.astype(jnp.bfloat16)
        side, slot, place = where(1, h)
        slots_ref[side, slot, place, :] = (key_ref[rows, :] + key_grad).astype(jnp.bfloat16)
        side, slot, place = where(2, h)
        slots_ref[side, slot, place, :] = (value_ref[rows, :] + value_grad).astype(jnp.bfloat16)

    attend_back(row_ref, turned_ref, q_ref, pair_ref, probs_ref, back_ref, put)
    for k, out_ref in enumerate(outs):
        out_ref[...] = slots_ref[k // 4, k % 4]


def product_kernel(t0, t1, t2, t3, n0, n1, n2, n3_low, n3_high, *refs):
    keep_ref, send_ref, sum_ref, n3 = refs[-4:]
    half = keep_ref.shape[0]
    core = lax.bitwise_and(lax.axis_index("clip"), 1)
    cut = n3_low.shape[0]
    n3[:cut, :] = n3_low[...]
    n3[cut:, :] = n3_high[...]
    total = None
    for t, n in ((t0, n0), (t1, n1), (t2, n2), (t3, n3)):
        term = jnp.dot(t[...], n[...], preferred_element_type=jnp.float32)
        total = term if total is None else total + term
    sum_ref[...] = total
    keep_ref[...] = sum_ref[pl.ds(pl.multiple_of(core * half, 8), half), :]
    other = sum_ref[pl.ds(pl.multiple_of((1 - core) * half, 8), half), :]
    send_ref[...] = other.astype(jnp.bfloat16)


def call(kernel, outs, kinds, flops, args, scratch=(), limit=30):
    spec = {
        "s": pl.BlockSpec(memory_space=pltpu.SMEM),
        "v": pl.BlockSpec(memory_space=pltpu.VMEM),
        "a": pl.BlockSpec(memory_space=pl.ANY),
    }
    return pl.pallas_call(
        kernel,
        out_shape=outs,
        in_specs=[spec[kind] for kind in kinds],
        out_specs=jax.tree.map(lambda _: spec["v"], outs),
        scratch_shapes=list(scratch),
        cost_estimate=pl.CostEstimate(flops=flops, bytes_accessed=4_000_000, transcendentals=0),
        compiler_params=pltpu.CompilerParams(vmem_limit_bytes=limit * 1024 * 1024),
    )(*args)


def fast_body(
    n_clip,
    patches,
    clip_tokens,
    positions,
    norm_gain,
    norm_bias,
    w_qkv,
    b_qkv,
    w_proj,
    b_proj,
    merge_gain,
    merge_bias,
    grad_placed,
):
    rows, width = patches.shape
    local = w_qkv.shape[2]
    heads = local // HEAD
    share_rows = grad_placed.shape[0]
    low = jnp.bfloat16
    shape = jax.ShapeDtypeStruct
    full = shape((rows, width), low)

    def swap(value):
        return lax.ppermute(value, "seq", [(0, 1), (1, 0)])

    def flip(value, bits):
        return lax.ppermute(value, "clip", [(i, i ^ bits) for i in range(n_clip)])

    half = rows // 2
    part, wide = shape((half, width), low), shape((half, width), jnp.float32)
    probs_half = shape((heads, half, rows), low)
    query = shape((half, local), low)
    attended = pltpu.VMEM((half, local), low)
    block = 3 * local // 8
    up_send = call(
        pull_kernel,
        part,
        "saa",
        4 * rows * share_rows * width,
        (clip_tokens, positions, grad_placed),
        (
            pltpu.VMEM(positions.shape, jnp.int32),
            pltpu.VMEM(grad_placed.shape, low),
            pltpu.SemaphoreType.DMA((5,)),
        ),
        limit=62,
    )
    up_came = swap(up_send)
    normed = call(norm_kernel, full, "vvv", 100 * rows * width, (norm_gain, norm_bias, patches))
    normed_of = [normed] + [flip(normed, q << 1) for q in (1, 2)]
    normed_of += [flip(normed_of[2][:half], 1 << 1), flip(normed_of[1][half:], 2 << 1)]
    other_query, pair, own_normed, w_query, other_probs, part_send = call(
        first_kernel,
        (query, shape((2, rows, local), low), part, shape((width, local), low), probs_half, part),
        "svvaa",
        7 * rows * width * local,
        (
            clip_tokens,
            b_qkv,
            normed,
            jnp.transpose(w_qkv, (1, 0, 2)),
            w_proj,
        ),
        (
            pltpu.VMEM((2, width, local), low),
            pltpu.VMEM((local, width), low),
            attended,
            pltpu.SemaphoreType.DMA((4,)),
        ),
        limit=49,
    )
    part_came = swap(part_send)
    own_query, own_probs, part_keep, up_keep, turned = call(
        second_kernel,
        (query, probs_half, wide, part, shape((width, local), low)),
        "svvvvvvv",
        5 * half * width * local,
        (
            clip_tokens,
            positions,
            grad_placed,
            b_qkv,
            own_normed,
            w_query,
            pair,
            w_proj,
        ),
        (attended,),
    )
    merged, own_rows = call(
        middle_kernel,
        (part, part),
        "v" * 8,
        100 * half * width,
        (
            b_proj,
            merge_gain,
            merge_bias,
            part_keep,
            part_came,
            patches,
            up_keep,
            up_came,
        ),
    )
    other_rows = swap(own_rows)
    other_merged = swap(merged)
    query_own, key_own, value_own = call(
        own_back_kernel,
        (
            shape((local, half), low),
            shape((local, rows), jnp.float32),
            shape((local, rows), jnp.float32),
        ),
        "vvvvv",
        4 * half * width * local,
        (own_rows, turned, own_query, pair, own_probs),
        (attended,),
    )
    sent = call(
        other_back_kernel,
        (shape((block, rows), low),) * 8,
        "v" * 8,
        4 * half * width * local,
        (
            other_rows,
            turned,
            other_query,
            pair,
            other_probs,
            query_own,
            key_own,
            value_own,
        ),
        (attended, pltpu.VMEM((2, 4, block, rows), low)),
    )

    def exchange(sent):
        diagonal = flip(sent[3], 3 << 1)
        high = flip(sent[2], 2 << 1)
        return [sent[0], flip(sent[1], 1 << 1), high, diagonal]

    def product(taken, after=()):
        return call(
            product_kernel,
            (shape((block // 2, width), jnp.float32), shape((block // 2, width), low)),
            "v" * 9 + "a" * len(after),
            8 * block * rows * width,
            (*taken, *normed_of, *after),
            (pltpu.VMEM((block, width), jnp.float32), pltpu.VMEM((rows, width), low)),
        )

    far_taken = exchange(sent[:4])
    near_taken = exchange(sent[4:])
    far_keep, far_send = product(far_taken)
    far_came = flip(far_send, 1)
    far_sum = (far_keep + far_came.astype(jnp.float32)).astype(low)
    crossing = flip(far_sum, 8)
    near_keep, near_send = product(near_taken, (far_sum,))
    near_came = flip(near_send, 1)
    placed = call(
        place_kernel,
        shape((share_rows, 4 * width), low),
        "svvva",
        8 * rows * share_rows * width,
        (clip_tokens, positions, merged, other_merged, far_sum),
    )
    summed = near_keep + near_came.astype(jnp.float32) + crossing.astype(jnp.float32)
    return (placed, summed[None])


def solution(mesh):
    n_clip, n_seq = mesh.shape["clip"], mesh.shape["seq"]
    fast = n_clip == 2 * 4 * 2 and n_seq == 2
    body = functools.partial(fast_body, n_clip) if fast else general_body
    return jax.shard_map(
        body,
        mesh=mesh,
        in_specs=(
            P("clip", None),
            P("clip"),
            P("clip", None),
            P(),
            P(),
            P(None, None, "seq"),
            P(None, "seq"),
            P("seq", None),
            P(),
            P(),
            P(),
            P(("clip", "seq"), None),
        ),
        out_specs=(P(("clip", "seq"), None), P("seq", "clip", None)),
        check_vma=False,
    )
```
